32 devices in a mesh: groups: 2 (over y), seq: 4 (over z), head: 4 (over x, core).
Axes of the slice: x: 2, y: 2, z: 4, core: 2. Of those that a mesh axis runs over, the one named last changes fastest.
Arguments:
- residual: bfloat16 [1024, 2048], P(('groups', 'seq')), parts along dimension 0, may hold values from -6 to 6
- query_in: bfloat16 [1024, 2048], P(('groups', 'seq'), 'head'), parts along dimension 0, may hold values from -6 to 6
- key_in: bfloat16 [1024, 2048], P(('groups', 'seq'), 'head'), parts along dimension 0, may hold values from -6 to 6
- value_in: bfloat16 [1024, 4096], P(('groups', 'seq'), 'head'), parts along dimension 0, may hold values from -6 to 6
- gating_in: bfloat16 [1024, 4096], P(('groups', 'seq'), 'head'), parts along dimension 0, may hold values from -6 to 6
- beta_logit: float32 [1024, 32], P(('groups', 'seq'), 'head'), parts along dimension 0, may hold values from -12 to 2
- decay_logit: float32 [1024, 32], P(('groups', 'seq'), 'head'), parts along dimension 0, may hold values from -16 to 1
- seq_length: int32 [2], P('groups'), parts along dimension 0, may hold values from 256 to 512
- conv_query: float32 [4, 2048], P(None, 'head'), may hold values from -3 to 3
- conv_key: float32 [4, 2048], P(None, 'head'), may hold values from -3 to 3
- conv_value: float32 [4, 4096], P(None, 'head'), may hold values from -3 to 3
- decay_rate: float32 [32], P('head'), may hold values from 0.5 to 17
- norm_gain: float32 [128], replicated, may hold values from 0.1 to 1.9
- out_weight: bfloat16 [4096, 2048], P('head'), may hold values from -0.09375 to 0.09375
- attn_gain: float32 [2048], replicated, may hold values from 0.1 to 1.9
- query_weight: bfloat16 [2048, 8192], P('seq', 'head'), may hold values from -1 to 1
- key_value_weight: bfloat16 [2048, 1024], P('seq'), may hold values from -10 to 10
Outputs:
- hidden_out: bfloat16 [1024, 2048], P(('groups', 'seq')), parts along dimension 0
- attention_out: bfloat16 [1024, 4096], P(('groups', 'seq'), 'head'), parts along dimension 0
The draws below stay inside these ranges and needn't reach their ends.
There are 2 independent parts, one for each index of `groups`. The reference program is written for one: setup_inputs(seed, part) draws one part's arguments, and reference() takes and returns one part's arrays. A program takes and returns all parts, laid end to end along the dimension named above; an argument that names none is the same for every part. Nothing has to cross between parts.
All inputs are finite; a program needn't handle non-finite values.
Results may differ from the reference program's by a relative error of at most 0.02.
The reference program's roundings to bfloat16 on the way count: a program that leaves them out, or rounds other values in their place, can miss the bound.
Values may be sent and summed in bfloat16 or wider, within the bound.
A program may use at most 128 MiB of HBM per device.

```python
import math
import jax
import jax.numpy as jnp
from jax import lax

MODEL_WIDTH = 2048
HK = 16
HV = 32
DK = 128
DV = 128
QUERY_HEADS = 16
KEY_VALUE_HEADS = 2
HEAD_WIDTH = 256
CONV = 4
TOK_DEV = 128
SEQUENCE_LENGTH = 512


def weight_pair(key):
    bound = 6.0 / math.sqrt(MODEL_WIDTH)
    first_matrix = jax.random.normal(jax.random.fold_in(key, 11), (MODEL_WIDTH, QUERY_HEADS * 2 * HEAD_WIDTH), jnp.float32) / math.sqrt(MODEL_WIDTH)
    first_matrix = jnp.clip(first_matrix, -bound, bound)
    second_matrix = jax.random.normal(jax.random.fold_in(key, 12), (MODEL_WIDTH, 2 * KEY_VALUE_HEADS * HEAD_WIDTH), jnp.float32) / math.sqrt(MODEL_WIDTH)
    second_matrix = jnp.clip(second_matrix, -bound, bound)
    return (first_matrix, second_matrix)


def draw_query_weight(key, part):
    return weight_pair(key)[0].astype(jnp.bfloat16)


def draw_key_value_weight(key, part):
    return weight_pair(key)[1].astype(jnp.bfloat16)


def draw_beta_logit(key, part):
    token_places = jnp.arange(SEQUENCE_LENGTH, dtype=jnp.int32)
    stretch_length = 3 * TOK_DEV
    stretch_total = SEQUENCE_LENGTH // stretch_length + 1
    quiet_table = jax.random.randint(jax.random.fold_in(key, 32), (stretch_total, HV), 0, 2)
    quiet_rows = quiet_table[token_places // stretch_length]
    active = jax.random.uniform(jax.random.fold_in(key, 31), (SEQUENCE_LENGTH, HV), jnp.float32, -2.5, 1.5)
    silent = jax.random.uniform(jax.random.fold_in(key, 33), (SEQUENCE_LENGTH, HV), jnp.float32, -12.0, -10.0)
    return jnp.where(quiet_rows == 1, silent, active)


def draw_decay_logit(key, part):
    token_places = jnp.arange(SEQUENCE_LENGTH, dtype=jnp.int32)
    slab_total = SEQUENCE_LENGTH // TOK_DEV
    slab_offset = jax.random.uniform(jax.random.fold_in(key, 24), (slab_total, HV), jnp.float32, -2.0, 1.0)
    starting_shift = -math.log(SEQUENCE_LENGTH) + jax.random.uniform(jax.random.fold_in(key, 21), (SEQUENCE_LENGTH, HV), jnp.float32, -1.5, 1.5)
    starting_shift = starting_shift + slab_offset[token_places // TOK_DEV]
    location_entries = jax.random.randint(jax.random.fold_in(key, 22), (3, HV), 0, SEQUENCE_LENGTH)
    contiguous_lines = jnp.any(token_places[:, None, None] == location_entries[None], axis=1)
    threshold_amount = jax.random.uniform(jax.random.fold_in(key, 23), (SEQUENCE_LENGTH, HV), jnp.float32, 0.0, 1.0)
    return jnp.where(contiguous_lines, threshold_amount, starting_shift)


def block_levels(own_key, shape, split, smallest, top_value):
    loudness = 1.0
    for dim, parts in split:
        draws = jax.random.uniform(jax.random.fold_in(jax.random.fold_in(own_key, 6), dim), (parts,), jnp.float32, smallest / len(split), top_value / len(split))
        loudness = loudness * jnp.repeat(jnp.exp(draws), shape[dim] // parts).reshape((-1,) + (1,) * (len(shape) - 1 - dim))
    return loudness


def gaussian(own_key, shape, deviation, most, shards=(), kind=jnp.bfloat16):
    result = jax.random.normal(own_key, shape, jnp.float32) * deviation
    if len(shards) > 0:
        result = block_levels(own_key, shape, shards, -0.22, 0.18) * result
    return jnp.clip(result, min=-most, max=most).astype(kind)


def setup_inputs(seed: int = 0, part: int = 0) -> dict:
    keys = jax.random.split(jax.random.key(seed), 18)
    own_keys = jax.random.split(jax.random.fold_in(keys[17], part), 18)
    return {
        "residual": gaussian(own_keys[0], (SEQUENCE_LENGTH, MODEL_WIDTH), 1.0, 6.0, ((0, 4),)),
        "query_in": gaussian(own_keys[1], (SEQUENCE_LENGTH, HK * DK), 1.0, 6.0, ((0, 4), (1, 4))),
        "key_in": gaussian(own_keys[2], (SEQUENCE_LENGTH, HK * DK), 1.0, 6.0, ((0, 4), (1, 4))),
        "value_in": gaussian(own_keys[3], (SEQUENCE_LENGTH, HV * DV), 1.0, 6.0, ((0, 4), (1, 4))),
        "gating_in": gaussian(own_keys[4], (SEQUENCE_LENGTH, HV * DV), 1.0, 6.0, ((0, 4), (1, 4))),
        "beta_logit": draw_beta_logit(jax.random.fold_in(jax.random.fold_in(keys[17], part), 71), part),
        "decay_logit": draw_decay_logit(jax.random.fold_in(jax.random.fold_in(keys[17], part), 71), part),
        "seq_length": jax.random.randint(own_keys[7], (1,), SEQUENCE_LENGTH // 2, SEQUENCE_LENGTH + 1).astype(jnp.int32),
        "conv_query": gaussian(keys[8], (CONV, HK * DK), 0.5, 3.0, ((1, 4),), jnp.float32),
        "conv_key": gaussian(keys[9], (CONV, HK * DK), 0.5, 3.0, ((1, 4),), jnp.float32),
        "conv_value": gaussian(keys[10], (CONV, HV * DV), 0.5, 3.0, ((1, 4),), jnp.float32),
        "decay_rate": jnp.clip(jnp.exp(math.log(17.0) - 3.5263605 * jax.random.uniform(keys[11], (HV,), jnp.float32) ** block_levels(keys[11], (HV,), ((0, 4),), -0.2, 0.2)), 0.5, 17.0),
        "norm_gain": jnp.clip(1.0 + 0.18 * jax.random.normal(keys[12], (DV,), jnp.float32), 0.1, 1.9),
        "out_weight": gaussian(keys[13], (HV * DV, MODEL_WIDTH), (HV * DV) ** -0.5, 0.09375, ((0, 4),)),
        "attn_gain": jnp.clip(1.0 + 0.18 * jax.random.normal(keys[14], (MODEL_WIDTH,), jnp.float32), 0.1, 1.9),
        "query_weight": draw_query_weight(jax.random.fold_in(keys[17], 71), part),
        "key_value_weight": draw_key_value_weight(jax.random.fold_in(keys[17], 71), part),
    }


EPSILON = 1e-06
NEGATIVE = -1e+30

def causal_conv(inputs, kernel):
    widened = inputs.astype(jnp.float32)
    padded = jnp.concatenate([jnp.zeros((CONV - 1, widened.shape[1]), jnp.float32), widened], 0)
    summed = jnp.zeros_like(widened)
    for offset in range(CONV):
        summed = summed + kernel[offset] * padded[offset:offset + widened.shape[0]]
    return jax.nn.silu(summed)

def unit_rows(tensor):
    return tensor / jnp.sqrt(lax.optimization_barrier(jnp.sum(tensor * tensor, -1, keepdims=True)) + EPSILON)

def reference(residual, query_in, key_in, value_in, gating_in, beta_logit, decay_logit, seq_length, conv_query, conv_key, conv_value, decay_rate, norm_gain, out_weight, attn_gain, query_weight, key_value_weight):
    highest_index = lax.Precision.HIGHEST
    positions = jnp.arange(SEQUENCE_LENGTH, dtype=jnp.int32)
    length_now = seq_length[0].astype(jnp.int32)
    alive_mask = (positions < length_now).astype(jnp.float32)
    queries = unit_rows(causal_conv(query_in, conv_query).reshape(SEQUENCE_LENGTH, HK, DK)) * DK ** (-0.5)
    keyset = unit_rows(causal_conv(key_in, conv_key).reshape(SEQUENCE_LENGTH, HK, DK))
    values = causal_conv(value_in, conv_value).reshape(SEQUENCE_LENGTH, HV, DV)
    queries = jnp.repeat(queries, HV // HK, axis=1)
    keyset = jnp.repeat(keyset, HV // HK, axis=1)
    betas = jax.nn.sigmoid(beta_logit) * alive_mask[:, None]
    log_decay = -decay_rate[None, :] * jax.nn.softplus(decay_logit) * alive_mask[:, None]

    def advance(recurrent_state, inputs):
        current_query, current_key, value_now, beta_now, decay_now = inputs
        recurrent_state = jnp.exp(decay_now)[:, None, None] * recurrent_state
        prediction = jnp.einsum('ino,in->io', recurrent_state, current_key, precision=highest_index)
        recurrent_state = recurrent_state + beta_now[:, None, None] * current_key[:, :, None] * (value_now - prediction)[:, None, :]
        return (recurrent_state, jnp.einsum('ino,in->io', recurrent_state, current_query, precision=highest_index))
    initial = jnp.zeros((HV, DK, DV), jnp.float32)
    _, outputs = lax.scan(advance, initial, (queries, keyset, values, betas, log_decay))
    gating = gating_in.astype(jnp.float32).reshape(SEQUENCE_LENGTH, HV, DV)
    scaled = outputs * lax.rsqrt(lax.optimization_barrier(jnp.mean(outputs * outputs, -1, keepdims=True)) + EPSILON)
    gated = (scaled * norm_gain * jax.nn.silu(gating)).astype(jnp.bfloat16).reshape(SEQUENCE_LENGTH, HV * DV)
    summed = jnp.dot(gated, out_weight, preferred_element_type=jnp.float32)
    hidden_out = (residual.astype(jnp.float32) + summed).astype(jnp.bfloat16)
    widened = hidden_out.astype(jnp.float32)
    normalized = (widened * lax.rsqrt(lax.optimization_barrier(jnp.mean(widened * widened, -1, keepdims=True)) + EPSILON) * attn_gain).astype(jnp.bfloat16)
    projected = jnp.dot(normalized, query_weight, preferred_element_type=jnp.float32).reshape(SEQUENCE_LENGTH, QUERY_HEADS, 2, HEAD_WIDTH)
    queries_att = projected[:, :, 0].astype(jnp.bfloat16)
    gating_att = projected[:, :, 1]
    key_value_full = jnp.dot(normalized, key_value_weight, preferred_element_type=jnp.float32).reshape(SEQUENCE_LENGTH, 2, KEY_VALUE_HEADS, HEAD_WIDTH).astype(jnp.bfloat16)
    group_width = QUERY_HEADS // KEY_VALUE_HEADS
    key_heads = jnp.repeat(key_value_full[:, 0].transpose(1, 0, 2), group_width, 0)
    value_heads = jnp.repeat(key_value_full[:, 1].transpose(1, 0, 2), group_width, 0)
    visible = (positions[None, :] <= positions[:, None]) & (positions[None, :] < length_now)

    def attend_head(operands):
        head_query, head_key, head_value = operands
        scores = jnp.dot(head_query, head_key.T, preferred_element_type=jnp.float32) * HEAD_WIDTH ** (-0.5)
        scores = jnp.where(visible, scores, NEGATIVE)
        peak = lax.optimization_barrier(jnp.max(scores, -1, keepdims=True))
        weights = jnp.where(visible, jnp.exp(scores - peak), 0.0)
        denominator = lax.optimization_barrier(jnp.sum(weights, -1, keepdims=True))
        return jnp.dot(weights.astype(jnp.bfloat16), head_value, preferred_element_type=jnp.float32) / denominator
    attended = lax.map(attend_head, (queries_att.transpose(1, 0, 2), key_heads, value_heads))
    attention_out = (attended.transpose(1, 0, 2) * jax.nn.sigmoid(gating_att)).astype(jnp.bfloat16).reshape(SEQUENCE_LENGTH, QUERY_HEADS * HEAD_WIDTH)
    return (hidden_out, attention_out)
```

```python
import functools

import jax
import jax.numpy as jnp
from jax import lax
from jax.experimental import pallas as pl
from jax.experimental.pallas import tpu as pltpu
from jax.sharding import PartitionSpec as P

DK = 128
DV = 128
QUERY_HEADS = 16
KEY_VALUE_HEADS = 2
HEAD_WIDTH = 256
CONV = 4
PAD = 8
TAIL = 16
MATES = 2
EARLY = 3

EPSILON = 1e-06
NEGATIVE = -1e30
MESH = pl.DeviceIdType.MESH
HIGHEST = lax.Precision.HIGHEST


def exact(a, b, contract=((1,), (0,))):
    return lax.dot_general(
        a, b, (contract, ((), ())), precision=HIGHEST, preferred_element_type=jnp.float32
    )


def mm(a, b, contract=((1,), (0,))):
    return lax.dot_general(
        a.astype(jnp.bfloat16),
        b.astype(jnp.bfloat16),
        (contract, ((), ())),
        preferred_element_type=jnp.float32,
    )


def softplus(x):
    return jnp.maximum(x, 0.0) + jnp.log1p(jnp.exp(-jnp.abs(x)))


def unit(x):
    return x / jnp.sqrt(jnp.sum(x * x, -1, keepdims=True) + EPSILON)


def kernel(
    count,
    groups,
    heads,
    residual_in,
    q_in,
    k_in,
    v_in,
    gate_in,
    beta_in,
    decay_in,
    length_ref,
    cq_in,
    ck_in,
    cv_in,
    rate_in,
    gain_in,
    ow_in,
    again_in,
    qw_in,
    kvw_in,
    hidden_out,
    attention_out,
    q_ref,
    k_ref,
    v_ref,
    gate_ref,
    beta_ref,
    decay_ref,
    cq_ref,
    ck_ref,
    cv_ref,
    rate_ref,
    gain_ref,
    ow_ref,
    again_ref,
    residual_ref,
    wq,
    wkv,
    tail_q,
    tail_k,
    tail_v,
    joined,
    mapping,
    local,
    injected,
    enter,
    leave,
    gated,
    summed,
    partial,
    landed,
    hidden,
    normed,
    kvall,
    attended,
    load_sems,
    tail_send,
    tail_recv,
    state_send,
    state_recv,
    z_send,
    z_recv,
    y_send,
    y_recv,
    m_send,
    m_recv,
    my_send,
    my_recv,
    rs_send,
    rs_recv,
    ag_send,
    ag_recv,
    kv_send,
    kv_recv,
    km_send,
    km_recv,
):
    me = lax.axis_index("seq")
    part = lax.axis_index("groups")
    lane = lax.axis_index("head")
    core = lax.rem(lane, MATES)
    mate = lane + 1 - 2 * core
    rows = q_ref.shape[0]
    key_heads = q_ref.shape[1] // DK
    value_heads = v_ref.shape[1] // DV
    share = value_heads // key_heads
    query_heads = wq.shape[0]
    units = query_heads + 1
    depth = qw_in.shape[0]
    piece = depth // groups
    quarter = piece // MATES
    slab = rows // heads
    early = min(EARLY, units)
    kv_head = lane * query_heads // (QUERY_HEADS // KEY_VALUE_HEADS)

    loads = []

    def load(source, target):
        copy = pltpu.make_async_copy(source, target, load_sems.at[len(loads)])
        copy.start()
        loads.append(copy)
        return copy

    own_rows = pl.ds(pl.multiple_of(me * depth, depth), depth)
    load_kv = [
        load(
            kvw_in.at[
                :, pl.ds(pl.multiple_of((kind * KEY_VALUE_HEADS + kv_head) * HEAD_WIDTH, HEAD_WIDTH), HEAD_WIDTH)
            ],
            wkv.at[own_rows, pl.ds(kind * HEAD_WIDTH, HEAD_WIDTH)],
        )
        for kind in range(2)
    ]
    load_decay = [load(a, b) for a, b in ((decay_in, decay_ref), (rate_in, rate_ref), (beta_in, beta_ref))]
    load_conv = [
        load(a, b)
        for a, b in (
            (q_in, q_ref),
            (k_in, k_ref),
            (v_in, v_ref),
            (cq_in, cq_ref),
            (ck_in, ck_ref),
            (cv_in, cv_ref),
        )
    ]

    barrier = pltpu.get_barrier_semaphore()
    for axis, size, place in (("seq", count, me), ("groups", groups, part), ("head", heads, lane)):
        for e in range(1, size):
            pl.semaphore_signal(
                barrier, inc=1, device_id={axis: lax.rem(place + e, size)}, device_id_type=MESH
            )
    pl.semaphore_wait(barrier, count + groups + heads - 3)

    def inside(block):
        return (block >= 0) & (block < count)

    def clamp(block):
        return jnp.clip(block, 0, count - 1)

    def remote(source, target, send, recv, axis, index):
        return pltpu.make_async_remote_copy(
            src_ref=source,
            dst_ref=target,
            send_sem=send,
            recv_sem=recv,
            device_id={axis: index},
            device_id_type=MESH,
        )

    follower = clamp(me + 1)
    tails = [
        remote(
            source.at[pl.ds(rows - TAIL, TAIL)],
            target,
            tail_send.at[i],
            tail_recv.at[i],
            "seq",
            follower,
        )
        for i, (source, target) in enumerate(((q_in, tail_q), (k_in, tail_k), (v_in, tail_v)))
    ]

    @pl.when(me < count - 1)
    def _():
        for copy in tails:
            copy.start()

    def spot(block, which, half, u):
        if u == 0:
            first = block * depth + which * piece + half * quarter
            return wkv.at[pl.ds(pl.multiple_of(first, quarter), quarter)]
        first = block * depth + which * piece
        return wq.at[u - 1, pl.ds(pl.multiple_of(first, piece), piece)]

    def sign_of(d):
        return 1 if d == 0 else -1

    def along(d, j, u):
        sign = sign_of(d)
        block = clamp(me - sign * j)
        target = spot(block, part, core, u)
        source = target
        if j == 0 and u > 0:
            source = qw_in.at[
                pl.ds(pl.multiple_of(part * piece, piece), piece),
                pl.ds((u - 1) * 2 * HEAD_WIDTH, 2 * HEAD_WIDTH),
            ]
        copy = remote(
            source, target, z_send.at[d, j, u], z_recv.at[d, j, u], "seq", clamp(me + sign)
        )
        return copy, inside(me - sign * j) & inside(me + sign)

    def arriving(d, j, u):
        sign = sign_of(d)
        target = spot(clamp(me - sign * (j + 1)), part, core, u)
        copy = remote(
            target, target, z_send.at[d, j, u], z_recv.at[d, j, u], "seq", clamp(me + sign)
        )
        return copy, inside(me - sign * (j + 1))

    def across(e, d, j, u, which):
        target = spot(clamp(me - sign_of(d) * (j + 1)), which, core, u)
        return remote(
            target,
            target,
            y_send.at[e - 1, d, j, u],
            y_recv.at[e - 1, d, j, u],
            "groups",
            lax.rem(part + e, groups),
        )

    def beside(d, j, half):
        target = spot(clamp(me - sign_of(d) * (j + 1)), part, half, 0)
        return remote(target, target, m_send.at[d, j], m_recv.at[d, j], "head", mate)

    def source_of(e):
        return lax.rem(part + groups - e, groups)

    def beyond(e, d, j, half):
        target = spot(clamp(me - sign_of(d) * (j + 1)), source_of(e), half, 0)
        return remote(
            target, target, my_send.at[e - 1, d, j], my_recv.at[e - 1, d, j], "head", mate
        )

    def onward(d, j, u):
        if j + 1 < count - 1:
            copy, go = along(d, j + 1, u)
            pl.when(go)(copy.start)

    def relay(d, j, u, forward=True):
        copy, here = arriving(d, j, u)

        @pl.when(here)
        def _():
            copy.wait_recv()
            for e in range(1, groups):
                across(e, d, j, u, part).start()
            if u == 0:
                beside(d, j, core).start()

        if forward:
            onward(d, j, u)

    def share_kv(d, j):
        _, here = arriving(d, j, 0)

        @pl.when(here)
        def _():
            for e in range(1, groups):
                across(e, d, j, 0, source_of(e)).wait_recv()
                beyond(e, d, j, core).start()

    for copy in load_kv:
        copy.wait()
    for u in range(units):
        for d in range(2):
            if d == 1 or u < early:
                copy, go = along(d, 0, u)
                pl.when(go)(copy.start)

    load_late = [
        load(gate_in, gate_ref),
        load(gain_in, gain_ref),
        load(ow_in, ow_ref),
        load(residual_in.at[pl.ds(pl.multiple_of(lane * slab, slab), slab)], residual_ref),
        load(again_in, again_ref),
    ]
    load_q = [
        load(qw_in.at[:, pl.ds(i * 2 * HEAD_WIDTH, 2 * HEAD_WIDTH)], wq.at[i, own_rows])
        for i in range(query_heads)
    ]

    for b in range(1, count):

        @pl.when(b > me)
        def _():
            kvall[:, b * rows : (b + 1) * rows] = jnp.zeros((2, rows, HEAD_WIDTH), kvall.dtype)

    for copy in load_decay:
        copy.wait()
    length = length_ref[0]
    at_row = me * rows + lax.broadcasted_iota(jnp.int32, (rows, value_heads), 0)
    alive = (at_row < length).astype(jnp.float32)
    beta = jax.nn.sigmoid(beta_ref[...]) * alive
    step = -rate_ref[...] * softplus(decay_ref[...]) * alive
    row = lax.broadcasted_iota(jnp.int32, (rows, rows), 0)
    column = lax.broadcasted_iota(jnp.int32, (rows, rows), 1)
    inclusive = row >= column
    run = exact(inclusive.astype(jnp.float32), step)
    run_t = exact(step, (row <= column).astype(jnp.float32), ((0,), (0,)))
    growth = jnp.exp(run)
    ending_t = jnp.exp(run_t[:, rows - 1 : rows] - run_t)
    eye = (row == column).astype(jnp.float32)

    for copy in load_conv:
        copy.wait()
    q_width = key_heads * DK
    joined[PAD:, :q_width] = q_ref[...].astype(jnp.float32)
    joined[PAD:, q_width : 2 * q_width] = k_ref[...].astype(jnp.float32)
    joined[PAD:, 2 * q_width :] = v_ref[...].astype(jnp.float32)

    @pl.when(me == 0)
    def _():
        enter[...] = jnp.zeros_like(enter)
        joined[:PAD] = jnp.zeros((PAD, joined.shape[1]), jnp.float32)

    @pl.when(me > 0)
    def _():
        for copy in tails:
            copy.wait_recv()
        joined[:PAD, :q_width] = tail_q[...].astype(jnp.float32)[TAIL - PAD :]
        joined[:PAD, q_width : 2 * q_width] = tail_k[...].astype(jnp.float32)[TAIL - PAD :]
        joined[:PAD, 2 * q_width :] = tail_v[...].astype(jnp.float32)[TAIL - PAD :]

    def conv(base, taps, h):
        first_column = base + h * DK
        total = jnp.zeros((rows, DK), jnp.float32)
        for j in range(CONV):
            first = PAD - CONV + 1 + j
            total = total + taps[j : j + 1, h * DK : (h + 1) * DK] * joined[
                first : first + rows, first_column : first_column + DK
            ]
        return total * jax.nn.sigmoid(total)

    queries, keyset, turned, grams = [], [], [], []
    for g in range(key_heads):
        q = unit(conv(0, cq_ref, g)) * DK ** (-0.5)
        k = unit(conv(q_width, ck_ref, g))
        k_t = k.T
        queries.append(q)
        keyset.append(k)
        turned.append(k_t)
        grams.append(mm(jnp.concatenate([k, q], 0), k_t))

    for d in range(2):
        relay(d, 0, 0, forward=d == 1)

    mixes, lower, inverse = [], [], []
    for h in range(value_heads):
        spread = run[:, h : h + 1] - run_t[h : h + 1, :]
        w = jnp.exp(jnp.where(inclusive, spread, NEGATIVE))
        gram = grams[h // share]
        mixes.append((gram[rows:] * w).astype(jnp.bfloat16))
        low = jnp.where(row > column, beta[:, h : h + 1] * w * gram[:rows], 0.0)
        lower.append(low)
        pair = (row // 2 == column // 2) & (row > column)
        inverse.append(eye - jnp.where(pair, low, 0.0))
    size = 2
    while size < rows:
        off = (row // (2 * size) == column // (2 * size)) & (row // size > column // size)
        half = [mm(jnp.where(off, low, 0.0), x) for low, x in zip(lower, inverse)]
        inverse = [x - mm(x, y) for x, y in zip(inverse, half)]
        size *= 2
    if early > 1:
        for d in range(2):
            relay(d, 0, 1, forward=d == 1)

    for h in range(value_heads):
        k = keyset[h // share]
        v = conv(2 * q_width, cv_ref, h)
        b = beta[:, h : h + 1]
        grown = growth[:, h : h + 1]
        wu = mm(inverse[h], jnp.concatenate([b * grown * k, b * v], 1))
        stop_t = (turned[h // share] * ending_t[h : h + 1, :]).astype(jnp.bfloat16)
        both = mm(jnp.concatenate([stop_t, mixes[h]], 0), wu)
        mapping[h, :DK] = both[:DK, :DK].astype(jnp.bfloat16)
        mapping[h, DK:] = (grown * queries[h // share] - both[DK:, :DK]).astype(jnp.bfloat16)
        injected[h] = both[:DK, DK:]
        local[h] = both[DK:, DK:]
    if early > 2:
        for d in range(2):
            relay(d, 0, 2, forward=d == 1)

    for copy in load_late[:2]:
        copy.wait()
    states = []
    for h in range(value_heads):
        copy = remote(
            leave.at[h], enter.at[h], state_send.at[h], state_recv.at[h], "seq", follower
        )
        states.append(copy)

        @pl.when(me > 0)
        def _():
            copy.wait_recv()

        state = enter[h]
        moved = mm(mapping[h], state)
        total = growth[rows - 1 : rows, h : h + 1] * state.astype(jnp.float32)
        leave[h] = (total - moved[:DK] + injected[h]).astype(leave.dtype)
        o = local[h] + moved[DK:]
        scaled = o * lax.rsqrt(jnp.mean(o * o, -1, keepdims=True) + EPSILON) * gain_ref[...]
        gate = gate_ref[:, h * DV : (h + 1) * DV].astype(jnp.float32)
        gated[:, h * DV : (h + 1) * DV] = (scaled * (gate * jax.nn.sigmoid(gate))).astype(
            gated.dtype
        )

        @pl.when(me < count - 1)
        def _():
            copy.start()

    for u in range(early, units):
        copy, go = along(0, 0, u)
        pl.when(go)(copy.start)
    for u in range(early):
        onward(0, 0, u)

    for copy in load_late[2:]:
        copy.wait()
    width = ow_ref.shape[1]
    tile = min(512, width)
    for c in range(0, width, tile):
        product = jnp.dot(
            gated[...], ow_ref[:, c : c + tile], preferred_element_type=jnp.float32
        )
        summed[:, c : c + tile] = product
        partial[:, c : c + tile] = product.astype(partial.dtype)

    def slab_of(index):
        return pl.ds(pl.multiple_of(index * slab, slab), slab)

    scatter, gather = [], []
    for e in range(1, heads):
        peer = lax.rem(lane + e, heads)
        scatter.append(
            remote(
                partial.at[slab_of(peer)],
                landed.at[e - 1],
                rs_send.at[e - 1],
                rs_recv.at[e - 1],
                "head",
                peer,
            )
        )
        gather.append(
            remote(
                hidden.at[slab_of(lane)],
                hidden.at[slab_of(lane)],
                ag_send.at[e - 1],
                ag_recv.at[e - 1],
                "head",
                peer,
            )
        )
    for copy in scatter:
        copy.start()
    for u in range(early, units):
        for d in range(2):
            relay(d, 0, u)
    for d in range(2):
        share_kv(d, 0)
    for copy in scatter:
        copy.wait_recv()
    total = residual_ref[...].astype(jnp.float32) + (
        summed[slab_of(lane)] + sum(landed[e].astype(jnp.float32) for e in range(heads - 1))
    )
    hidden[slab_of(lane)] = total.astype(hidden.dtype)
    for copy in gather:
        copy.start()
    for j in range(1, count - 1):
        for d in range(2):
            relay(d, j, 0)
    for j in range(1, count - 1):
        for d in range(2):
            share_kv(d, j)
    for e in range(1, heads):
        peer = lax.rem(lane + heads - e, heads)
        remote(
            hidden.at[slab_of(peer)],
            hidden.at[slab_of(peer)],
            ag_send.at[e - 1],
            ag_recv.at[e - 1],
            "head",
            peer,
        ).wait_recv()
    save_hidden = load(hidden, hidden_out)
    widened = hidden[...].astype(jnp.float32)
    normed[...] = (
        widened
        * lax.rsqrt(jnp.mean(widened * widened, -1, keepdims=True) + EPSILON)
        * again_ref[...]
    ).astype(normed.dtype)

    for j in range(count - 1):
        for d in range(2):
            _, here = arriving(d, j, 0)

            @pl.when(here)
            def _():
                beside(d, j, 1 - core).wait_recv()
                for e in range(1, groups):
                    beyond(e, d, j, 1 - core).wait_recv()

    own_block = pl.ds(pl.multiple_of(me * rows, rows), rows)
    for kind in range(2):
        kvall[kind, own_block] = jnp.dot(
            normed[...],
            wkv[:, kind * HEAD_WIDTH : (kind + 1) * HEAD_WIDTH],
            preferred_element_type=jnp.float32,
        ).astype(kvall.dtype)

    def block_at(block):
        return pl.ds(pl.multiple_of(clamp(block) * rows, rows), rows)

    def later(e, block, axis, index, kind, send, recv):
        place = kvall.at[kind, block_at(block)]
        return remote(place, place, send.at[e - 1], recv.at[e - 1], axis, index)

    for e in range(1, count):

        @pl.when(me + e < count)
        def _():
            later(e, me, "seq", clamp(me + e), core, kv_send, kv_recv).start()

    for j in range(1, count - 1):
        for u in range(1, units):
            for d in range(2):
                if (j, u) < (count - 2, 1) or count == 2:
                    relay(d, j, u)

    for e in range(1, count):

        @pl.when(me >= e)
        def _():
            later(e, me - e, "seq", clamp(me - e), core, kv_send, kv_recv).wait_recv()
            later(e, me - e, "head", mate, core, km_send, km_recv).start()

    for e in range(1, count):

        @pl.when(me >= e)
        def _():
            later(e, me - e, "head", mate, 1 - core, km_send, km_recv).wait_recv()

    for copy in load_q:
        copy.wait()
    keys_total = count * rows
    at_query = me * rows + lax.broadcasted_iota(jnp.int32, (rows, keys_total), 0)
    at_key = lax.broadcasted_iota(jnp.int32, (rows, keys_total), 1)
    visible = (at_key <= at_query) & (at_key < length)
    for i in range(query_heads):
        if count > 2:
            for d in range(2):
                relay(d, count - 2, i + 1)
        for j in range(count - 1):
            for d in range(2):
                _, here = arriving(d, j, i + 1)

                @pl.when(here)
                def _():
                    for e in range(1, groups):
                        across(e, d, j, i + 1, source_of(e)).wait_recv()

        projected = jnp.dot(normed[...], wq[i], preferred_element_type=jnp.float32)
        scores = (
            lax.dot_general(
                projected[:, :HEAD_WIDTH].astype(jnp.bfloat16),
                kvall[0],
                (((1,), (1,)), ((), ())),
                preferred_element_type=jnp.float32,
            )
            * HEAD_WIDTH ** (-0.5)
        )
        scores = jnp.where(visible, scores, NEGATIVE)
        peak = jnp.max(scores, -1, keepdims=True)
        weights = jnp.where(visible, jnp.exp(scores - peak), 0.0)
        norm = jnp.sum(weights, -1, keepdims=True)
        mixed = jnp.dot(
            weights.astype(jnp.bfloat16), kvall[1], preferred_element_type=jnp.float32
        )
        attended[:, i * HEAD_WIDTH : (i + 1) * HEAD_WIDTH] = (
            mixed / norm * jax.nn.sigmoid(projected[:, HEAD_WIDTH:])
        ).astype(attended.dtype)
    save_attended = load(attended, attention_out)

    @pl.when(me < count - 1)
    def _():
        for copy in tails + states:
            copy.wait_send()

    for copy in scatter + gather:
        copy.wait_send()
    for j in range(count - 1):
        for d in range(2):
            for u in range(units):
                copy, go = along(d, j, u)
                pl.when(go)(copy.wait_send)
            _, here = arriving(d, j, 0)

            @pl.when(here)
            def _():
                for e in range(1, groups):
                    for u in range(units):
                        across(e, d, j, u, part).wait_send()
                    beyond(e, d, j, core).wait_send()
                beside(d, j, core).wait_send()

    for e in range(1, count):

        @pl.when(me + e < count)
        def _():
            later(e, me, "seq", clamp(me + e), core, kv_send, kv_recv).wait_send()

        @pl.when(me >= e)
        def _():
            later(e, me - e, "head", mate, core, km_send, km_recv).wait_send()

    save_hidden.wait()
    save_attended.wait()


def shards(
    residual,
    query_in,
    key_in,
    value_in,
    gating_in,
    beta_logit,
    decay_logit,
    seq_length,
    conv_query,
    conv_key,
    conv_value,
    decay_rate,
    norm_gain,
    out_weight,
    attn_gain,
    query_weight,
    key_value_weight,
):
    count = lax.axis_size("seq")
    groups = lax.axis_size("groups")
    heads = lax.axis_size("head")
    rows, model = residual.shape
    value_heads = beta_logit.shape[1]
    query_heads = query_weight.shape[1] // (2 * HEAD_WIDTH)
    units = query_heads + 1
    width = query_in.shape[1] + key_in.shape[1] + value_in.shape[1]
    depth = query_weight.shape[0] * count
    f32, bf16 = jnp.float32, jnp.bfloat16
    dma = pltpu.SemaphoreType.DMA
    anywhere = pl.BlockSpec(memory_space=pl.ANY)
    smem = pl.BlockSpec(memory_space=pltpu.SMEM)
    rate = decay_rate[None, :]
    gain = norm_gain[None, :]
    attn = attn_gain[None, :]
    like = lambda a: pltpu.VMEM(a.shape, a.dtype)
    return pl.pallas_call(
        functools.partial(kernel, count, groups, heads),
        out_shape=(
            jax.ShapeDtypeStruct(residual.shape, bf16),
            jax.ShapeDtypeStruct((rows, query_heads * HEAD_WIDTH), bf16),
        ),
        in_specs=[anywhere] * 7 + [smem] + [anywhere] * 9,
        out_specs=(anywhere, anywhere),
        scratch_shapes=[
            like(query_in),
            like(key_in),
            like(value_in),
            like(gating_in),
            like(beta_logit),
            like(decay_logit),
            like(conv_query),
            like(conv_key),
            like(conv_value),
            like(rate),
            like(gain),
            like(out_weight),
            like(attn),
            pltpu.VMEM((rows // heads, model), bf16),
            pltpu.VMEM((query_heads, depth, 2 * HEAD_WIDTH), bf16),
            pltpu.VMEM((depth, 2 * HEAD_WIDTH), bf16),
            pltpu.VMEM((TAIL, query_in.shape[1]), bf16),
            pltpu.VMEM((TAIL, key_in.shape[1]), bf16),
            pltpu.VMEM((TAIL, value_in.shape[1]), bf16),
            pltpu.VMEM((rows + PAD, width), f32),
            pltpu.VMEM((value_heads, DK + rows, DK), bf16),
            pltpu.VMEM((value_heads, rows, DV), f32),
            pltpu.VMEM((value_heads, DK, DV), f32),
            pltpu.VMEM((value_heads, DK, DV), bf16),
            pltpu.VMEM((value_heads, DK, DV), bf16),
            pltpu.VMEM((rows, value_heads * DV), bf16),
            pltpu.VMEM((rows, model), f32),
            pltpu.VMEM((rows, model), bf16),
            pltpu.VMEM((heads - 1, rows // heads, model), bf16),
            pltpu.VMEM((rows, model), bf16),
            pltpu.VMEM((rows, model), bf16),
            pltpu.VMEM((2, count * rows, HEAD_WIDTH), bf16),
            pltpu.VMEM((rows, query_heads * HEAD_WIDTH), bf16),
            dma((24 + query_heads,)),
            dma((3,)),
            dma((3,)),
            dma((value_heads,)),
            dma((value_heads,)),
            dma((2, count - 1, units)),
            dma((2, count - 1, units)),
            dma((groups - 1, 2, count - 1, units)),
            dma((groups - 1, 2, count - 1, units)),
            dma((2, count - 1)),
            dma((2, count - 1)),
            dma((groups - 1, 2, count - 1)),
            dma((groups - 1, 2, count - 1)),
            dma((heads - 1,)),
            dma((heads - 1,)),
            dma((heads - 1,)),
            dma((heads - 1,)),
            dma((count - 1,)),
            dma((count - 1,)),
            dma((count - 1,)),
            dma((count - 1,)),
        ],
        compiler_params=pltpu.CompilerParams(
            collective_id=0, has_side_effects=True, vmem_limit_bytes=56 * 2**20
        ),
        name="layer",
    )(
        residual,
        query_in,
        key_in,
        value_in,
        gating_in,
        beta_logit,
        decay_logit,
        seq_length,
        conv_query,
        conv_key,
        conv_value,
        rate,
        gain,
        out_weight,
        attn,
        query_weight,
        key_value_weight,
    )


def solution(mesh):
    placed = (
        P(("groups", "seq"), None),
        P(("groups", "seq"), "head"),
        P(("groups", "seq"), "head"),
        P(("groups", "seq"), "head"),
        P(("groups", "seq"), "head"),
        P(("groups", "seq"), "head"),
        P(("groups", "seq"), "head"),
        P("groups"),
        P(None, "head"),
        P(None, "head"),
        P(None, "head"),
        P("head"),
        P(),
        P("head", None),
        P(),
        P("seq", "head"),
        P("seq", None),
    )
    return jax.shard_map(
        shards,
        mesh=mesh,
        in_specs=placed,
        out_specs=(P(("groups", "seq"), None), P(("groups", "seq"), "head")),
        check_vma=False,
    )
```

```python
import functools

import jax
import jax.numpy as jnp
from jax import lax
from jax.experimental import pallas as pl
from jax.experimental.pallas import tpu as pltpu
from jax.sharding import PartitionSpec as P

DK = 128
DV = 128
QUERY_HEADS = 16
KEY_VALUE_HEADS = 2
HEAD_WIDTH = 256
CONV = 4
PAD = 8
TAIL = 16
MATES = 2
EARLY = 3

EPSILON = 1e-06
NEGATIVE = -1e30
MESH = pl.DeviceIdType.MESH
HIGHEST = lax.Precision.HIGHEST


def exact(a, b, contract=((1,), (0,))):
    return lax.dot_general(
        a, b, (contract, ((), ())), precision=HIGHEST, preferred_element_type=jnp.float32
    )


def mm(a, b, contract=((1,), (0,))):
    return lax.dot_general(
        a.astype(jnp.bfloat16),
        b.astype(jnp.bfloat16),
        (contract, ((), ())),
        preferred_element_type=jnp.float32,
    )


def softplus(x):
    return jnp.maximum(x, 0.0) + jnp.log1p(jnp.exp(-jnp.abs(x)))


def unit(x):
    return x / jnp.sqrt(jnp.sum(x * x, -1, keepdims=True) + EPSILON)


INPUTS = [
    "residual_in",
    "q_in",
    "k_in",
    "v_in",
    "gate_in",
    "beta_in",
    "decay_in",
    "length_ref",
    "cq_in",
    "ck_in",
    "cv_in",
    "rate_in",
    "gain_in",
    "ow_in",
    "again_in",
    "qw_in",
    "kvw_in",
]
OUTPUTS = ["hidden_out", "attention_out"]


def remote(source, target, send, recv, axis, index):
    return pltpu.make_async_remote_copy(
        src_ref=source,
        dst_ref=target,
        send_sem=send,
        recv_sem=recv,
        device_id={axis: index},
        device_id_type=MESH,
    )


def sign_of(d):
    return 1 if d == 0 else -1


class Layer:
    def __init__(self, sizes, names, refs):
        self.count, self.groups, self.heads = sizes
        for name, ref in zip(names, refs, strict=True):
            setattr(self, name, ref)
        self.me = lax.axis_index("seq")
        self.part = lax.axis_index("groups")
        self.lane = lax.axis_index("head")
        self.core = lax.rem(self.lane, MATES)
        self.mate = self.lane + 1 - 2 * self.core
        self.rows = self.q_ref.shape[0]
        self.key_heads = self.q_ref.shape[1] // DK
        self.value_heads = self.v_ref.shape[1] // DV
        self.share = self.value_heads // self.key_heads
        self.depth = self.qw_in.shape[0]
        self.piece = self.depth // self.groups
        self.quarter = self.piece // MATES
        self.slab = self.rows // self.heads
        self.query_heads = self.qw_in.shape[1] // (2 * HEAD_WIDTH)
        self.kv_head = self.lane * self.query_heads // (QUERY_HEADS // KEY_VALUE_HEADS)
        self.own_rows = pl.ds(pl.multiple_of(self.me * self.depth, self.depth), self.depth)
        self.follower = self.clamp(self.me + 1)
        self.loads = 0

    def load(self, source, target):
        copy = pltpu.make_async_copy(source, target, self.load_sems.at[self.loads])
        copy.start()
        self.loads += 1
        return copy

    def inside(self, block):
        return (block >= 0) & (block < self.count)

    def clamp(self, block):
        return jnp.clip(block, 0, self.count - 1)

    def slab_of(self, index):
        return pl.ds(pl.multiple_of(index * self.slab, self.slab), self.slab)


    def kv_spot(self, block, which, half):
        first = block * self.depth + which * self.piece + half * self.quarter
        return self.wkv.at[pl.ds(pl.multiple_of(first, self.quarter), self.quarter)]

    def begin(self):
        load = self.load
        self.load_kv = [
            load(
                self.kvw_in.at[
                    :,
                    pl.ds(
                        pl.multiple_of(
                            (kind * KEY_VALUE_HEADS + self.kv_head) * HEAD_WIDTH, HEAD_WIDTH
                        ),
                        HEAD_WIDTH,
                    ),
                ],
                self.wkv.at[self.own_rows, pl.ds(kind * HEAD_WIDTH, HEAD_WIDTH)],
            )
            for kind in range(2)
        ]
        self.load_decay = [
            load(self.decay_in, self.decay_ref),
            load(self.rate_in, self.rate_ref),
            load(self.beta_in, self.beta_ref),
        ]
        self.load_conv = [
            load(self.q_in, self.q_ref),
            load(self.k_in, self.k_ref),
            load(self.v_in, self.v_ref),
            load(self.cq_in, self.cq_ref),
            load(self.ck_in, self.ck_ref),
            load(self.cv_in, self.cv_ref),
        ]

        barrier = pltpu.get_barrier_semaphore()
        for axis, size, place in (
            ("seq", self.count, self.me),
            ("groups", self.groups, self.part),
            ("head", self.heads, self.lane),
        ):
            for e in range(1, size):
                pl.semaphore_signal(
                    barrier,
                    inc=1,
                    device_id={axis: lax.rem(place + e, size)},
                    device_id_type=MESH,
                )
        pl.semaphore_wait(barrier, self.count + self.groups + self.heads - 3)

        last = pl.ds(self.rows - TAIL, TAIL)
        self.tails = [
            remote(
                source.at[last],
                target,
                self.tail_send.at[i],
                self.tail_recv.at[i],
                "seq",
                self.follower,
            )
            for i, (source, target) in enumerate(
                (
                    (self.q_in, self.tail_q),
                    (self.k_in, self.tail_k),
                    (self.v_in, self.tail_v),
                )
            )
        ]

        @pl.when(self.me < self.count - 1)
        def _():
            for copy in self.tails:
                copy.start()

    def load_rest(self):
        load = self.load
        self.load_late = [
            load(self.gate_in, self.gate_ref),
            load(self.gain_in, self.gain_ref),
            load(self.ow_in, self.ow_ref),
            load(self.residual_in.at[self.slab_of(self.lane)], self.residual_ref),
            load(self.again_in, self.again_ref),
        ]

    def delta(self, pumps):
        rows, value_heads, share = self.rows, self.value_heads, self.share
        key_heads = self.key_heads
        for copy in self.load_decay:
            copy.wait()
        length = self.length_ref[0]
        at_row = self.me * rows + lax.broadcasted_iota(jnp.int32, (rows, value_heads), 0)
        alive = (at_row < length).astype(jnp.float32)
        beta = jax.nn.sigmoid(self.beta_ref[...]) * alive
        step = -self.rate_ref[...] * softplus(self.decay_ref[...]) * alive
        row = lax.broadcasted_iota(jnp.int32, (rows, rows), 0)
        column = lax.broadcasted_iota(jnp.int32, (rows, rows), 1)
        inclusive = row >= column
        run = exact(inclusive.astype(jnp.float32), step)
        run_t = exact(step, (row <= column).astype(jnp.float32), ((0,), (0,)))
        growth = jnp.exp(run)
        self.final = growth[rows - 1 : rows]
        ending_t = jnp.exp(run_t[:, rows - 1 : rows] - run_t)
        eye = (row == column).astype(jnp.float32)

        for copy in self.load_conv:
            copy.wait()
        q_width = key_heads * DK
        joined = self.joined
        joined[PAD:, :q_width] = self.q_ref[...].astype(jnp.float32)
        joined[PAD:, q_width : 2 * q_width] = self.k_ref[...].astype(jnp.float32)
        joined[PAD:, 2 * q_width :] = self.v_ref[...].astype(jnp.float32)

        @pl.when(self.me == 0)
        def _():
            self.enter[...] = jnp.zeros_like(self.enter)
            joined[:PAD] = jnp.zeros((PAD, joined.shape[1]), jnp.float32)

        @pl.when(self.me > 0)
        def _():
            for copy in self.tails:
                copy.wait_recv()
            joined[:PAD, :q_width] = self.tail_q[...].astype(jnp.float32)[TAIL - PAD :]
            joined[:PAD, q_width : 2 * q_width] = self.tail_k[...].astype(jnp.float32)[
                TAIL - PAD :
            ]
            joined[:PAD, 2 * q_width :] = self.tail_v[...].astype(jnp.float32)[TAIL - PAD :]

        def conv(base, taps, h):
            first_column = base + h * DK
            total = jnp.zeros((rows, DK), jnp.float32)
            for j in range(CONV):
                first = PAD - CONV + 1 + j
                total = total + taps[j : j + 1, h * DK : (h + 1) * DK] * joined[
                    first : first + rows, first_column : first_column + DK
                ]
            return total * jax.nn.sigmoid(total)

        queries, keyset, turned, grams = [], [], [], []
        for g in range(key_heads):
            q = unit(conv(0, self.cq_ref, g)) * DK ** (-0.5)
            k = unit(conv(q_width, self.ck_ref, g))
            k_t = k.T
            queries.append(q)
            keyset.append(k)
            turned.append(k_t)
            grams.append(mm(jnp.concatenate([k, q], 0), k_t))
        pumps[0]()

        mixes, lower, inverse = [], [], []
        for h in range(value_heads):
            spread = run[:, h : h + 1] - run_t[h : h + 1, :]
            w = jnp.exp(jnp.where(inclusive, spread, NEGATIVE))
            gram = grams[h // share]
            mixes.append((gram[rows:] * w).astype(jnp.bfloat16))
            low = jnp.where(row > column, beta[:, h : h + 1] * w * gram[:rows], 0.0)
            lower.append(low)
            pair = (row // 2 == column // 2) & (row > column)
            inverse.append(eye - jnp.where(pair, low, 0.0))
        size = 2
        while size < rows:
            off = (row // (2 * size) == column // (2 * size)) & (row // size > column // size)
            half = [mm(jnp.where(off, low, 0.0), x) for low, x in zip(lower, inverse)]
            inverse = [x - mm(x, y) for x, y in zip(inverse, half)]
            size *= 2
        pumps[1]()

        for h in range(value_heads):
            k = keyset[h // share]
            v = conv(2 * q_width, self.cv_ref, h)
            b = beta[:, h : h + 1]
            grown = growth[:, h : h + 1]
            wu = mm(inverse[h], jnp.concatenate([b * grown * k, b * v], 1))
            stop_t = (turned[h // share] * ending_t[h : h + 1, :]).astype(jnp.bfloat16)
            both = mm(jnp.concatenate([stop_t, mixes[h]], 0), wu)
            self.mapping[h, :DK] = both[:DK, :DK].astype(jnp.bfloat16)
            self.mapping[h, DK:] = (grown * queries[h // share] - both[DK:, :DK]).astype(
                jnp.bfloat16
            )
            self.injected[h] = both[:DK, DK:]
            self.local[h] = both[DK:, DK:]
        pumps[2]()

        for copy in self.load_late[:2]:
            copy.wait()
        self.states = []
        for h in range(value_heads):
            copy = remote(
                self.leave.at[h],
                self.enter.at[h],
                self.state_send.at[h],
                self.state_recv.at[h],
                "seq",
                self.follower,
            )
            self.states.append(copy)

            @pl.when(self.me > 0)
            def _():
                copy.wait_recv()

            state = self.enter[h]
            moved = mm(self.mapping[h], state)
            total = self.final[:, h : h + 1] * state.astype(jnp.float32)
            self.leave[h] = (total - moved[:DK] + self.injected[h]).astype(self.leave.dtype)
            o = self.local[h] + moved[DK:]
            scaled = (
                o * lax.rsqrt(jnp.mean(o * o, -1, keepdims=True) + EPSILON) * self.gain_ref[...]
            )
            gate = self.gate_ref[:, h * DV : (h + 1) * DV].astype(jnp.float32)
            self.gated[:, h * DV : (h + 1) * DV] = (
                scaled * (gate * jax.nn.sigmoid(gate))
            ).astype(self.gated.dtype)

            @pl.when(self.me < self.count - 1)
            def _():
                copy.start()

    def project_out(self):
        for copy in self.load_late[2:]:
            copy.wait()
        width = self.ow_ref.shape[1]
        tile = min(512, width)
        for c in range(0, width, tile):
            product = jnp.dot(
                self.gated[...],
                self.ow_ref[:, c : c + tile],
                preferred_element_type=jnp.float32,
            )
            self.summed[:, c : c + tile] = product
            self.partial[:, c : c + tile] = product.astype(self.partial.dtype)
        self.scatter = []
        for e in range(1, self.heads):
            peer = lax.rem(self.lane + e, self.heads)
            self.scatter.append(
                remote(
                    self.partial.at[self.slab_of(peer)],
                    self.landed.at[e - 1],
                    self.rs_send.at[e - 1],
                    self.rs_recv.at[e - 1],
                    "head",
                    peer,
                )
            )
        for copy in self.scatter:
            copy.start()

    def hidden_slab(self):
        for copy in self.scatter:
            copy.wait_recv()
        return self.residual_ref[...].astype(jnp.float32) + (
            self.summed[self.slab_of(self.lane)]
            + sum(self.landed[e].astype(jnp.float32) for e in range(self.heads - 1))
        )

    def gather_hidden(self, e, index):
        place = self.hidden.at[self.slab_of(index)]
        peer = lax.rem(self.lane + e, self.heads)
        return remote(
            place, place, self.ag_send.at[e - 1], self.ag_recv.at[e - 1], "head", peer
        )

    def send_hidden(self):
        for e in range(1, self.heads):
            self.gather_hidden(e, self.lane).start()

    def wait_hidden(self):
        for e in range(1, self.heads):
            self.gather_hidden(e, lax.rem(self.lane + self.heads - e, self.heads)).wait_recv()

    def scaled(self, hidden):
        widened = hidden.astype(jnp.float32)
        mean = jnp.mean(widened * widened, -1, keepdims=True)
        return (widened * lax.rsqrt(mean + EPSILON) * self.again_ref[...]).astype(jnp.bfloat16)

    def end(self):
        @pl.when(self.me < self.count - 1)
        def _():
            for copy in self.tails + self.states:
                copy.wait_send()

        for copy in self.scatter:
            copy.wait_send()
        for e in range(1, self.heads):
            self.gather_hidden(e, self.lane).wait_send()

    def attend(self, queries, keys, values, visible):
        scores = (
            lax.dot_general(
                queries, keys, (((1,), (1,)), ((), ())), preferred_element_type=jnp.float32
            )
            * HEAD_WIDTH ** (-0.5)
        )
        scores = jnp.where(visible, scores, NEGATIVE)
        peak = jnp.max(scores, -1, keepdims=True)
        weights = jnp.where(visible, jnp.exp(scores - peak), 0.0)
        norm = jnp.sum(weights, -1, keepdims=True)
        mixed = jnp.dot(weights.astype(jnp.bfloat16), values, preferred_element_type=jnp.float32)
        return mixed / norm


class Ring(Layer):
    def spot(self, block, which, half, u):
        if u == 0:
            return self.kv_spot(block, which, half)
        first = block * self.depth + which * self.piece
        return self.wq.at[u - 1, pl.ds(pl.multiple_of(first, self.piece), self.piece)]

    def along(self, d, j, u):
        sign = sign_of(d)
        block = self.clamp(self.me - sign * j)
        target = self.spot(block, self.part, self.core, u)
        source = target
        if j == 0 and u > 0:
            source = self.qw_in.at[
                pl.ds(pl.multiple_of(self.part * self.piece, self.piece), self.piece),
                pl.ds((u - 1) * 2 * HEAD_WIDTH, 2 * HEAD_WIDTH),
            ]
        copy = remote(
            source,
            target,
            self.z_send.at[d, j, u],
            self.z_recv.at[d, j, u],
            "seq",
            self.clamp(self.me + sign),
        )
        return copy, self.inside(self.me - sign * j) & self.inside(self.me + sign)

    def arriving(self, d, j, u):
        sign = sign_of(d)
        target = self.spot(self.clamp(self.me - sign * (j + 1)), self.part, self.core, u)
        copy = remote(
            target,
            target,
            self.z_send.at[d, j, u],
            self.z_recv.at[d, j, u],
            "seq",
            self.clamp(self.me + sign),
        )
        return copy, self.inside(self.me - sign * (j + 1))

    def across(self, e, d, j, u, which):
        target = self.spot(self.clamp(self.me - sign_of(d) * (j + 1)), which, self.core, u)
        return remote(
            target,
            target,
            self.y_send.at[e - 1, d, j, u],
            self.y_recv.at[e - 1, d, j, u],
            "groups",
            lax.rem(self.part + e, self.groups),
        )

    def beside(self, d, j, half):
        target = self.kv_spot(self.clamp(self.me - sign_of(d) * (j + 1)), self.part, half)
        return remote(target, target, self.m_send.at[d, j], self.m_recv.at[d, j], "head", self.mate)

    def source_of(self, e):
        return lax.rem(self.part + self.groups - e, self.groups)

    def beyond(self, e, d, j, half):
        target = self.kv_spot(self.clamp(self.me - sign_of(d) * (j + 1)), self.source_of(e), half)
        return remote(
            target,
            target,
            self.my_send.at[e - 1, d, j],
            self.my_recv.at[e - 1, d, j],
            "head",
            self.mate,
        )

    def onward(self, d, j, u):
        if j + 1 < self.count - 1:
            copy, go = self.along(d, j + 1, u)
            pl.when(go)(copy.start)

    def relay(self, d, j, u, forward=True):
        copy, here = self.arriving(d, j, u)

        @pl.when(here)
        def _():
            copy.wait_recv()
            for e in range(1, self.groups):
                self.across(e, d, j, u, self.part).start()
            if u == 0:
                self.beside(d, j, self.core).start()

        if forward:
            self.onward(d, j, u)

    def share_kv(self, d, j):
        _, here = self.arriving(d, j, 0)

        @pl.when(here)
        def _():
            for e in range(1, self.groups):
                self.across(e, d, j, 0, self.source_of(e)).wait_recv()
                self.beyond(e, d, j, self.core).start()

    def wait_kv(self, d, j):
        _, here = self.arriving(d, j, 0)

        @pl.when(here)
        def _():
            self.beside(d, j, 1 - self.core).wait_recv()
            for e in range(1, self.groups):
                self.beyond(e, d, j, 1 - self.core).wait_recv()

    def end_weights(self, units):
        for j in range(self.count - 1):
            for d in range(2):
                for u in range(units):
                    copy, go = self.along(d, j, u)
                    pl.when(go)(copy.wait_send)
                _, here = self.arriving(d, j, 0)

                @pl.when(here)
                def _():
                    for e in range(1, self.groups):
                        for u in range(units):
                            self.across(e, d, j, u, self.part).wait_send()
                        self.beyond(e, d, j, self.core).wait_send()
                    self.beside(d, j, self.core).wait_send()


def ring_kernel(sizes, names, *refs):
    s = Ring(sizes, names, refs)
    count, groups, me, rows = s.count, s.groups, s.me, s.rows
    units = s.query_heads + 1
    early = min(EARLY, units)
    s.begin()
    for copy in s.load_kv:
        copy.wait()
    for u in range(units):
        for d in range(2):
            if d == 1 or u < early:
                copy, go = s.along(d, 0, u)
                pl.when(go)(copy.start)
    s.load_rest()
    load_q = [
        s.load(
            s.qw_in.at[:, pl.ds(i * 2 * HEAD_WIDTH, 2 * HEAD_WIDTH)], s.wq.at[i, s.own_rows]
        )
        for i in range(s.query_heads)
    ]

    for b in range(1, count):

        @pl.when(b > me)
        def _():
            s.kvall[:, b * rows : (b + 1) * rows] = jnp.zeros(
                (2, rows, HEAD_WIDTH), s.kvall.dtype
            )

    def pump(u):
        def run():
            if u < early:
                for d in range(2):
                    s.relay(d, 0, u, forward=d == 1)

        return run

    s.delta([pump(u) for u in range(3)])
    for u in range(early, units):
        copy, go = s.along(0, 0, u)
        pl.when(go)(copy.start)
    for u in range(early):
        s.onward(0, 0, u)
    s.project_out()
    for u in range(early, units):
        for d in range(2):
            s.relay(d, 0, u)
    for d in range(2):
        s.share_kv(d, 0)
    s.hidden[s.slab_of(s.lane)] = s.hidden_slab().astype(s.hidden.dtype)
    s.send_hidden()
    for j in range(1, count - 1):
        for d in range(2):
            s.relay(d, j, 0)
    for j in range(1, count - 1):
        for d in range(2):
            s.share_kv(d, j)
    s.wait_hidden()
    save_hidden = s.load(s.hidden, s.hidden_out)
    s.normed[...] = s.scaled(s.hidden[...])

    for j in range(count - 1):
        for d in range(2):
            s.wait_kv(d, j)
    own_block = pl.ds(pl.multiple_of(me * rows, rows), rows)
    for kind in range(2):
        s.kvall[kind, own_block] = jnp.dot(
            s.normed[...],
            s.wkv[:, kind * HEAD_WIDTH : (kind + 1) * HEAD_WIDTH],
            preferred_element_type=jnp.float32,
        ).astype(s.kvall.dtype)

    def later(e, block, axis, index, kind, send, recv):
        place = s.kvall.at[kind, pl.ds(pl.multiple_of(s.clamp(block) * rows, rows), rows)]
        return remote(place, place, send.at[e - 1], recv.at[e - 1], axis, index)

    def sent_kv(e):
        return later(e, me, "seq", s.clamp(me + e), s.core, s.kv_send, s.kv_recv)

    def mate_kv(e, kind):
        return later(e, me - e, "head", s.mate, kind, s.km_send, s.km_recv)

    for e in range(1, count):
        pl.when(me + e < count)(sent_kv(e).start)

    for j in range(1, count - 1):
        for u in range(1, units):
            for d in range(2):
                if (j, u) < (count - 2, 1) or count == 2:
                    s.relay(d, j, u)

    for e in range(1, count):

        @pl.when(me >= e)
        def _():
            later(e, me - e, "seq", s.clamp(me - e), s.core, s.kv_send, s.kv_recv).wait_recv()
            mate_kv(e, s.core).start()

    for e in range(1, count):
        pl.when(me >= e)(mate_kv(e, 1 - s.core).wait_recv)

    for copy in load_q:
        copy.wait()
    keys_total = count * rows
    at_query = me * rows + lax.broadcasted_iota(jnp.int32, (rows, keys_total), 0)
    at_key = lax.broadcasted_iota(jnp.int32, (rows, keys_total), 1)
    visible = (at_key <= at_query) & (at_key < s.length_ref[0])
    for i in range(s.query_heads):
        if count > 2:
            for d in range(2):
                s.relay(d, count - 2, i + 1)
        for j in range(count - 1):
            for d in range(2):
                _, here = s.arriving(d, j, i + 1)

                @pl.when(here)
                def _():
                    for e in range(1, groups):
                        s.across(e, d, j, i + 1, s.source_of(e)).wait_recv()

        projected = jnp.dot(s.normed[...], s.wq[i], preferred_element_type=jnp.float32)
        mixed = s.attend(
            projected[:, :HEAD_WIDTH].astype(jnp.bfloat16), s.kvall[0], s.kvall[1], visible
        )
        s.attended[:, i * HEAD_WIDTH : (i + 1) * HEAD_WIDTH] = (
            mixed * jax.nn.sigmoid(projected[:, HEAD_WIDTH:])
        ).astype(s.attended.dtype)
    save_attended = s.load(s.attended, s.attention_out)

    s.end()
    s.end_weights(units)
    for e in range(1, count):
        pl.when(me + e < count)(sent_kv(e).wait_send)
        pl.when(me >= e)(mate_kv(e, s.core).wait_send)
    save_hidden.wait()
    save_attended.wait()


class Split(Ring):
    def weights(self, d, dist):
        sign = sign_of(d)
        peer = self.me + sign * dist
        wide = self.wq.shape[1]
        first = pl.multiple_of(self.part * self.piece, self.piece)
        target = pl.multiple_of(self.me * self.depth + self.part * self.piece, self.piece)
        copy = remote(
            self.qw_in.at[
                pl.ds(first, self.piece),
                pl.ds(pl.multiple_of(self.clamp(peer) * wide, wide), wide),
            ],
            self.wq.at[pl.ds(target, self.piece)],
            self.w_send.at[d, dist - 1],
            self.w_recv.at[d, dist - 1],
            "seq",
            self.clamp(peer),
        )
        return copy, self.inside(peer)

    def weights_across(self, e, d, dist, which):
        block = self.clamp(self.me - sign_of(d) * dist)
        first = pl.multiple_of(block * self.depth + which * self.piece, self.piece)
        place = self.wq.at[pl.ds(first, self.piece)]
        return remote(
            place,
            place,
            self.wy_send.at[e - 1, d, dist - 1],
            self.wy_recv.at[e - 1, d, dist - 1],
            "groups",
            lax.rem(self.part + e, self.groups),
        )

    def weights_relay(self, d, dist):
        block = self.me - sign_of(d) * dist
        first = self.clamp(block) * self.depth + self.part * self.piece
        place = self.wq.at[pl.ds(pl.multiple_of(first, self.piece), self.piece)]

        @pl.when(self.inside(block))
        def _():
            remote(
                place,
                place,
                self.w_send.at[d, dist - 1],
                self.w_recv.at[d, dist - 1],
                "seq",
                self.clamp(block),
            ).wait_recv()
            for e in range(1, self.groups):
                self.weights_across(e, d, dist, self.part).start()

    def weights_wait(self, d, dist):
        @pl.when(self.inside(self.me - sign_of(d) * dist))
        def _():
            for e in range(1, self.groups):
                self.weights_across(e, d, dist, self.source_of(e)).wait_recv()


    def place(self, block, index):
        first = block * self.rows + index * self.slab
        return self.every.at[pl.ds(pl.multiple_of(first, self.slab), self.slab)]

    def far(self, d, dist, block, index):
        place = self.place(self.clamp(block), self.lane)
        return remote(
            place,
            place,
            self.n_send.at[d, dist - 1],
            self.n_recv.at[d, dist - 1],
            "seq",
            self.clamp(index),
        )

    def near(self, d, dist, f, block, index):
        place = self.place(self.clamp(block), index)
        peer = lax.rem(self.lane + MATES * f, self.heads)
        return remote(
            place,
            place,
            self.x_send.at[d, dist, f - 1],
            self.x_recv.at[d, dist, f - 1],
            "head",
            peer,
        )

    def twin(self, d, dist, f, block, index):
        place = self.place(self.clamp(block), index)
        return remote(
            place, place, self.t_send.at[d, dist, f], self.t_recv.at[d, dist, f], "head", self.mate
        )

    def back(self, f, lane):
        return lax.rem(lane + self.heads - MATES * f, self.heads)

    def chips(self):
        return range(1, self.heads // MATES)

    def block_at(self, d, dist):
        return self.me - sign_of(d) * dist

    def steps(self, dist):
        return (0,) if dist == 0 else (0, 1)

    def rows_sent(self, dist):
        for d in self.steps(dist):
            block = self.block_at(d, dist)

            @pl.when(self.inside(block))
            def _():
                if dist > 0:
                    self.far(d, dist, block, block).wait_recv()
                for f in self.chips():
                    self.near(d, dist, f, block, self.lane).start()
                self.twin(d, dist, 0, block, self.lane).start()

    def rows_passed(self, dist):
        for d in self.steps(dist):
            block = self.block_at(d, dist)

            @pl.when(self.inside(block))
            def _():
                for f in self.chips():
                    self.near(d, dist, f, block, self.back(f, self.lane)).wait_recv()
                    self.twin(d, dist, f, block, self.back(f, self.lane)).start()

    def rows_ready(self, d, dist, block):
        for f in range(self.heads // MATES):
            self.twin(d, dist, f, block, self.back(f, self.mate)).wait_recv()

    def end_rows(self):
        for dist in range(self.count):
            for d in self.steps(dist):
                block = self.block_at(d, dist)
                if dist > 0:
                    peer = self.me + sign_of(d) * dist
                    pl.when(self.inside(peer))(self.far(d, dist, self.me, peer).wait_send)

                @pl.when(self.inside(block))
                def _():
                    for f in self.chips():
                        self.near(d, dist, f, block, self.lane).wait_send()
                    for f in range(self.heads // MATES):
                        self.twin(d, dist, f, block, self.back(f, self.lane)).wait_send()


def split_kernel(sizes, names, *refs):
    s = Split(sizes, names, refs)
    count, groups, me, rows = s.count, s.groups, s.me, s.rows
    wide = s.wq.shape[1]
    mine = wide // (2 * HEAD_WIDTH)
    s.begin()
    for copy in s.load_kv:
        copy.wait()
    for d in range(2):
        copy, go = s.along(d, 0, 0)
        pl.when(go)(copy.start)
    for dist in range(count - 1, 0, -1):
        for d in range(2):
            if d == 1 or dist > 1:
                copy, go = s.weights(d, dist)
                pl.when(go)(copy.start)
    s.load_rest()
    load_q = s.load(
        s.qw_in.at[:, pl.ds(pl.multiple_of(me * wide, wide), wide)], s.wq.at[s.own_rows]
    )

    def pump_first():
        for d in range(2):
            s.relay(d, 0, 0)

    def pump_second():
        for j in range(1, count - 1):
            for d in range(2):
                s.relay(d, j, 0)
        for d in range(2):
            s.share_kv(d, 0)

    def pump_third():
        s.weights_relay(1, 1)

    s.delta([pump_first, pump_second, pump_third])
    copy, go = s.weights(0, 1)
    pl.when(go)(copy.start)
    s.project_out()
    for j in range(1, count - 1):
        for d in range(2):
            s.share_kv(d, j)
    for dist in range(2, count):
        for d in range(2):
            s.weights_relay(d, dist)
    hidden = s.hidden_slab().astype(s.hidden.dtype)
    s.hidden[s.slab_of(s.lane)] = hidden
    s.every[pl.ds(pl.multiple_of(me * rows + s.lane * s.slab, s.slab), s.slab)] = s.scaled(hidden)
    for dist in range(1, count):
        for d in range(2):
            peer = me + sign_of(d) * dist
            pl.when(s.inside(peer))(s.far(d, dist, me, peer).start)
    s.rows_sent(0)
    s.weights_relay(0, 1)
    for j in range(count - 1):
        for d in range(2):
            s.wait_kv(d, j)
    load_q.wait()
    for dist in range(1, count):
        for d in range(2):
            s.weights_wait(d, dist)

    def project(block):
        at = pl.ds(pl.multiple_of(block * rows, rows), rows)
        x = s.every[at]
        for i in range(mine):
            first = i * 2 * HEAD_WIDTH
            query = jnp.dot(
                x, s.wq[:, first : first + HEAD_WIDTH], preferred_element_type=jnp.float32
            )
            gate = jnp.dot(
                x,
                s.wq[:, first + HEAD_WIDTH : first + 2 * HEAD_WIDTH],
                preferred_element_type=jnp.float32,
            )
            s.asked[i, at] = query.astype(jnp.bfloat16)
            s.opened[i, at] = jax.nn.sigmoid(gate)
        for kind in range(2):
            s.kvall[kind, at] = jnp.dot(
                x,
                s.wkv[:, kind * HEAD_WIDTH : (kind + 1) * HEAD_WIDTH],
                preferred_element_type=jnp.float32,
            ).astype(s.kvall.dtype)

    def project_at(dist):
        for d in s.steps(dist):
            block = s.block_at(d, dist)

            @pl.when(s.inside(block))
            def _():
                s.rows_ready(d, dist, block)
                project(block)

    s.rows_passed(0)
    for dist in range(1, count):
        s.rows_sent(dist)
        if dist > 1:
            s.rows_passed(dist - 1)
        project_at(dist - 1)
    s.send_hidden()
    s.rows_passed(count - 1)
    project_at(count - 1)

    span = mine * HEAD_WIDTH
    length = s.length_ref[0]

    def result(b, rank):
        return remote(
            s.attended.at[b],
            s.collected.at[:, pl.ds(pl.multiple_of(rank * span, span), span)],
            s.r_send.at[b],
            s.r_recv.at[rank],
            "seq",
            b,
        )

    for b in range(count):
        seen = (b + 1) * rows
        at_query = b * rows + lax.broadcasted_iota(jnp.int32, (rows, seen), 0)
        at_key = lax.broadcasted_iota(jnp.int32, (rows, seen), 1)
        visible = (at_key <= at_query) & (at_key < length)
        at = slice(b * rows, seen)
        for i in range(mine):
            mixed = s.attend(s.asked[i, at], s.kvall[0, :seen], s.kvall[1, :seen], visible)
            s.attended[b, :, i * HEAD_WIDTH : (i + 1) * HEAD_WIDTH] = (
                mixed * s.opened[i, at]
            ).astype(s.attended.dtype)

        @pl.when(me != b)
        def _():
            result(b, me).start()

        @pl.when(me == b)
        def _():
            s.collected[:, pl.ds(pl.multiple_of(me * span, span), span)] = s.attended[b]

    s.wait_hidden()
    save_hidden = s.load(s.hidden, s.hidden_out)
    for b in range(count):
        pl.when(me != b)(result(b, jnp.int32(b)).wait_recv)
    save_attended = s.load(s.collected, s.attention_out)

    for b in range(count):
        pl.when(me != b)(result(b, me).wait_send)
    s.end()
    s.end_weights(1)
    s.end_rows()
    for dist in range(1, count):
        for d in range(2):
            copy, go = s.weights(d, dist)
            pl.when(go)(copy.wait_send)

            @pl.when(s.inside(me - sign_of(d) * dist))
            def _():
                for e in range(1, groups):
                    s.weights_across(e, d, dist, s.part).wait_send()

    save_hidden.wait()
    save_attended.wait()


def shards(
    residual,
    query_in,
    key_in,
    value_in,
    gating_in,
    beta_logit,
    decay_logit,
    seq_length,
    conv_query,
    conv_key,
    conv_value,
    decay_rate,
    norm_gain,
    out_weight,
    attn_gain,
    query_weight,
    key_value_weight,
):
    count = lax.axis_size("seq")
    groups = lax.axis_size("groups")
    heads = lax.axis_size("head")
    rows, model = residual.shape
    value_heads = beta_logit.shape[1]
    query_heads = query_weight.shape[1] // (2 * HEAD_WIDTH)
    width = query_in.shape[1] + key_in.shape[1] + value_in.shape[1]
    depth = query_weight.shape[0] * count
    slab = rows // heads
    f32, bf16 = jnp.float32, jnp.bfloat16
    dma = pltpu.SemaphoreType.DMA
    anywhere = pl.BlockSpec(memory_space=pl.ANY)
    smem = pl.BlockSpec(memory_space=pltpu.SMEM)
    rate = decay_rate[None, :]
    gain = norm_gain[None, :]
    attn = attn_gain[None, :]
    like = lambda a: pltpu.VMEM(a.shape, a.dtype)
    split = query_heads % count == 0
    units = 1 if split else query_heads + 1
    scratch = dict(
        q_ref=like(query_in),
        k_ref=like(key_in),
        v_ref=like(value_in),
        gate_ref=like(gating_in),
        beta_ref=like(beta_logit),
        decay_ref=like(decay_logit),
        cq_ref=like(conv_query),
        ck_ref=like(conv_key),
        cv_ref=like(conv_value),
        rate_ref=like(rate),
        gain_ref=like(gain),
        ow_ref=like(out_weight),
        again_ref=like(attn),
        residual_ref=pltpu.VMEM((slab, model), bf16),
        wkv=pltpu.VMEM((depth, 2 * HEAD_WIDTH), bf16),
        tail_q=pltpu.VMEM((TAIL, query_in.shape[1]), bf16),
        tail_k=pltpu.VMEM((TAIL, key_in.shape[1]), bf16),
        tail_v=pltpu.VMEM((TAIL, value_in.shape[1]), bf16),
        joined=pltpu.VMEM((rows + PAD, width), f32),
        mapping=pltpu.VMEM((value_heads, DK + rows, DK), bf16),
        local=pltpu.VMEM((value_heads, rows, DV), f32),
        injected=pltpu.VMEM((value_heads, DK, DV), f32),
        enter=pltpu.VMEM((value_heads, DK, DV), bf16),
        leave=pltpu.VMEM((value_heads, DK, DV), bf16),
        gated=pltpu.VMEM((rows, value_heads * DV), bf16),
        summed=pltpu.VMEM((rows, model), f32),
        partial=pltpu.VMEM((rows, model), bf16),
        landed=pltpu.VMEM((heads - 1, slab, model), bf16),
        hidden=pltpu.VMEM((rows, model), bf16),
        kvall=pltpu.VMEM((2, count * rows, HEAD_WIDTH), bf16),
        load_sems=dma((24 + query_heads,)),
        tail_send=dma((3,)),
        tail_recv=dma((3,)),
        state_send=dma((value_heads,)),
        state_recv=dma((value_heads,)),
        z_send=dma((2, count - 1, units)),
        z_recv=dma((2, count - 1, units)),
        y_send=dma((groups - 1, 2, count - 1, units)),
        y_recv=dma((groups - 1, 2, count - 1, units)),
        m_send=dma((2, count - 1)),
        m_recv=dma((2, count - 1)),
        my_send=dma((groups - 1, 2, count - 1)),
        my_recv=dma((groups - 1, 2, count - 1)),
        rs_send=dma((heads - 1,)),
        rs_recv=dma((heads - 1,)),
        ag_send=dma((heads - 1,)),
        ag_recv=dma((heads - 1,)),
    )
    if split:
        mine = query_heads // count
        chips = heads // MATES
        scratch.update(
            wq=pltpu.VMEM((depth, mine * 2 * HEAD_WIDTH), bf16),
            every=pltpu.VMEM((count * rows, model), bf16),
            asked=pltpu.VMEM((mine, count * rows, HEAD_WIDTH), bf16),
            opened=pltpu.VMEM((mine, count * rows, HEAD_WIDTH), f32),
            attended=pltpu.VMEM((count, rows, mine * HEAD_WIDTH), bf16),
            collected=pltpu.VMEM((rows, query_heads * HEAD_WIDTH), bf16),
            w_send=dma((2, count - 1)),
            w_recv=dma((2, count - 1)),
            wy_send=dma((groups - 1, 2, count - 1)),
            wy_recv=dma((groups - 1, 2, count - 1)),
            n_send=dma((2, count - 1)),
            n_recv=dma((2, count - 1)),
            x_send=dma((2, count, chips - 1)),
            x_recv=dma((2, count, chips - 1)),
            t_send=dma((2, count, chips)),
            t_recv=dma((2, count, chips)),
            r_send=dma((count,)),
            r_recv=dma((count,)),
        )
    else:
        scratch.update(
            wq=pltpu.VMEM((query_heads, depth, 2 * HEAD_WIDTH), bf16),
            normed=pltpu.VMEM((rows, model), bf16),
            attended=pltpu.VMEM((rows, query_heads * HEAD_WIDTH), bf16),
            kv_send=dma((count - 1,)),
            kv_recv=dma((count - 1,)),
            km_send=dma((count - 1,)),
            km_recv=dma((count - 1,)),
        )
    return pl.pallas_call(
        functools.partial(
            split_kernel if split else ring_kernel,
            (count, groups, heads),
            INPUTS + OUTPUTS + list(scratch),
        ),
        out_shape=(
            jax.ShapeDtypeStruct(residual.shape, bf16),
            jax.ShapeDtypeStruct((rows, query_heads * HEAD_WIDTH), bf16),
        ),
        in_specs=[anywhere] * 7 + [smem] + [anywhere] * 9,
        out_specs=(anywhere, anywhere),
        scratch_shapes=list(scratch.values()),
        compiler_params=pltpu.CompilerParams(
            collective_id=0, has_side_effects=True, vmem_limit_bytes=56 * 2**20
        ),
        name="layer",
    )(
        residual,
        query_in,
        key_in,
        value_in,
        gating_in,
        beta_logit,
        decay_logit,
        seq_length,
        conv_query,
        conv_key,
        conv_value,
        rate,
        gain,
        out_weight,
        attn,
        query_weight,
        key_value_weight,
    )


def solution(mesh):
    placed = (
        P(("groups", "seq"), None),
        P(("groups", "seq"), "head"),
        P(("groups", "seq"), "head"),
        P(("groups", "seq"), "head"),
        P(("groups", "seq"), "head"),
        P(("groups", "seq"), "head"),
        P(("groups", "seq"), "head"),
        P("groups"),
        P(None, "head"),
        P(None, "head"),
        P(None, "head"),
        P("head"),
        P(),
        P("head", None),
        P(),
        P("seq", "head"),
        P("seq", None),
    )
    return jax.shard_map(
        shards,
        mesh=mesh,
        in_specs=placed,
        out_specs=(P(("groups", "seq"), None), P(("groups", "seq"), "head")),
        check_vma=False,
    )
```

```python
import functools

import jax
import jax.numpy as jnp
from jax import lax
from jax.experimental import pallas as pl
from jax.experimental.pallas import tpu as pltpu
from jax.sharding import PartitionSpec as P

DK = 128
DV = 128
QUERY_HEADS = 16
KEY_VALUE_HEADS = 2
HEAD_WIDTH = 256
CONV = 4
PAD = 8
TAIL = 16
MATES = 2
EARLY = 3
PIECES = 2

EPSILON = 1e-06
NEGATIVE = -1e30
MESH = pl.DeviceIdType.MESH
HIGHEST = lax.Precision.HIGHEST


def exact(a, b, contract=((1,), (0,))):
    return lax.dot_general(
        a, b, (contract, ((), ())), precision=HIGHEST, preferred_element_type=jnp.float32
    )


def mm(a, b, contract=((1,), (0,))):
    return lax.dot_general(
        a.astype(jnp.bfloat16),
        b.astype(jnp.bfloat16),
        (contract, ((), ())),
        preferred_element_type=jnp.float32,
    )


def softplus(x):
    return jnp.maximum(x, 0.0) + jnp.log1p(jnp.exp(-jnp.abs(x)))


def unit(x):
    return x / jnp.sqrt(jnp.sum(x * x, -1, keepdims=True) + EPSILON)


INPUTS = [
    "residual_in",
    "q_in",
    "k_in",
    "v_in",
    "gate_in",
    "beta_in",
    "decay_in",
    "length_ref",
    "cq_in",
    "ck_in",
    "cv_in",
    "rate_in",
    "gain_in",
    "ow_in",
    "again_in",
    "qw_in",
    "kvw_in",
]
OUTPUTS = ["hidden_out", "attention_out"]


def remote(source, target, send, recv, axis, index):
    return pltpu.make_async_remote_copy(
        src_ref=source,
        dst_ref=target,
        send_sem=send,
        recv_sem=recv,
        device_id={axis: index},
        device_id_type=MESH,
    )


def sign_of(d):
    return 1 if d == 0 else -1


class Layer:
    def __init__(self, sizes, names, refs):
        self.count, self.groups, self.heads = sizes
        for name, ref in zip(names, refs, strict=True):
            setattr(self, name, ref)
        self.me = lax.axis_index("seq")
        self.part = lax.axis_index("groups")
        self.lane = lax.axis_index("head")
        self.core = lax.rem(self.lane, MATES)
        self.mate = self.lane + 1 - 2 * self.core
        self.rows = self.q_ref.shape[0]
        self.key_heads = self.q_ref.shape[1] // DK
        self.value_heads = self.v_ref.shape[1] // DV
        self.share = self.value_heads // self.key_heads
        self.depth = self.qw_in.shape[0]
        self.piece = self.depth // self.groups
        self.quarter = self.piece // MATES
        self.slab = self.rows // self.heads
        self.query_heads = self.qw_in.shape[1] // (2 * HEAD_WIDTH)
        self.kv_head = self.lane * self.query_heads // (QUERY_HEADS // KEY_VALUE_HEADS)
        self.own_rows = pl.ds(pl.multiple_of(self.me * self.depth, self.depth), self.depth)
        self.follower = self.clamp(self.me + 1)
        self.loads = 0

    def load(self, source, target):
        copy = pltpu.make_async_copy(source, target, self.load_sems.at[self.loads])
        copy.start()
        self.loads += 1
        return copy

    def inside(self, block):
        return (block >= 0) & (block < self.count)

    def clamp(self, block):
        return jnp.clip(block, 0, self.count - 1)

    def slab_of(self, index):
        return pl.ds(pl.multiple_of(index * self.slab, self.slab), self.slab)


    def kv_spot(self, block, which, half):
        first = block * self.depth + which * self.piece + half * self.quarter
        return self.wkv.at[pl.ds(pl.multiple_of(first, self.quarter), self.quarter)]

    def begin(self):
        load = self.load
        self.load_kv = [
            load(
                self.kvw_in.at[
                    :,
                    pl.ds(
                        pl.multiple_of(
                            (kind * KEY_VALUE_HEADS + self.kv_head) * HEAD_WIDTH, HEAD_WIDTH
                        ),
                        HEAD_WIDTH,
                    ),
                ],
                self.wkv.at[self.own_rows, pl.ds(kind * HEAD_WIDTH, HEAD_WIDTH)],
            )
            for kind in range(2)
        ]
        self.load_decay = [
            load(self.decay_in, self.decay_ref),
            load(self.rate_in, self.rate_ref),
            load(self.beta_in, self.beta_ref),
        ]
        self.load_conv = [
            load(self.q_in, self.q_ref),
            load(self.k_in, self.k_ref),
            load(self.v_in, self.v_ref),
            load(self.cq_in, self.cq_ref),
            load(self.ck_in, self.ck_ref),
            load(self.cv_in, self.cv_ref),
        ]

        barrier = pltpu.get_barrier_semaphore()
        for axis, size, place in (
            ("seq", self.count, self.me),
            ("groups", self.groups, self.part),
            ("head", self.heads, self.lane),
        ):
            for e in range(1, size):
                pl.semaphore_signal(
                    barrier,
                    inc=1,
                    device_id={axis: lax.rem(place + e, size)},
                    device_id_type=MESH,
                )
        pl.semaphore_wait(barrier, self.count + self.groups + self.heads - 3)

        last = pl.ds(self.rows - TAIL, TAIL)
        self.tails = [
            remote(
                source.at[last],
                target,
                self.tail_send.at[i],
                self.tail_recv.at[i],
                "seq",
                self.follower,
            )
            for i, (source, target) in enumerate(
                (
                    (self.q_in, self.tail_q),
                    (self.k_in, self.tail_k),
                    (self.v_in, self.tail_v),
                )
            )
        ]

        @pl.when(self.me < self.count - 1)
        def _():
            for copy in self.tails:
                copy.start()

    def load_rest(self):
        load = self.load
        self.load_late = [
            load(self.gate_in, self.gate_ref),
            load(self.gain_in, self.gain_ref),
            load(self.ow_in, self.ow_ref),
            load(self.residual_in.at[self.slab_of(self.lane)], self.residual_ref),
            load(self.again_in, self.again_ref),
        ]

    def delta(self, pumps):
        rows, value_heads, share = self.rows, self.value_heads, self.share
        key_heads = self.key_heads
        for copy in self.load_decay:
            copy.wait()
        length = self.length_ref[0]
        at = self.me * rows + lax.broadcasted_iota(jnp.int32, (value_heads, rows), 1)
        alive = (at < length).astype(jnp.float32)
        beta_t = jax.nn.sigmoid(self.beta_ref[...]) * alive
        square = (value_heads, value_heads)
        diagonal = lax.broadcasted_iota(jnp.int32, square, 0) == lax.broadcasted_iota(
            jnp.int32, square, 1
        )
        rate = jnp.sum(jnp.where(diagonal, self.rate_ref[...], 0.0), -1, keepdims=True)
        step_t = -rate * softplus(self.decay_ref[...]) * alive
        row = lax.broadcasted_iota(jnp.int32, (rows, rows), 0)
        column = lax.broadcasted_iota(jnp.int32, (rows, rows), 1)
        inclusive = row >= column
        run_t = exact(step_t, (row <= column).astype(jnp.float32))
        blank = jnp.zeros((rows - 2 * value_heads, rows), jnp.float32)
        turned_over = jnp.concatenate([beta_t, run_t, blank], 0).T
        beta = turned_over[:, :value_heads]
        run = turned_over[:, value_heads : 2 * value_heads]
        growth = jnp.exp(run)
        self.final = growth[rows - 1 : rows]
        ending_t = jnp.exp(run_t[:, rows - 1 : rows] - run_t)
        eye = (row == column).astype(jnp.float32)

        for copy in self.load_conv:
            copy.wait()
        q_width = key_heads * DK
        joined = self.joined
        joined[PAD:, :q_width] = self.q_ref[...].astype(jnp.float32)
        joined[PAD:, q_width : 2 * q_width] = self.k_ref[...].astype(jnp.float32)
        joined[PAD:, 2 * q_width :] = self.v_ref[...].astype(jnp.float32)

        @pl.when(self.me == 0)
        def _():
            self.enter[...] = jnp.zeros_like(self.enter)
            joined[:PAD] = jnp.zeros((PAD, joined.shape[1]), jnp.float32)

        @pl.when(self.me > 0)
        def _():
            for copy in self.tails:
                copy.wait_recv()
            joined[:PAD, :q_width] = self.tail_q[...].astype(jnp.float32)[TAIL - PAD :]
            joined[:PAD, q_width : 2 * q_width] = self.tail_k[...].astype(jnp.float32)[
                TAIL - PAD :
            ]
            joined[:PAD, 2 * q_width :] = self.tail_v[...].astype(jnp.float32)[TAIL - PAD :]

        def conv(base, taps, h):
            first_column = base + h * DK
            total = jnp.zeros((rows, DK), jnp.float32)
            for j in range(CONV):
                first = PAD - CONV + 1 + j
                total = total + taps[j : j + 1, h * DK : (h + 1) * DK] * joined[
                    first : first + rows, first_column : first_column + DK
                ]
            return total * jax.nn.sigmoid(total)

        queries, keyset, turned, grams = [], [], [], []
        for g in range(key_heads):
            q = unit(conv(0, self.cq_ref, g)) * DK ** (-0.5)
            k = unit(conv(q_width, self.ck_ref, g))
            k_t = k.T
            queries.append(q)
            keyset.append(k)
            turned.append(k_t)
            grams.append(mm(jnp.concatenate([k, q], 0), k_t))
            if g == key_heads // 2 - 1:
                pumps[0]()
        pumps[1]()

        mixes, lower, inverse = [], [], []
        for h in range(value_heads):
            spread = run[:, h : h + 1] - run_t[h : h + 1, :]
            w = jnp.exp(jnp.where(inclusive, spread, NEGATIVE))
            gram = grams[h // share]
            mixes.append((gram[rows:] * w).astype(jnp.bfloat16))
            low = jnp.where(row > column, beta[:, h : h + 1] * w * gram[:rows], 0.0)
            lower.append(low)
            pair = (row // 2 == column // 2) & (row > column)
            inverse.append(eye - jnp.where(pair, low, 0.0))
        size = 2
        while size < rows:
            off = (row // (2 * size) == column // (2 * size)) & (row // size > column // size)
            half = [mm(jnp.where(off, low, 0.0), x) for low, x in zip(lower, inverse)]
            inverse = [x - mm(x, y) for x, y in zip(inverse, half)]
            size *= 2
        pumps[2]()

        for h in range(value_heads):
            k = keyset[h // share]
            v = conv(2 * q_width, self.cv_ref, h)
            b = beta[:, h : h + 1]
            grown = growth[:, h : h + 1]
            wu = mm(inverse[h], jnp.concatenate([b * grown * k, b * v], 1))
            stop_t = (turned[h // share] * ending_t[h : h + 1, :]).astype(jnp.bfloat16)
            both = mm(jnp.concatenate([stop_t, mixes[h]], 0), wu)
            self.mapping[h, :DK] = both[:DK, :DK].astype(jnp.bfloat16)
            self.mapping[h, DK:] = (grown * queries[h // share] - both[DK:, :DK]).astype(
                jnp.bfloat16
            )
            self.injected[h] = both[:DK, DK:]
            self.local[h] = both[DK:, DK:]
        pumps[3]()

    def chain(self):
        for copy in self.load_late[:2]:
            copy.wait()
        self.states = []
        for h in range(self.value_heads):
            copy = remote(
                self.leave.at[h],
                self.enter.at[h],
                self.state_send.at[h],
                self.state_recv.at[h],
                "seq",
                self.follower,
            )
            self.states.append(copy)

            @pl.when(self.me > 0)
            def _():
                copy.wait_recv()

            state = self.enter[h]
            moved = mm(self.mapping[h], state)
            total = self.final[:, h : h + 1] * state.astype(jnp.float32)
            self.leave[h] = (total - moved[:DK] + self.injected[h]).astype(self.leave.dtype)
            o = self.local[h] + moved[DK:]
            scaled = (
                o * lax.rsqrt(jnp.mean(o * o, -1, keepdims=True) + EPSILON) * self.gain_ref[...]
            )
            gate = self.gate_ref[:, h * DV : (h + 1) * DV].astype(jnp.float32)
            self.gated[:, h * DV : (h + 1) * DV] = (
                scaled * (gate * jax.nn.sigmoid(gate))
            ).astype(self.gated.dtype)

            @pl.when(self.me < self.count - 1)
            def _():
                copy.start()

    def project_out(self):
        for copy in self.load_late[2:]:
            copy.wait()
        width = self.ow_ref.shape[1]
        tile = min(512, width)
        for c in range(0, width, tile):
            product = jnp.dot(
                self.gated[...],
                self.ow_ref[:, c : c + tile],
                preferred_element_type=jnp.float32,
            )
            self.summed[:, c : c + tile] = product
            self.partial[:, c : c + tile] = product.astype(self.partial.dtype)
        self.scatter = []
        for e in range(1, self.heads):
            peer = lax.rem(self.lane + e, self.heads)
            self.scatter.append(
                remote(
                    self.partial.at[self.slab_of(peer)],
                    self.landed.at[e - 1],
                    self.rs_send.at[e - 1],
                    self.rs_recv.at[e - 1],
                    "head",
                    peer,
                )
            )
        for copy in self.scatter:
            copy.start()

    def hidden_slab(self):
        for copy in self.scatter:
            copy.wait_recv()
        return self.residual_ref[...].astype(jnp.float32) + (
            self.summed[self.slab_of(self.lane)]
            + sum(self.landed[e].astype(jnp.float32) for e in range(self.heads - 1))
        )

    def gather_hidden(self, e, index):
        place = self.hidden.at[self.slab_of(index)]
        peer = lax.rem(self.lane + e, self.heads)
        return remote(
            place, place, self.ag_send.at[e - 1], self.ag_recv.at[e - 1], "head", peer
        )

    def send_hidden(self):
        for e in range(1, self.heads):
            self.gather_hidden(e, self.lane).start()

    def wait_hidden(self):
        for e in range(1, self.heads):
            self.gather_hidden(e, lax.rem(self.lane + self.heads - e, self.heads)).wait_recv()

    def scaled(self, hidden):
        widened = hidden.astype(jnp.float32)
        mean = jnp.mean(widened * widened, -1, keepdims=True)
        return (widened * lax.rsqrt(mean + EPSILON) * self.again_ref[...]).astype(jnp.bfloat16)

    def end(self):
        @pl.when(self.me < self.count - 1)
        def _():
            for copy in self.tails + self.states:
                copy.wait_send()

        for copy in self.scatter:
            copy.wait_send()
        for e in range(1, self.heads):
            self.gather_hidden(e, self.lane).wait_send()

    def attend(self, queries, keys, values, visible):
        scores = (
            lax.dot_general(
                queries, keys, (((1,), (1,)), ((), ())), preferred_element_type=jnp.float32
            )
            * HEAD_WIDTH ** (-0.5)
        )
        scores = jnp.where(visible, scores, NEGATIVE)
        peak = jnp.max(scores, -1, keepdims=True)
        weights = jnp.where(visible, jnp.exp(scores - peak), 0.0)
        norm = jnp.sum(weights, -1, keepdims=True)
        mixed = jnp.dot(weights.astype(jnp.bfloat16), values, preferred_element_type=jnp.float32)
        return mixed / norm


class Ring(Layer):
    def spot(self, block, which, half, u):
        if u == 0:
            return self.kv_spot(block, which, half)
        first = block * self.depth + which * self.piece
        return self.wq.at[u - 1, pl.ds(pl.multiple_of(first, self.piece), self.piece)]

    def along(self, d, j, u):
        sign = sign_of(d)
        block = self.clamp(self.me - sign * j)
        target = self.spot(block, self.part, self.core, u)
        source = target
        if j == 0 and u > 0:
            source = self.qw_in.at[
                pl.ds(pl.multiple_of(self.part * self.piece, self.piece), self.piece),
                pl.ds((u - 1) * 2 * HEAD_WIDTH, 2 * HEAD_WIDTH),
            ]
        copy = remote(
            source,
            target,
            self.z_send.at[d, j, u],
            self.z_recv.at[d, j, u],
            "seq",
            self.clamp(self.me + sign),
        )
        return copy, self.inside(self.me - sign * j) & self.inside(self.me + sign)

    def arriving(self, d, j, u):
        sign = sign_of(d)
        target = self.spot(self.clamp(self.me - sign * (j + 1)), self.part, self.core, u)
        copy = remote(
            target,
            target,
            self.z_send.at[d, j, u],
            self.z_recv.at[d, j, u],
            "seq",
            self.clamp(self.me + sign),
        )
        return copy, self.inside(self.me - sign * (j + 1))

    def across(self, e, d, j, u, which):
        target = self.spot(self.clamp(self.me - sign_of(d) * (j + 1)), which, self.core, u)
        return remote(
            target,
            target,
            self.y_send.at[e - 1, d, j, u],
            self.y_recv.at[e - 1, d, j, u],
            "groups",
            lax.rem(self.part + e, self.groups),
        )

    def beside(self, d, j, half):
        target = self.kv_spot(self.clamp(self.me - sign_of(d) * (j + 1)), self.part, half)
        return remote(target, target, self.m_send.at[d, j], self.m_recv.at[d, j], "head", self.mate)

    def source_of(self, e):
        return lax.rem(self.part + self.groups - e, self.groups)

    def beyond(self, e, d, j, half):
        target = self.kv_spot(self.clamp(self.me - sign_of(d) * (j + 1)), self.source_of(e), half)
        return remote(
            target,
            target,
            self.my_send.at[e - 1, d, j],
            self.my_recv.at[e - 1, d, j],
            "head",
            self.mate,
        )

    def onward(self, d, j, u):
        if j + 1 < self.count - 1:
            copy, go = self.along(d, j + 1, u)
            pl.when(go)(copy.start)

    def relay(self, d, j, u, forward=True):
        copy, here = self.arriving(d, j, u)

        @pl.when(here)
        def _():
            copy.wait_recv()
            for e in range(1, self.groups):
                self.across(e, d, j, u, self.part).start()
            if u == 0:
                self.beside(d, j, self.core).start()

        if forward:
            self.onward(d, j, u)

    def kv_relays(self, d, first, last):
        for j in range(max(first, 1), last):
            self.relay(d, j, 0)

    def share_kv(self, d, j):
        _, here = self.arriving(d, j, 0)

        @pl.when(here)
        def _():
            for e in range(1, self.groups):
                self.across(e, d, j, 0, self.source_of(e)).wait_recv()
                self.beyond(e, d, j, self.core).start()

    def wait_kv(self, d, j):
        _, here = self.arriving(d, j, 0)

        @pl.when(here)
        def _():
            self.beside(d, j, 1 - self.core).wait_recv()
            for e in range(1, self.groups):
                self.beyond(e, d, j, 1 - self.core).wait_recv()

    def end_weights(self, units):
        for j in range(self.count - 1):
            for d in range(2):
                for u in range(units):
                    copy, go = self.along(d, j, u)
                    pl.when(go)(copy.wait_send)
                _, here = self.arriving(d, j, 0)

                @pl.when(here)
                def _():
                    for e in range(1, self.groups):
                        for u in range(units):
                            self.across(e, d, j, u, self.part).wait_send()
                        self.beyond(e, d, j, self.core).wait_send()
                    self.beside(d, j, self.core).wait_send()


def ring_kernel(sizes, names, *refs):
    s = Ring(sizes, names, refs)
    count, groups, me, rows = s.count, s.groups, s.me, s.rows
    units = s.query_heads + 1
    early = min(EARLY, units)
    s.begin()
    for copy in s.load_kv:
        copy.wait()
    for u in range(units):
        for d in range(2):
            if d == 1 or u < early:
                copy, go = s.along(d, 0, u)
                pl.when(go)(copy.start)
    s.load_rest()
    load_q = [
        s.load(
            s.qw_in.at[:, pl.ds(i * 2 * HEAD_WIDTH, 2 * HEAD_WIDTH)], s.wq.at[i, s.own_rows]
        )
        for i in range(s.query_heads)
    ]

    for b in range(1, count):

        @pl.when(b > me)
        def _():
            s.kvall[:, b * rows : (b + 1) * rows] = jnp.zeros(
                (2, rows, HEAD_WIDTH), s.kvall.dtype
            )

    def pump(u):
        def run():
            if u < early:
                for d in range(2):
                    s.relay(d, 0, u, forward=d == 1)

        return run

    s.delta([lambda: None] + [pump(u) for u in range(3)])
    s.chain()
    for u in range(early, units):
        copy, go = s.along(0, 0, u)
        pl.when(go)(copy.start)
    for u in range(early):
        s.onward(0, 0, u)
    s.project_out()
    for u in range(early, units):
        for d in range(2):
            s.relay(d, 0, u)
    for d in range(2):
        s.share_kv(d, 0)
    s.hidden[s.slab_of(s.lane)] = s.hidden_slab().astype(s.hidden.dtype)
    s.send_hidden()
    for j in range(1, count - 1):
        for d in range(2):
            s.relay(d, j, 0)
    for j in range(1, count - 1):
        for d in range(2):
            s.share_kv(d, j)
    s.wait_hidden()
    save_hidden = s.load(s.hidden, s.hidden_out)
    s.normed[...] = s.scaled(s.hidden[...])

    for j in range(count - 1):
        for d in range(2):
            s.wait_kv(d, j)
    own_block = pl.ds(pl.multiple_of(me * rows, rows), rows)
    for kind in range(2):
        s.kvall[kind, own_block] = jnp.dot(
            s.normed[...],
            s.wkv[:, kind * HEAD_WIDTH : (kind + 1) * HEAD_WIDTH],
            preferred_element_type=jnp.float32,
        ).astype(s.kvall.dtype)

    def later(e, block, axis, index, kind, send, recv):
        place = s.kvall.at[kind, pl.ds(pl.multiple_of(s.clamp(block) * rows, rows), rows)]
        return remote(place, place, send.at[e - 1], recv.at[e - 1], axis, index)

    def sent_kv(e):
        return later(e, me, "seq", s.clamp(me + e), s.core, s.kv_send, s.kv_recv)

    def mate_kv(e, kind):
        return later(e, me - e, "head", s.mate, kind, s.km_send, s.km_recv)

    for e in range(1, count):
        pl.when(me + e < count)(sent_kv(e).start)

    for j in range(1, count - 1):
        for u in range(1, units):
            for d in range(2):
                if (j, u) < (count - 2, 1) or count == 2:
                    s.relay(d, j, u)

    for e in range(1, count):

        @pl.when(me >= e)
        def _():
            later(e, me - e, "seq", s.clamp(me - e), s.core, s.kv_send, s.kv_recv).wait_recv()
            mate_kv(e, s.core).start()

    for e in range(1, count):
        pl.when(me >= e)(mate_kv(e, 1 - s.core).wait_recv)

    for copy in load_q:
        copy.wait()
    keys_total = count * rows
    at_query = me * rows + lax.broadcasted_iota(jnp.int32, (rows, keys_total), 0)
    at_key = lax.broadcasted_iota(jnp.int32, (rows, keys_total), 1)
    visible = (at_key <= at_query) & (at_key < s.length_ref[0])
    for i in range(s.query_heads):
        if count > 2:
            for d in range(2):
                s.relay(d, count - 2, i + 1)
        for j in range(count - 1):
            for d in range(2):
                _, here = s.arriving(d, j, i + 1)

                @pl.when(here)
                def _():
                    for e in range(1, groups):
                        s.across(e, d, j, i + 1, s.source_of(e)).wait_recv()

        projected = jnp.dot(s.normed[...], s.wq[i], preferred_element_type=jnp.float32)
        mixed = s.attend(
            projected[:, :HEAD_WIDTH].astype(jnp.bfloat16), s.kvall[0], s.kvall[1], visible
        )
        s.attended[:, i * HEAD_WIDTH : (i + 1) * HEAD_WIDTH] = (
            mixed * jax.nn.sigmoid(projected[:, HEAD_WIDTH:])
        ).astype(s.attended.dtype)
    save_attended = s.load(s.attended, s.attention_out)

    s.end()
    s.end_weights(units)
    for e in range(1, count):
        pl.when(me + e < count)(sent_kv(e).wait_send)
        pl.when(me >= e)(mate_kv(e, s.core).wait_send)
    save_hidden.wait()
    save_attended.wait()


class Split(Ring):
    def weights(self, d, dist, p):
        sign = sign_of(d)
        peer = self.me + sign * dist
        wide = self.wq.shape[1]
        size = self.piece // PIECES
        first = pl.multiple_of(self.part * self.piece + p * size, size)
        copy = remote(
            self.qw_in.at[
                pl.ds(first, size),
                pl.ds(pl.multiple_of(self.clamp(peer) * wide, wide), wide),
            ],
            self.weight_rows(self.me, self.part, p),
            self.w_send.at[d, dist - 1, p],
            self.w_recv.at[d, dist - 1, p],
            "seq",
            self.clamp(peer),
        )
        return copy, self.inside(peer)

    def weight_rows(self, block, which, p):
        size = self.piece // PIECES
        first = self.clamp(block) * self.depth + which * self.piece + p * size
        return self.wq.at[pl.ds(pl.multiple_of(first, size), size)]

    def weights_across(self, e, d, dist, which, p):
        place = self.weight_rows(self.me - sign_of(d) * dist, which, p)
        return remote(
            place,
            place,
            self.wy_send.at[e - 1, d, dist - 1, p],
            self.wy_recv.at[e - 1, d, dist - 1, p],
            "groups",
            lax.rem(self.part + e, self.groups),
        )

    def weights_relay(self, d, dist):
        block = self.me - sign_of(d) * dist

        @pl.when(self.inside(block))
        def _():
            for p in range(PIECES):
                place = self.weight_rows(block, self.part, p)
                remote(
                    place,
                    place,
                    self.w_send.at[d, dist - 1, p],
                    self.w_recv.at[d, dist - 1, p],
                    "seq",
                    self.clamp(block),
                ).wait_recv()
                for e in range(1, self.groups):
                    self.weights_across(e, d, dist, self.part, p).start()

    def weights_wait(self, d, dist):
        @pl.when(self.inside(self.me - sign_of(d) * dist))
        def _():
            for e in range(1, self.groups):
                for p in range(PIECES):
                    self.weights_across(e, d, dist, self.source_of(e), p).wait_recv()


    def place(self, block, index):
        first = block * self.rows + index * self.slab
        return self.every.at[pl.ds(pl.multiple_of(first, self.slab), self.slab)]

    def far(self, d, dist, block):
        place = self.place(self.clamp(block), self.lane)
        return remote(
            place,
            place,
            self.n_send.at[d, dist],
            self.n_recv.at[d, dist],
            "seq",
            self.clamp(self.me + sign_of(d)),
        )

    def rows_onward(self, d, dist):
        block = self.me - sign_of(d) * dist
        go = self.inside(block) & self.inside(self.me + sign_of(d))
        return self.far(d, dist, block), go

    def near(self, d, dist, f, block, index):
        place = self.place(self.clamp(block), index)
        peer = lax.rem(self.lane + MATES * f, self.heads)
        return remote(
            place,
            place,
            self.x_send.at[d, dist, f - 1],
            self.x_recv.at[d, dist, f - 1],
            "head",
            peer,
        )

    def twin(self, d, dist, f, block, index):
        place = self.place(self.clamp(block), index)
        return remote(
            place, place, self.t_send.at[d, dist, f], self.t_recv.at[d, dist, f], "head", self.mate
        )

    def back(self, f, lane):
        return lax.rem(lane + self.heads - MATES * f, self.heads)

    def chips(self):
        return range(1, self.heads // MATES)

    def block_at(self, d, dist):
        return self.me - sign_of(d) * dist

    def steps(self, dist):
        return (0,) if dist == 0 else (0, 1)

    def rows_sent(self, d, dist):
        block = self.block_at(d, dist)

        @pl.when(self.inside(block))
        def _():
            if dist > 0:
                self.far(d, dist - 1, block).wait_recv()
            for f in self.chips():
                self.near(d, dist, f, block, self.lane).start()
            self.twin(d, dist, 0, block, self.lane).start()

        if 0 < dist < self.count - 1:
            copy, go = self.rows_onward(d, dist)
            pl.when(go)(copy.start)

    def rows_passed(self, d, dist):
        block = self.block_at(d, dist)

        @pl.when(self.inside(block))
        def _():
            for f in self.chips():
                self.near(d, dist, f, block, self.back(f, self.lane)).wait_recv()
                self.twin(d, dist, f, block, self.back(f, self.lane)).start()

    def rows_ready(self, d, dist, block):
        for f in range(self.heads // MATES):
            self.twin(d, dist, f, block, self.back(f, self.mate)).wait_recv()

    def end_rows(self):
        for dist in range(self.count - 1):
            for d in range(2):
                copy, go = self.rows_onward(d, dist)
                pl.when(go)(copy.wait_send)
        for dist in range(self.count):
            for d in self.steps(dist):
                block = self.block_at(d, dist)

                @pl.when(self.inside(block))
                def _():
                    for f in self.chips():
                        self.near(d, dist, f, block, self.lane).wait_send()
                    for f in range(self.heads // MATES):
                        self.twin(d, dist, f, block, self.back(f, self.lane)).wait_send()


def split_kernel(sizes, names, *refs):
    s = Split(sizes, names, refs)
    count, groups, me, rows = s.count, s.groups, s.me, s.rows
    wide = s.wq.shape[1]
    mine = wide // (2 * HEAD_WIDTH)
    s.begin()
    last = count - 1

    def send_weights(d, dist):
        for p in range(PIECES):
            copy, go = s.weights(d, dist, p)
            pl.when(go)(copy.start)

    for copy in s.load_kv:
        copy.wait()
    for d in range(2):
        copy, go = s.along(d, 0, 0)
        pl.when(go)(copy.start)
    pl.when(me > 0)(functools.partial(send_weights, 0, 1))
    s.load_rest()
    load_q = s.load(
        s.qw_in.at[:, pl.ds(pl.multiple_of(me * wide, wide), wide)], s.wq.at[s.own_rows]
    )

    def pump_heads():
        @pl.when(me > 0)
        def _():
            s.relay(0, 0, 0, forward=False)
            s.relay(1, 0, 0)
            send_weights(1, 1)

    def pump_updates():
        @pl.when(me > 0)
        def _():
            for j in range(1, last - 1):
                s.relay(1, j, 0)

        pl.when(me > 1)(functools.partial(s.weights_relay, 0, 1))
        for dist in range(2, count):
            send_weights(1, dist)

    s.delta([pump_heads, lambda: None, lambda: None, pump_updates])
    s.chain()
    s.onward(0, 0, 0)
    s.project_out()
    s.kv_relays(0, 1, last - 1)
    hidden = s.hidden_slab().astype(s.hidden.dtype)
    s.hidden[s.slab_of(s.lane)] = hidden
    s.every[pl.ds(pl.multiple_of(me * rows + s.lane * s.slab, s.slab), s.slab)] = s.scaled(hidden)
    for d in range(2):
        copy, go = s.rows_onward(d, 0)
        pl.when(go)(copy.start)
    s.rows_sent(0, 0)

    s.rows_sent(0, 1)

    def send_far():
        for dist in range(last, 1, -1):
            send_weights(0, dist)

    @pl.when(me == 0)
    def _():
        send_weights(0, 1)
        s.relay(1, 0, 0)

    pl.when(me == 1)(functools.partial(s.weights_relay, 0, 1))
    pl.when(me > 0)(send_far)
    s.weights_relay(1, 1)
    for d in range(2):
        s.share_kv(d, 0)
    pl.when(me == 0)(functools.partial(s.kv_relays, 1, 1, last - 1))
    for d in range(2):
        s.kv_relays(d, last - 1, last)

    def far_weights(d):
        for dist in range(last - 1, 1, -1):
            s.weights_relay(d, dist)

    pl.when(me > 0)(functools.partial(far_weights, 1))
    s.rows_passed(0, 0)

    @pl.when(me == 0)
    def _():
        s.weights_relay(1, last)
        send_far()

    s.rows_sent(1, 1)
    for dist in range(2, last):
        s.rows_sent(0, dist)
    s.rows_passed(0, 1)
    for j in range(1, last):
        for d in range(2):
            s.share_kv(d, j)
    s.weights_relay(0, last)
    pl.when(me == 0)(functools.partial(far_weights, 1))
    far_weights(0)
    for dist in range(2, last):
        s.rows_sent(1, dist)
    s.rows_sent(0, last)
    s.rows_passed(1, 1)
    for dist in range(2, last):
        s.rows_passed(0, dist)
    s.rows_sent(1, last)
    for dist in range(2, last):
        s.rows_passed(1, dist)

    def project(block):
        at = pl.ds(pl.multiple_of(block * rows, rows), rows)
        x = s.every[at]
        for i in range(mine):
            first = i * 2 * HEAD_WIDTH
            query = jnp.dot(
                x, s.wq[:, first : first + HEAD_WIDTH], preferred_element_type=jnp.float32
            )
            gate = jnp.dot(
                x,
                s.wq[:, first + HEAD_WIDTH : first + 2 * HEAD_WIDTH],
                preferred_element_type=jnp.float32,
            )
            s.asked[i, at] = query.astype(jnp.bfloat16)
            s.opened[i, at] = jax.nn.sigmoid(gate)
        for kind in range(2):
            s.kvall[kind, at] = jnp.dot(
                x,
                s.wkv[:, kind * HEAD_WIDTH : (kind + 1) * HEAD_WIDTH],
                preferred_element_type=jnp.float32,
            ).astype(s.kvall.dtype)

    def project_at(dist):
        for d in s.steps(dist):
            block = s.block_at(d, dist)

            @pl.when(s.inside(block))
            def _():
                s.rows_ready(d, dist, block)
                project(block)

    s.send_hidden()
    for d in range(2):
        s.rows_passed(d, last)
    for j in range(last):
        for d in range(2):
            s.wait_kv(d, j)
    load_q.wait()
    for dist in range(1, count):
        for d in range(2):
            s.weights_wait(d, dist)
    for dist in range(last):
        project_at(dist)
    project_at(last)

    span = mine * HEAD_WIDTH
    length = s.length_ref[0]

    def result(b, rank):
        return remote(
            s.attended.at[b],
            s.collected.at[:, pl.ds(pl.multiple_of(rank * span, span), span)],
            s.r_send.at[b],
            s.r_recv.at[rank],
            "seq",
            b,
        )

    for b in range(count):
        seen = (b + 1) * rows
        at_query = b * rows + lax.broadcasted_iota(jnp.int32, (rows, seen), 0)
        at_key = lax.broadcasted_iota(jnp.int32, (rows, seen), 1)
        visible = (at_key <= at_query) & (at_key < length)
        at = slice(b * rows, seen)
        for i in range(mine):
            mixed = s.attend(s.asked[i, at], s.kvall[0, :seen], s.kvall[1, :seen], visible)
            s.attended[b, :, i * HEAD_WIDTH : (i + 1) * HEAD_WIDTH] = (
                mixed * s.opened[i, at]
            ).astype(s.attended.dtype)

        @pl.when(me != b)
        def _():
            result(b, me).start()

        @pl.when(me == b)
        def _():
            s.collected[:, pl.ds(pl.multiple_of(me * span, span), span)] = s.attended[b]

    s.wait_hidden()
    save_hidden = s.load(s.hidden, s.hidden_out)
    for b in range(count):
        pl.when(me != b)(result(b, jnp.int32(b)).wait_recv)
    save_attended = s.load(s.collected, s.attention_out)

    for b in range(count):
        pl.when(me != b)(result(b, me).wait_send)
    s.end()
    s.end_weights(1)
    s.end_rows()
    for dist in range(1, count):
        for d in range(2):
            for p in range(PIECES):
                copy, go = s.weights(d, dist, p)
                pl.when(go)(copy.wait_send)

            @pl.when(s.inside(me - sign_of(d) * dist))
            def _():
                for e in range(1, groups):
                    for p in range(PIECES):
                        s.weights_across(e, d, dist, s.part, p).wait_send()

    save_hidden.wait()
    save_attended.wait()


def shards(
    residual,
    query_in,
    key_in,
    value_in,
    gating_in,
    beta_logit,
    decay_logit,
    seq_length,
    conv_query,
    conv_key,
    conv_value,
    decay_rate,
    norm_gain,
    out_weight,
    attn_gain,
    query_weight,
    key_value_weight,
):
    count = lax.axis_size("seq")
    groups = lax.axis_size("groups")
    heads = lax.axis_size("head")
    rows, model = residual.shape
    value_heads = beta_logit.shape[1]
    query_heads = query_weight.shape[1] // (2 * HEAD_WIDTH)
    width = query_in.shape[1] + key_in.shape[1] + value_in.shape[1]
    depth = query_weight.shape[0] * count
    slab = rows // heads
    f32, bf16 = jnp.float32, jnp.bfloat16
    dma = pltpu.SemaphoreType.DMA
    anywhere = pl.BlockSpec(memory_space=pl.ANY)
    smem = pl.BlockSpec(memory_space=pltpu.SMEM)
    rate = decay_rate[None, :]
    beta_t, decay_t = beta_logit.T, decay_logit.T
    gain = norm_gain[None, :]
    attn = attn_gain[None, :]
    like = lambda a: pltpu.VMEM(a.shape, a.dtype)
    split = query_heads % count == 0
    units = 1 if split else query_heads + 1
    scratch = dict(
        q_ref=like(query_in),
        k_ref=like(key_in),
        v_ref=like(value_in),
        gate_ref=like(gating_in),
        beta_ref=like(beta_t),
        decay_ref=like(decay_t),
        cq_ref=like(conv_query),
        ck_ref=like(conv_key),
        cv_ref=like(conv_value),
        rate_ref=like(rate),
        gain_ref=like(gain),
        ow_ref=like(out_weight),
        again_ref=like(attn),
        residual_ref=pltpu.VMEM((slab, model), bf16),
        wkv=pltpu.VMEM((depth, 2 * HEAD_WIDTH), bf16),
        tail_q=pltpu.VMEM((TAIL, query_in.shape[1]), bf16),
        tail_k=pltpu.VMEM((TAIL, key_in.shape[1]), bf16),
        tail_v=pltpu.VMEM((TAIL, value_in.shape[1]), bf16),
        joined=pltpu.VMEM((rows + PAD, width), f32),
        mapping=pltpu.VMEM((value_heads, DK + rows, DK), bf16),
        local=pltpu.VMEM((value_heads, rows, DV), f32),
        injected=pltpu.VMEM((value_heads, DK, DV), f32),
        enter=pltpu.VMEM((value_heads, DK, DV), bf16),
        leave=pltpu.VMEM((value_heads, DK, DV), bf16),
        gated=pltpu.VMEM((rows, value_heads * DV), bf16),
        summed=pltpu.VMEM((rows, model), f32),
        partial=pltpu.VMEM((rows, model), bf16),
        landed=pltpu.VMEM((heads - 1, slab, model), bf16),
        hidden=pltpu.VMEM((rows, model), bf16),
        kvall=pltpu.VMEM((2, count * rows, HEAD_WIDTH), bf16),
        load_sems=dma((24 + query_heads,)),
        tail_send=dma((3,)),
        tail_recv=dma((3,)),
        state_send=dma((value_heads,)),
        state_recv=dma((value_heads,)),
        z_send=dma((2, count - 1, units)),
        z_recv=dma((2, count - 1, units)),
        y_send=dma((groups - 1, 2, count - 1, units)),
        y_recv=dma((groups - 1, 2, count - 1, units)),
        m_send=dma((2, count - 1)),
        m_recv=dma((2, count - 1)),
        my_send=dma((groups - 1, 2, count - 1)),
        my_recv=dma((groups - 1, 2, count - 1)),
        rs_send=dma((heads - 1,)),
        rs_recv=dma((heads - 1,)),
        ag_send=dma((heads - 1,)),
        ag_recv=dma((heads - 1,)),
    )
    if split:
        mine = query_heads // count
        chips = heads // MATES
        scratch.update(
            wq=pltpu.VMEM((depth, mine * 2 * HEAD_WIDTH), bf16),
            every=pltpu.VMEM((count * rows, model), bf16),
            asked=pltpu.VMEM((mine, count * rows, HEAD_WIDTH), bf16),
            opened=pltpu.VMEM((mine, count * rows, HEAD_WIDTH), f32),
            attended=pltpu.VMEM((count, rows, mine * HEAD_WIDTH), bf16),
            collected=pltpu.VMEM((rows, query_heads * HEAD_WIDTH), bf16),
            w_send=dma((2, count - 1, PIECES)),
            w_recv=dma((2, count - 1, PIECES)),
            wy_send=dma((groups - 1, 2, count - 1, PIECES)),
            wy_recv=dma((groups - 1, 2, count - 1, PIECES)),
            n_send=dma((2, count - 1)),
            n_recv=dma((2, count - 1)),
            x_send=dma((2, count, chips - 1)),
            x_recv=dma((2, count, chips - 1)),
            t_send=dma((2, count, chips)),
            t_recv=dma((2, count, chips)),
            r_send=dma((count,)),
            r_recv=dma((count,)),
        )
    else:
        scratch.update(
            wq=pltpu.VMEM((query_heads, depth, 2 * HEAD_WIDTH), bf16),
            normed=pltpu.VMEM((rows, model), bf16),
            attended=pltpu.VMEM((rows, query_heads * HEAD_WIDTH), bf16),
            kv_send=dma((count - 1,)),
            kv_recv=dma((count - 1,)),
            km_send=dma((count - 1,)),
            km_recv=dma((count - 1,)),
        )
    return pl.pallas_call(
        functools.partial(
            split_kernel if split else ring_kernel,
            (count, groups, heads),
            INPUTS + OUTPUTS + list(scratch),
        ),
        out_shape=(
            jax.ShapeDtypeStruct(residual.shape, bf16),
            jax.ShapeDtypeStruct((rows, query_heads * HEAD_WIDTH), bf16),
        ),
        in_specs=[anywhere] * 7 + [smem] + [anywhere] * 9,
        out_specs=(anywhere, anywhere),
        scratch_shapes=list(scratch.values()),
        compiler_params=pltpu.CompilerParams(
            collective_id=0, has_side_effects=True, vmem_limit_bytes=56 * 2**20
        ),
        name="layer",
    )(
        residual,
        query_in,
        key_in,
        value_in,
        gating_in,
        beta_t,
        decay_t,
        seq_length,
        conv_query,
        conv_key,
        conv_value,
        rate,
        gain,
        out_weight,
        attn,
        query_weight,
        key_value_weight,
    )


def solution(mesh):
    placed = (
        P(("groups", "seq"), None),
        P(("groups", "seq"), "head"),
        P(("groups", "seq"), "head"),
        P(("groups", "seq"), "head"),
        P(("groups", "seq"), "head"),
        P(("groups", "seq"), "head"),
        P(("groups", "seq"), "head"),
        P("groups"),
        P(None, "head"),
        P(None, "head"),
        P(None, "head"),
        P("head"),
        P(),
        P("head", None),
        P(),
        P("seq", "head"),
        P("seq", None),
    )
    return jax.shard_map(
        shards,
        mesh=mesh,
        in_specs=placed,
        out_specs=(P(("groups", "seq"), None), P(("groups", "seq"), "head")),
        check_vma=False,
    )
```

```python
import functools

import jax
import jax.numpy as jnp
from jax import lax
from jax.experimental import pallas as pl
from jax.experimental.pallas import tpu as pltpu
from jax.sharding import PartitionSpec as P

DK = 128
DV = 128
QUERY_HEADS = 16
KEY_VALUE_HEADS = 2
HEAD_WIDTH = 256
CONV = 4
PAD = 8
TAIL = 16
MATES = 2
EARLY = 3
PIECES = 2

EPSILON = 1e-06
NEGATIVE = -1e30
MESH = pl.DeviceIdType.MESH
HIGHEST = lax.Precision.HIGHEST


def exact(a, b, contract=((1,), (0,))):
    return lax.dot_general(
        a, b, (contract, ((), ())), precision=HIGHEST, preferred_element_type=jnp.float32
    )


def mm(a, b, contract=((1,), (0,))):
    return lax.dot_general(
        a.astype(jnp.bfloat16),
        b.astype(jnp.bfloat16),
        (contract, ((), ())),
        preferred_element_type=jnp.float32,
    )


def softplus(x):
    return jnp.maximum(x, 0.0) + jnp.log1p(jnp.exp(-jnp.abs(x)))


def unit(x):
    return x / jnp.sqrt(jnp.sum(x * x, -1, keepdims=True) + EPSILON)


INPUTS = [
    "residual_in",
    "q_in",
    "k_in",
    "v_in",
    "gate_in",
    "beta_in",
    "decay_in",
    "length_ref",
    "cq_in",
    "ck_in",
    "cv_in",
    "rate_in",
    "gain_in",
    "ow_in",
    "again_in",
    "qw_in",
    "kvw_in",
]
OUTPUTS = ["hidden_out", "attention_out"]


def remote(source, target, send, recv, axis, index):
    return pltpu.make_async_remote_copy(
        src_ref=source,
        dst_ref=target,
        send_sem=send,
        recv_sem=recv,
        device_id={axis: index},
        device_id_type=MESH,
    )


def sign_of(d):
    return 1 if d == 0 else -1


class Layer:
    def __init__(self, sizes, names, refs):
        self.count, self.groups, self.heads = sizes
        for name, ref in zip(names, refs, strict=True):
            setattr(self, name, ref)
        self.me = lax.axis_index("seq")
        self.part = lax.axis_index("groups")
        self.lane = lax.axis_index("head")
        self.core = lax.rem(self.lane, MATES)
        self.mate = self.lane + 1 - 2 * self.core
        self.rows = self.q_ref.shape[0]
        self.key_heads = self.q_ref.shape[1] // DK
        self.value_heads = self.v_ref.shape[1] // DV
        self.share = self.value_heads // self.key_heads
        self.depth = self.qw_in.shape[0]
        self.piece = self.depth // self.groups
        self.quarter = self.piece // MATES
        self.slab = self.rows // self.heads
        self.query_heads = self.qw_in.shape[1] // (2 * HEAD_WIDTH)
        self.kv_head = self.lane * self.query_heads // (QUERY_HEADS // KEY_VALUE_HEADS)
        self.own_rows = pl.ds(pl.multiple_of(self.me * self.depth, self.depth), self.depth)
        self.follower = self.clamp(self.me + 1)
        self.loads = 0

    def load(self, source, target):
        copy = pltpu.make_async_copy(source, target, self.load_sems.at[self.loads])
        copy.start()
        self.loads += 1
        return copy

    def inside(self, block):
        return (block >= 0) & (block < self.count)

    def clamp(self, block):
        return jnp.clip(block, 0, self.count - 1)

    def slab_of(self, index):
        return pl.ds(pl.multiple_of(index * self.slab, self.slab), self.slab)


    def kv_spot(self, block, which, half):
        first = block * self.depth + which * self.piece + half * self.quarter
        return self.wkv.at[pl.ds(pl.multiple_of(first, self.quarter), self.quarter)]

    def begin(self):
        load = self.load
        self.load_kv = [
            load(
                self.kvw_in.at[
                    :,
                    pl.ds(
                        pl.multiple_of(
                            (kind * KEY_VALUE_HEADS + self.kv_head) * HEAD_WIDTH, HEAD_WIDTH
                        ),
                        HEAD_WIDTH,
                    ),
                ],
                self.wkv.at[self.own_rows, pl.ds(kind * HEAD_WIDTH, HEAD_WIDTH)],
            )
            for kind in range(2)
        ]
        self.load_decay = [
            load(self.decay_in, self.decay_ref),
            load(self.rate_in, self.rate_ref),
            load(self.beta_in, self.beta_ref),
        ]
        self.load_conv = [
            load(self.q_in, self.q_ref),
            load(self.k_in, self.k_ref),
            load(self.v_in, self.v_ref),
            load(self.cq_in, self.cq_ref),
            load(self.ck_in, self.ck_ref),
            load(self.cv_in, self.cv_ref),
        ]

        barrier = pltpu.get_barrier_semaphore()
        for axis, size, place in (
            ("seq", self.count, self.me),
            ("groups", self.groups, self.part),
            ("head", self.heads, self.lane),
        ):
            for e in range(1, size):
                pl.semaphore_signal(
                    barrier,
                    inc=1,
                    device_id={axis: lax.rem(place + e, size)},
                    device_id_type=MESH,
                )
        pl.semaphore_wait(barrier, self.count + self.groups + self.heads - 3)

        last = pl.ds(self.rows - TAIL, TAIL)
        self.tails = [
            remote(
                source.at[last],
                target,
                self.tail_send.at[i],
                self.tail_recv.at[i],
                "seq",
                self.follower,
            )
            for i, (source, target) in enumerate(
                (
                    (self.q_in, self.tail_q),
                    (self.k_in, self.tail_k),
                    (self.v_in, self.tail_v),
                )
            )
        ]

        @pl.when(self.me < self.count - 1)
        def _():
            for copy in self.tails:
                copy.start()

    def load_rest(self):
        load = self.load
        self.load_late = [
            load(self.gate_in, self.gate_ref),
            load(self.gain_in, self.gain_ref),
            load(self.ow_in, self.ow_ref),
            load(self.residual_in.at[self.slab_of(self.lane)], self.residual_ref),
            load(self.again_in, self.again_ref),
        ]

    def delta(self, pumps):
        rows, value_heads, share = self.rows, self.value_heads, self.share
        key_heads = self.key_heads
        for copy in self.load_decay:
            copy.wait()
        length = self.length_ref[0]
        at = self.me * rows + lax.broadcasted_iota(jnp.int32, (value_heads, rows), 1)
        alive = (at < length).astype(jnp.float32)
        beta_t = jax.nn.sigmoid(self.beta_ref[...]) * alive
        square = (value_heads, value_heads)
        diagonal = lax.broadcasted_iota(jnp.int32, square, 0) == lax.broadcasted_iota(
            jnp.int32, square, 1
        )
        rate = jnp.sum(jnp.where(diagonal, self.rate_ref[...], 0.0), -1, keepdims=True)
        step_t = -rate * softplus(self.decay_ref[...]) * alive
        row = lax.broadcasted_iota(jnp.int32, (rows, rows), 0)
        column = lax.broadcasted_iota(jnp.int32, (rows, rows), 1)
        inclusive = row >= column
        run_t = exact(step_t, (row <= column).astype(jnp.float32))
        blank = jnp.zeros((rows - 2 * value_heads, rows), jnp.float32)
        turned_over = jnp.concatenate([beta_t, run_t, blank], 0).T
        beta = turned_over[:, :value_heads]
        run = turned_over[:, value_heads : 2 * value_heads]
        growth = jnp.exp(run)
        self.final = growth[rows - 1 : rows]
        ending_t = jnp.exp(run_t[:, rows - 1 : rows] - run_t)
        eye = (row == column).astype(jnp.float32)

        for copy in self.load_conv:
            copy.wait()
        q_width = key_heads * DK
        joined = self.joined
        joined[PAD:, :q_width] = self.q_ref[...].astype(jnp.float32)
        joined[PAD:, q_width : 2 * q_width] = self.k_ref[...].astype(jnp.float32)
        joined[PAD:, 2 * q_width :] = self.v_ref[...].astype(jnp.float32)

        @pl.when(self.me == 0)
        def _():
            self.enter[...] = jnp.zeros_like(self.enter)
            joined[:PAD] = jnp.zeros((PAD, joined.shape[1]), jnp.float32)

        @pl.when(self.me > 0)
        def _():
            for copy in self.tails:
                copy.wait_recv()
            joined[:PAD, :q_width] = self.tail_q[...].astype(jnp.float32)[TAIL - PAD :]
            joined[:PAD, q_width : 2 * q_width] = self.tail_k[...].astype(jnp.float32)[
                TAIL - PAD :
            ]
            joined[:PAD, 2 * q_width :] = self.tail_v[...].astype(jnp.float32)[TAIL - PAD :]

        def conv(base, taps, h):
            first_column = base + h * DK
            total = jnp.zeros((rows, DK), jnp.float32)
            for j in range(CONV):
                first = PAD - CONV + 1 + j
                total = total + taps[j : j + 1, h * DK : (h + 1) * DK] * joined[
                    first : first + rows, first_column : first_column + DK
                ]
            return total * jax.nn.sigmoid(total)

        queries, keyset, turned, grams = [], [], [], []
        for g in range(key_heads):
            q = unit(conv(0, self.cq_ref, g)) * DK ** (-0.5)
            k = unit(conv(q_width, self.ck_ref, g))
            k_t = k.T
            queries.append(q)
            keyset.append(k)
            turned.append(k_t)
            grams.append(mm(jnp.concatenate([k, q], 0), k_t))
            if g == key_heads // 2 - 1:
                pumps[0]()
        pumps[1]()

        mixes, lower, inverse = [], [], []
        for h in range(value_heads):
            spread = run[:, h : h + 1] - run_t[h : h + 1, :]
            w = jnp.exp(jnp.where(inclusive, spread, NEGATIVE))
            gram = grams[h // share]
            mixes.append((gram[rows:] * w).astype(jnp.bfloat16))
            low = jnp.where(row > column, beta[:, h : h + 1] * w * gram[:rows], 0.0)
            lower.append(low)
            pair = (row // 2 == column // 2) & (row > column)
            inverse.append(eye - jnp.where(pair, low, 0.0))
        size = 2
        while size < rows:
            off = (row // (2 * size) == column // (2 * size)) & (row // size > column // size)
            half = [mm(jnp.where(off, low, 0.0), x) for low, x in zip(lower, inverse)]
            inverse = [x - mm(x, y) for x, y in zip(inverse, half)]
            size *= 2
        pumps[2]()

        for h in range(value_heads):
            k = keyset[h // share]
            v = conv(2 * q_width, self.cv_ref, h)
            b = beta[:, h : h + 1]
            grown = growth[:, h : h + 1]
            wu = mm(inverse[h], jnp.concatenate([b * grown * k, b * v], 1))
            stop_t = (turned[h // share] * ending_t[h : h + 1, :]).astype(jnp.bfloat16)
            both = mm(jnp.concatenate([stop_t, mixes[h]], 0), wu)
            self.mapping[h, :DK] = both[:DK, :DK].astype(jnp.bfloat16)
            self.mapping[h, DK:] = (grown * queries[h // share] - both[DK:, :DK]).astype(
                jnp.bfloat16
            )
            self.injected[h] = both[:DK, DK:]
            self.local[h] = both[DK:, DK:]
        pumps[3]()

    def chain(self):
        for copy in self.load_late[:2]:
            copy.wait()
        self.states = []
        for h in range(self.value_heads):
            copy = remote(
                self.leave.at[h],
                self.enter.at[h],
                self.state_send.at[h],
                self.state_recv.at[h],
                "seq",
                self.follower,
            )
            self.states.append(copy)

            @pl.when(self.me > 0)
            def _():
                copy.wait_recv()

            state = self.enter[h]
            moved = mm(self.mapping[h], state)
            total = self.final[:, h : h + 1] * state.astype(jnp.float32)
            self.leave[h] = (total - moved[:DK] + self.injected[h]).astype(self.leave.dtype)
            o = self.local[h] + moved[DK:]
            scaled = (
                o * lax.rsqrt(jnp.mean(o * o, -1, keepdims=True) + EPSILON) * self.gain_ref[...]
            )
            gate = self.gate_ref[:, h * DV : (h + 1) * DV].astype(jnp.float32)
            self.gated[:, h * DV : (h + 1) * DV] = (
                scaled * (gate * jax.nn.sigmoid(gate))
            ).astype(self.gated.dtype)

            @pl.when(self.me < self.count - 1)
            def _():
                copy.start()

    def project_out(self):
        for copy in self.load_late[2:]:
            copy.wait()
        width = self.ow_ref.shape[1]
        tile = min(512, width)
        for c in range(0, width, tile):
            product = jnp.dot(
                self.gated[...],
                self.ow_ref[:, c : c + tile],
                preferred_element_type=jnp.float32,
            )
            self.summed[:, c : c + tile] = product
            self.partial[:, c : c + tile] = product.astype(self.partial.dtype)
        self.scatter = []
        for e in range(1, self.heads):
            peer = lax.rem(self.lane + e, self.heads)
            self.scatter.append(
                remote(
                    self.partial.at[self.slab_of(peer)],
                    self.landed.at[e - 1],
                    self.rs_send.at[e - 1],
                    self.rs_recv.at[e - 1],
                    "head",
                    peer,
                )
            )
        for copy in self.scatter:
            copy.start()

    def hidden_slab(self):
        for copy in self.scatter:
            copy.wait_recv()
        return self.residual_ref[...].astype(jnp.float32) + (
            self.summed[self.slab_of(self.lane)]
            + sum(self.landed[e].astype(jnp.float32) for e in range(self.heads - 1))
        )

    def gather_hidden(self, e, index):
        place = self.hidden.at[self.slab_of(index)]
        peer = lax.rem(self.lane + e, self.heads)
        return remote(
            place, place, self.ag_send.at[e - 1], self.ag_recv.at[e - 1], "head", peer
        )

    def send_hidden(self):
        for e in range(1, self.heads):
            self.gather_hidden(e, self.lane).start()

    def wait_hidden(self):
        for e in range(1, self.heads):
            self.gather_hidden(e, lax.rem(self.lane + self.heads - e, self.heads)).wait_recv()

    def scaled(self, hidden):
        widened = hidden.astype(jnp.float32)
        mean = jnp.mean(widened * widened, -1, keepdims=True)
        return (widened * lax.rsqrt(mean + EPSILON) * self.again_ref[...]).astype(jnp.bfloat16)

    def end(self):
        @pl.when(self.me < self.count - 1)
        def _():
            for copy in self.tails + self.states:
                copy.wait_send()

        for copy in self.scatter:
            copy.wait_send()
        for e in range(1, self.heads):
            self.gather_hidden(e, self.lane).wait_send()

    def attend(self, queries, keys, values, visible):
        scores = (
            lax.dot_general(
                queries, keys, (((1,), (1,)), ((), ())), preferred_element_type=jnp.float32
            )
            * HEAD_WIDTH ** (-0.5)
        )
        scores = jnp.where(visible, scores, NEGATIVE)
        peak = jnp.max(scores, -1, keepdims=True)
        weights = jnp.where(visible, jnp.exp(scores - peak), 0.0)
        norm = jnp.sum(weights, -1, keepdims=True)
        mixed = jnp.dot(weights.astype(jnp.bfloat16), values, preferred_element_type=jnp.float32)
        return mixed / norm


class Ring(Layer):
    def spot(self, block, which, half, u):
        if u == 0:
            return self.kv_spot(block, which, half)
        first = block * self.depth + which * self.piece
        return self.wq.at[u - 1, pl.ds(pl.multiple_of(first, self.piece), self.piece)]

    def along(self, d, j, u):
        sign = sign_of(d)
        block = self.clamp(self.me - sign * j)
        target = self.spot(block, self.part, self.core, u)
        source = target
        if j == 0 and u > 0:
            source = self.qw_in.at[
                pl.ds(pl.multiple_of(self.part * self.piece, self.piece), self.piece),
                pl.ds((u - 1) * 2 * HEAD_WIDTH, 2 * HEAD_WIDTH),
            ]
        copy = remote(
            source,
            target,
            self.z_send.at[d, j, u],
            self.z_recv.at[d, j, u],
            "seq",
            self.clamp(self.me + sign),
        )
        return copy, self.inside(self.me - sign * j) & self.inside(self.me + sign)

    def arriving(self, d, j, u):
        sign = sign_of(d)
        target = self.spot(self.clamp(self.me - sign * (j + 1)), self.part, self.core, u)
        copy = remote(
            target,
            target,
            self.z_send.at[d, j, u],
            self.z_recv.at[d, j, u],
            "seq",
            self.clamp(self.me + sign),
        )
        return copy, self.inside(self.me - sign * (j + 1))

    def across(self, e, d, j, u, which):
        target = self.spot(self.clamp(self.me - sign_of(d) * (j + 1)), which, self.core, u)
        return remote(
            target,
            target,
            self.y_send.at[e - 1, d, j, u],
            self.y_recv.at[e - 1, d, j, u],
            "groups",
            lax.rem(self.part + e, self.groups),
        )

    def beside(self, d, j, half):
        target = self.kv_spot(self.clamp(self.me - sign_of(d) * (j + 1)), self.part, half)
        return remote(target, target, self.m_send.at[d, j], self.m_recv.at[d, j], "head", self.mate)

    def source_of(self, e):
        return lax.rem(self.part + self.groups - e, self.groups)

    def beyond(self, e, d, j, half):
        target = self.kv_spot(self.clamp(self.me - sign_of(d) * (j + 1)), self.source_of(e), half)
        return remote(
            target,
            target,
            self.my_send.at[e - 1, d, j],
            self.my_recv.at[e - 1, d, j],
            "head",
            self.mate,
        )

    def onward(self, d, j, u):
        if j + 1 < self.count - 1:
            copy, go = self.along(d, j + 1, u)
            pl.when(go)(copy.start)

    def relay(self, d, j, u, forward=True):
        copy, here = self.arriving(d, j, u)

        @pl.when(here)
        def _():
            copy.wait_recv()
            for e in range(1, self.groups):
                self.across(e, d, j, u, self.part).start()
            if u == 0:
                self.beside(d, j, self.core).start()

        if forward:
            self.onward(d, j, u)

    def kv_relays(self, d, first, last):
        for j in range(max(first, 1), last):
            self.relay(d, j, 0)

    def share_kv(self, d, j):
        _, here = self.arriving(d, j, 0)

        @pl.when(here)
        def _():
            for e in range(1, self.groups):
                self.across(e, d, j, 0, self.source_of(e)).wait_recv()
                self.beyond(e, d, j, self.core).start()

    def wait_kv(self, d, j):
        _, here = self.arriving(d, j, 0)

        @pl.when(here)
        def _():
            self.beside(d, j, 1 - self.core).wait_recv()
            for e in range(1, self.groups):
                self.beyond(e, d, j, 1 - self.core).wait_recv()

    def end_weights(self, units):
        for j in range(self.count - 1):
            for d in range(2):
                for u in range(units):
                    copy, go = self.along(d, j, u)
                    pl.when(go)(copy.wait_send)
                _, here = self.arriving(d, j, 0)

                @pl.when(here)
                def _():
                    for e in range(1, self.groups):
                        for u in range(units):
                            self.across(e, d, j, u, self.part).wait_send()
                        self.beyond(e, d, j, self.core).wait_send()
                    self.beside(d, j, self.core).wait_send()


def ring_kernel(sizes, names, *refs):
    s = Ring(sizes, names, refs)
    count, groups, me, rows = s.count, s.groups, s.me, s.rows
    units = s.query_heads + 1
    early = min(EARLY, units)
    s.begin()
    for copy in s.load_kv:
        copy.wait()
    for u in range(units):
        for d in range(2):
            if d == 1 or u < early:
                copy, go = s.along(d, 0, u)
                pl.when(go)(copy.start)
    s.load_rest()
    load_q = [
        s.load(
            s.qw_in.at[:, pl.ds(i * 2 * HEAD_WIDTH, 2 * HEAD_WIDTH)], s.wq.at[i, s.own_rows]
        )
        for i in range(s.query_heads)
    ]

    for b in range(1, count):

        @pl.when(b > me)
        def _():
            s.kvall[:, b * rows : (b + 1) * rows] = jnp.zeros(
                (2, rows, HEAD_WIDTH), s.kvall.dtype
            )

    def pump(u):
        def run():
            if u < early:
                for d in range(2):
                    s.relay(d, 0, u, forward=d == 1)

        return run

    s.delta([lambda: None] + [pump(u) for u in range(3)])
    s.chain()
    for u in range(early, units):
        copy, go = s.along(0, 0, u)
        pl.when(go)(copy.start)
    for u in range(early):
        s.onward(0, 0, u)
    s.project_out()
    for u in range(early, units):
        for d in range(2):
            s.relay(d, 0, u)
    for d in range(2):
        s.share_kv(d, 0)
    s.hidden[s.slab_of(s.lane)] = s.hidden_slab().astype(s.hidden.dtype)
    s.send_hidden()
    for j in range(1, count - 1):
        for d in range(2):
            s.relay(d, j, 0)
    for j in range(1, count - 1):
        for d in range(2):
            s.share_kv(d, j)
    s.wait_hidden()
    save_hidden = s.load(s.hidden, s.hidden_out)
    s.normed[...] = s.scaled(s.hidden[...])

    for j in range(count - 1):
        for d in range(2):
            s.wait_kv(d, j)
    own_block = pl.ds(pl.multiple_of(me * rows, rows), rows)
    for kind in range(2):
        s.kvall[kind, own_block] = jnp.dot(
            s.normed[...],
            s.wkv[:, kind * HEAD_WIDTH : (kind + 1) * HEAD_WIDTH],
            preferred_element_type=jnp.float32,
        ).astype(s.kvall.dtype)

    def later(e, block, axis, index, kind, send, recv):
        place = s.kvall.at[kind, pl.ds(pl.multiple_of(s.clamp(block) * rows, rows), rows)]
        return remote(place, place, send.at[e - 1], recv.at[e - 1], axis, index)

    def sent_kv(e):
        return later(e, me, "seq", s.clamp(me + e), s.core, s.kv_send, s.kv_recv)

    def mate_kv(e, kind):
        return later(e, me - e, "head", s.mate, kind, s.km_send, s.km_recv)

    for e in range(1, count):
        pl.when(me + e < count)(sent_kv(e).start)

    for j in range(1, count - 1):
        for u in range(1, units):
            for d in range(2):
                if (j, u) < (count - 2, 1) or count == 2:
                    s.relay(d, j, u)

    for e in range(1, count):

        @pl.when(me >= e)
        def _():
            later(e, me - e, "seq", s.clamp(me - e), s.core, s.kv_send, s.kv_recv).wait_recv()
            mate_kv(e, s.core).start()

    for e in range(1, count):
        pl.when(me >= e)(mate_kv(e, 1 - s.core).wait_recv)

    for copy in load_q:
        copy.wait()
    keys_total = count * rows
    at_query = me * rows + lax.broadcasted_iota(jnp.int32, (rows, keys_total), 0)
    at_key = lax.broadcasted_iota(jnp.int32, (rows, keys_total), 1)
    visible = (at_key <= at_query) & (at_key < s.length_ref[0])
    for i in range(s.query_heads):
        if count > 2:
            for d in range(2):
                s.relay(d, count - 2, i + 1)
        for j in range(count - 1):
            for d in range(2):
                _, here = s.arriving(d, j, i + 1)

                @pl.when(here)
                def _():
                    for e in range(1, groups):
                        s.across(e, d, j, i + 1, s.source_of(e)).wait_recv()

        projected = jnp.dot(s.normed[...], s.wq[i], preferred_element_type=jnp.float32)
        mixed = s.attend(
            projected[:, :HEAD_WIDTH].astype(jnp.bfloat16), s.kvall[0], s.kvall[1], visible
        )
        s.attended[:, i * HEAD_WIDTH : (i + 1) * HEAD_WIDTH] = (
            mixed * jax.nn.sigmoid(projected[:, HEAD_WIDTH:])
        ).astype(s.attended.dtype)
    save_attended = s.load(s.attended, s.attention_out)

    s.end()
    s.end_weights(units)
    for e in range(1, count):
        pl.when(me + e < count)(sent_kv(e).wait_send)
        pl.when(me >= e)(mate_kv(e, s.core).wait_send)
    save_hidden.wait()
    save_attended.wait()


class Split(Ring):
    def weights(self, d, dist, p):
        sign = sign_of(d)
        peer = self.me + sign * dist
        wide = self.wq.shape[1]
        size = self.piece // PIECES
        first = pl.multiple_of(self.part * self.piece + p * size, size)
        copy = remote(
            self.qw_in.at[
                pl.ds(first, size),
                pl.ds(pl.multiple_of(self.clamp(peer) * wide, wide), wide),
            ],
            self.weight_rows(self.me, self.part, p),
            self.w_send.at[d, dist - 1, p],
            self.w_recv.at[d, dist - 1, p],
            "seq",
            self.clamp(peer),
        )
        return copy, self.inside(peer)

    def weight_rows(self, block, which, p):
        size = self.piece // PIECES
        first = self.clamp(block) * self.depth + which * self.piece + p * size
        return self.wq.at[pl.ds(pl.multiple_of(first, size), size)]

    def weights_across(self, e, d, dist, which, p):
        place = self.weight_rows(self.me - sign_of(d) * dist, which, p)
        return remote(
            place,
            place,
            self.wy_send.at[e - 1, d, dist - 1, p],
            self.wy_recv.at[e - 1, d, dist - 1, p],
            "groups",
            lax.rem(self.part + e, self.groups),
        )

    def weights_relay(self, d, dist):
        block = self.me - sign_of(d) * dist

        @pl.when(self.inside(block))
        def _():
            for p in range(PIECES):
                place = self.weight_rows(block, self.part, p)
                remote(
                    place,
                    place,
                    self.w_send.at[d, dist - 1, p],
                    self.w_recv.at[d, dist - 1, p],
                    "seq",
                    self.clamp(block),
                ).wait_recv()
                for e in range(1, self.groups):
                    self.weights_across(e, d, dist, self.part, p).start()

    def weights_wait(self, d, dist):
        @pl.when(self.inside(self.me - sign_of(d) * dist))
        def _():
            for e in range(1, self.groups):
                for p in range(PIECES):
                    self.weights_across(e, d, dist, self.source_of(e), p).wait_recv()


    def place(self, block, index):
        first = block * self.rows + index * self.slab
        return self.every.at[pl.ds(pl.multiple_of(first, self.slab), self.slab)]

    def far(self, d, dist, block):
        place = self.place(self.clamp(block), self.lane)
        return remote(
            place,
            place,
            self.n_send.at[d, dist],
            self.n_recv.at[d, dist],
            "seq",
            self.clamp(self.me + sign_of(d)),
        )

    def rows_onward(self, d, dist):
        block = self.me - sign_of(d) * dist
        go = self.inside(block) & self.inside(self.me + sign_of(d))
        return self.far(d, dist, block), go

    def near(self, d, dist, f, block, index):
        place = self.place(self.clamp(block), index)
        peer = lax.rem(self.lane + MATES * f, self.heads)
        return remote(
            place,
            place,
            self.x_send.at[d, dist, f - 1],
            self.x_recv.at[d, dist, f - 1],
            "head",
            peer,
        )

    def twin(self, d, dist, f, block, index):
        place = self.place(self.clamp(block), index)
        return remote(
            place, place, self.t_send.at[d, dist, f], self.t_recv.at[d, dist, f], "head", self.mate
        )

    def back(self, f, lane):
        return lax.rem(lane + self.heads - MATES * f, self.heads)

    def chips(self):
        return range(1, self.heads // MATES)

    def block_at(self, d, dist):
        return self.me - sign_of(d) * dist

    def steps(self, dist):
        return (0,) if dist == 0 else (0, 1)

    def rows_sent(self, d, dist):
        block = self.block_at(d, dist)

        @pl.when(self.inside(block))
        def _():
            if dist > 0:
                self.far(d, dist - 1, block).wait_recv()
            for f in self.chips():
                self.near(d, dist, f, block, self.lane).start()
            self.twin(d, dist, 0, block, self.lane).start()

        if 0 < dist < self.count - 1:
            copy, go = self.rows_onward(d, dist)
            pl.when(go)(copy.start)

    def rows_passed(self, d, dist):
        block = self.block_at(d, dist)

        @pl.when(self.inside(block))
        def _():
            for f in self.chips():
                self.near(d, dist, f, block, self.back(f, self.lane)).wait_recv()
                self.twin(d, dist, f, block, self.back(f, self.lane)).start()

    def rows_ready(self, d, dist, block):
        for f in range(self.heads // MATES):
            self.twin(d, dist, f, block, self.back(f, self.mate)).wait_recv()

    def end_rows(self):
        for dist in range(self.count - 1):
            for d in range(2):
                copy, go = self.rows_onward(d, dist)
                pl.when(go)(copy.wait_send)
        for dist in range(self.count):
            for d in self.steps(dist):
                block = self.block_at(d, dist)

                @pl.when(self.inside(block))
                def _():
                    for f in self.chips():
                        self.near(d, dist, f, block, self.lane).wait_send()
                    for f in range(self.heads // MATES):
                        self.twin(d, dist, f, block, self.back(f, self.lane)).wait_send()


def split_kernel(sizes, names, *refs):
    s = Split(sizes, names, refs)
    count, groups, me, rows = s.count, s.groups, s.me, s.rows
    wide = s.wq.shape[1]
    mine = wide // (2 * HEAD_WIDTH)
    s.begin()
    last = count - 1

    def send_weights(d, dist):
        for p in range(PIECES):
            copy, go = s.weights(d, dist, p)
            pl.when(go)(copy.start)

    for copy in s.load_kv:
        copy.wait()
    for d in range(2):
        copy, go = s.along(d, 0, 0)
        pl.when(go)(copy.start)
    pl.when(me > 0)(functools.partial(send_weights, 0, 1))
    s.load_rest()
    load_q = s.load(
        s.qw_in.at[:, pl.ds(pl.multiple_of(me * wide, wide), wide)], s.wq.at[s.own_rows]
    )

    def pump_heads():
        @pl.when(me > 0)
        def _():
            s.relay(0, 0, 0, forward=False)
            s.relay(1, 0, 0)
            send_weights(1, 1)

    def pump_updates():
        @pl.when(me > 0)
        def _():
            for j in range(1, last - 1):
                s.relay(1, j, 0)

        pl.when(me > 1)(functools.partial(s.weights_relay, 0, 1))
        for dist in range(2, count):
            send_weights(1, dist)

    s.delta([pump_heads, lambda: None, lambda: None, pump_updates])
    s.chain()
    s.onward(0, 0, 0)
    s.project_out()
    s.kv_relays(0, 1, last - 1)
    for dist in range(1, last):
        pl.when(me == dist)(functools.partial(s.rows_sent, 0, dist))
    hidden = s.hidden_slab().astype(s.hidden.dtype)
    s.hidden[s.slab_of(s.lane)] = hidden
    s.every[pl.ds(pl.multiple_of(me * rows + s.lane * s.slab, s.slab), s.slab)] = s.scaled(hidden)
    for d in range(2):
        copy, go = s.rows_onward(d, 0)
        pl.when(go)(copy.start)
    s.rows_sent(0, 0)

    def send_far():
        for dist in range(last, 1, -1):
            send_weights(0, dist)

    def far_weights(d):
        for dist in range(last - 1, 1, -1):
            s.weights_relay(d, dist)

    pl.when((me != 1) & (me != last))(functools.partial(s.rows_sent, 0, 1))

    @pl.when(me == 0)
    def _():
        send_weights(0, 1)
        s.relay(1, 0, 0)

    pl.when(me == 1)(functools.partial(s.weights_relay, 0, 1))
    s.weights_relay(1, 1)
    pl.when(me > 0)(send_far)
    for d in range(2):
        s.share_kv(d, 0)
    pl.when(me == 0)(functools.partial(s.kv_relays, 1, 1, last - 1))
    for d in range(2):
        s.kv_relays(d, last - 1, last)
    pl.when(me > 0)(functools.partial(far_weights, 1))
    if last > 1:
        s.rows_sent(0, last)
    s.rows_passed(0, 0)

    @pl.when(me == 0)
    def _():
        s.weights_relay(1, last)
        send_far()

    if last > 1:
        s.weights_relay(0, last)
    pl.when(me == last)(functools.partial(s.rows_sent, 0, 1))
    s.rows_sent(1, 1)
    for j in range(1, last):
        for d in range(2):
            s.share_kv(d, j)
    if last > 1:
        s.rows_passed(0, last)
    far_weights(0)
    for dist in range(2, last):
        pl.when(me != dist)(functools.partial(s.rows_sent, 0, dist))
    pl.when(me == 0)(functools.partial(far_weights, 1))
    for dist in range(2, last):
        s.rows_sent(1, dist)
    s.rows_passed(0, 1)
    s.rows_passed(1, 1)
    for dist in range(2, last):
        s.rows_passed(0, dist)
    if last > 1:
        s.rows_sent(1, last)
    for dist in range(2, last):
        s.rows_passed(1, dist)

    def project(first, size):
        at = pl.ds(pl.multiple_of(first, rows), size)
        x = s.every[at]
        for i in range(mine):
            first = i * 2 * HEAD_WIDTH
            query = jnp.dot(
                x, s.wq[:, first : first + HEAD_WIDTH], preferred_element_type=jnp.float32
            )
            gate = jnp.dot(
                x,
                s.wq[:, first + HEAD_WIDTH : first + 2 * HEAD_WIDTH],
                preferred_element_type=jnp.float32,
            )
            s.asked[i, at] = query.astype(jnp.bfloat16)
            s.opened[i, at] = jax.nn.sigmoid(gate)
        for kind in range(2):
            s.kvall[kind, at] = jnp.dot(
                x,
                s.wkv[:, kind * HEAD_WIDTH : (kind + 1) * HEAD_WIDTH],
                preferred_element_type=jnp.float32,
            ).astype(s.kvall.dtype)

    upper = 2 * me >= count

    def ready(far):
        for dist in range(count):
            for d in s.steps(dist):
                block = s.block_at(d, dist)
                end = jnp.where(upper, 0, last)
                wanted = block == end if far else block != end

                @pl.when(s.inside(block) & wanted)
                def _():
                    s.rows_ready(d, dist, block)

    s.send_hidden()
    for j in range(last):
        for d in range(2):
            s.wait_kv(d, j)
    load_q.wait()
    for dist in range(1, count):
        for d in range(2):
            s.weights_wait(d, dist)
    ready(False)
    project(jnp.where(upper, rows, 0), last * rows)
    if last > 1:
        s.rows_passed(1, last)
    ready(True)
    project(jnp.where(upper, 0, last * rows), rows)

    span = mine * HEAD_WIDTH
    length = s.length_ref[0]

    def result(b, rank):
        return remote(
            s.attended.at[b],
            s.attention_out.at[:, pl.ds(pl.multiple_of(rank * span, span), span)],
            s.r_send.at[b],
            s.r_recv.at[rank],
            "seq",
            b,
        )

    for b in range(count):
        seen = (b + 1) * rows
        at_query = b * rows + lax.broadcasted_iota(jnp.int32, (rows, seen), 0)
        at_key = lax.broadcasted_iota(jnp.int32, (rows, seen), 1)
        visible = (at_key <= at_query) & (at_key < length)
        at = slice(b * rows, seen)
        for i in range(mine):
            mixed = s.attend(s.asked[i, at], s.kvall[0, :seen], s.kvall[1, :seen], visible)
            s.attended[b, :, i * HEAD_WIDTH : (i + 1) * HEAD_WIDTH] = (
                mixed * s.opened[i, at]
            ).astype(s.attended.dtype)

        @pl.when(me != b)
        def _():
            result(b, me).start()

    own = s.load(
        s.attended.at[me],
        s.attention_out.at[:, pl.ds(pl.multiple_of(me * span, span), span)],
    )
    s.wait_hidden()
    save_hidden = s.load(s.hidden, s.hidden_out)
    for b in range(count):
        pl.when(me != b)(result(b, jnp.int32(b)).wait_recv)

    for b in range(count):
        pl.when(me != b)(result(b, me).wait_send)
    s.end()
    s.end_weights(1)
    s.end_rows()
    for dist in range(1, count):
        for d in range(2):
            for p in range(PIECES):
                copy, go = s.weights(d, dist, p)
                pl.when(go)(copy.wait_send)

            @pl.when(s.inside(me - sign_of(d) * dist))
            def _():
                for e in range(1, groups):
                    for p in range(PIECES):
                        s.weights_across(e, d, dist, s.part, p).wait_send()

    save_hidden.wait()
    own.wait()


def shards(
    residual,
    query_in,
    key_in,
    value_in,
    gating_in,
    beta_logit,
    decay_logit,
    seq_length,
    conv_query,
    conv_key,
    conv_value,
    decay_rate,
    norm_gain,
    out_weight,
    attn_gain,
    query_weight,
    key_value_weight,
):
    count = lax.axis_size("seq")
    groups = lax.axis_size("groups")
    heads = lax.axis_size("head")
    rows, model = residual.shape
    value_heads = beta_logit.shape[1]
    query_heads = query_weight.shape[1] // (2 * HEAD_WIDTH)
    width = query_in.shape[1] + key_in.shape[1] + value_in.shape[1]
    depth = query_weight.shape[0] * count
    slab = rows // heads
    f32, bf16 = jnp.float32, jnp.bfloat16
    dma = pltpu.SemaphoreType.DMA
    anywhere = pl.BlockSpec(memory_space=pl.ANY)
    smem = pl.BlockSpec(memory_space=pltpu.SMEM)
    rate = decay_rate[None, :]
    beta_t, decay_t = beta_logit.T, decay_logit.T
    gain = norm_gain[None, :]
    attn = attn_gain[None, :]
    like = lambda a: pltpu.VMEM(a.shape, a.dtype)
    split = query_heads % count == 0
    units = 1 if split else query_heads + 1
    scratch = dict(
        q_ref=like(query_in),
        k_ref=like(key_in),
        v_ref=like(value_in),
        gate_ref=like(gating_in),
        beta_ref=like(beta_t),
        decay_ref=like(decay_t),
        cq_ref=like(conv_query),
        ck_ref=like(conv_key),
        cv_ref=like(conv_value),
        rate_ref=like(rate),
        gain_ref=like(gain),
        ow_ref=like(out_weight),
        again_ref=like(attn),
        residual_ref=pltpu.VMEM((slab, model), bf16),
        wkv=pltpu.VMEM((depth, 2 * HEAD_WIDTH), bf16),
        tail_q=pltpu.VMEM((TAIL, query_in.shape[1]), bf16),
        tail_k=pltpu.VMEM((TAIL, key_in.shape[1]), bf16),
        tail_v=pltpu.VMEM((TAIL, value_in.shape[1]), bf16),
        joined=pltpu.VMEM((rows + PAD, width), f32),
        mapping=pltpu.VMEM((value_heads, DK + rows, DK), bf16),
        local=pltpu.VMEM((value_heads, rows, DV), f32),
        injected=pltpu.VMEM((value_heads, DK, DV), f32),
        enter=pltpu.VMEM((value_heads, DK, DV), bf16),
        leave=pltpu.VMEM((value_heads, DK, DV), bf16),
        gated=pltpu.VMEM((rows, value_heads * DV), bf16),
        summed=pltpu.VMEM((rows, model), f32),
        partial=pltpu.VMEM((rows, model), bf16),
        landed=pltpu.VMEM((heads - 1, slab, model), bf16),
        hidden=pltpu.VMEM((rows, model), bf16),
        kvall=pltpu.VMEM((2, count * rows, HEAD_WIDTH), bf16),
        load_sems=dma((24 + query_heads,)),
        tail_send=dma((3,)),
        tail_recv=dma((3,)),
        state_send=dma((value_heads,)),
        state_recv=dma((value_heads,)),
        z_send=dma((2, count - 1, units)),
        z_recv=dma((2, count - 1, units)),
        y_send=dma((groups - 1, 2, count - 1, units)),
        y_recv=dma((groups - 1, 2, count - 1, units)),
        m_send=dma((2, count - 1)),
        m_recv=dma((2, count - 1)),
        my_send=dma((groups - 1, 2, count - 1)),
        my_recv=dma((groups - 1, 2, count - 1)),
        rs_send=dma((heads - 1,)),
        rs_recv=dma((heads - 1,)),
        ag_send=dma((heads - 1,)),
        ag_recv=dma((heads - 1,)),
    )
    if split:
        mine = query_heads // count
        chips = heads // MATES
        scratch.update(
            wq=pltpu.VMEM((depth, mine * 2 * HEAD_WIDTH), bf16),
            every=pltpu.VMEM((count * rows, model), bf16),
            asked=pltpu.VMEM((mine, count * rows, HEAD_WIDTH), bf16),
            opened=pltpu.VMEM((mine, count * rows, HEAD_WIDTH), f32),
            attended=pltpu.VMEM((count, rows, mine * HEAD_WIDTH), bf16),
            w_send=dma((2, count - 1, PIECES)),
            w_recv=dma((2, count - 1, PIECES)),
            wy_send=dma((groups - 1, 2, count - 1, PIECES)),
            wy_recv=dma((groups - 1, 2, count - 1, PIECES)),
            n_send=dma((2, count - 1)),
            n_recv=dma((2, count - 1)),
            x_send=dma((2, count, chips - 1)),
            x_recv=dma((2, count, chips - 1)),
            t_send=dma((2, count, chips)),
            t_recv=dma((2, count, chips)),
            r_send=dma((count,)),
            r_recv=dma((count,)),
        )
    else:
        scratch.update(
            wq=pltpu.VMEM((query_heads, depth, 2 * HEAD_WIDTH), bf16),
            normed=pltpu.VMEM((rows, model), bf16),
            attended=pltpu.VMEM((rows, query_heads * HEAD_WIDTH), bf16),
            kv_send=dma((count - 1,)),
            kv_recv=dma((count - 1,)),
            km_send=dma((count - 1,)),
            km_recv=dma((count - 1,)),
        )
    return pl.pallas_call(
        functools.partial(
            split_kernel if split else ring_kernel,
            (count, groups, heads),
            INPUTS + OUTPUTS + list(scratch),
        ),
        out_shape=(
            jax.ShapeDtypeStruct(residual.shape, bf16),
            jax.ShapeDtypeStruct((rows, query_heads * HEAD_WIDTH), bf16),
        ),
        in_specs=[anywhere] * 7 + [smem] + [anywhere] * 9,
        out_specs=(anywhere, anywhere),
        scratch_shapes=list(scratch.values()),
        compiler_params=pltpu.CompilerParams(
            collective_id=0, has_side_effects=True, vmem_limit_bytes=56 * 2**20
        ),
        name="layer",
    )(
        residual,
        query_in,
        key_in,
        value_in,
        gating_in,
        beta_t,
        decay_t,
        seq_length,
        conv_query,
        conv_key,
        conv_value,
        rate,
        gain,
        out_weight,
        attn,
        query_weight,
        key_value_weight,
    )


def solution(mesh):
    placed = (
        P(("groups", "seq"), None),
        P(("groups", "seq"), "head"),
        P(("groups", "seq"), "head"),
        P(("groups", "seq"), "head"),
        P(("groups", "seq"), "head"),
        P(("groups", "seq"), "head"),
        P(("groups", "seq"), "head"),
        P("groups"),
        P(None, "head"),
        P(None, "head"),
        P(None, "head"),
        P("head"),
        P(),
        P("head", None),
        P(),
        P("seq", "head"),
        P("seq", None),
    )
    return jax.shard_map(
        shards,
        mesh=mesh,
        in_specs=placed,
        out_specs=(P(("groups", "seq"), None), P(("groups", "seq"), "head")),
        check_vma=False,
    )
```

```python
import functools

import jax
import jax.numpy as jnp
from jax import lax
from jax.experimental import pallas as pl
from jax.experimental.pallas import tpu as pltpu
from jax.sharding import PartitionSpec as P

DK = 128
DV = 128
QUERY_HEADS = 16
KEY_VALUE_HEADS = 2
HEAD_WIDTH = 256
CONV = 4
PAD = 8
TAIL = 8
MATES = 2
EARLY = 3
PIECES = 2

EPSILON = 1e-06
NEGATIVE = -1e30
MESH = pl.DeviceIdType.MESH
HIGHEST = lax.Precision.HIGHEST


def exact(a, b, contract=((1,), (0,))):
    return lax.dot_general(
        a, b, (contract, ((), ())), precision=HIGHEST, preferred_element_type=jnp.float32
    )


def mm(a, b, contract=((1,), (0,))):
    return lax.dot_general(
        a.astype(jnp.bfloat16),
        b.astype(jnp.bfloat16),
        (contract, ((), ())),
        preferred_element_type=jnp.float32,
    )


def softplus(x):
    return jnp.maximum(x, 0.0) + jnp.log1p(jnp.exp(-jnp.abs(x)))


def unit(x):
    return x / jnp.sqrt(jnp.sum(x * x, -1, keepdims=True) + EPSILON)


INPUTS = [
    "residual_in",
    "q_in",
    "k_in",
    "v_in",
    "gate_in",
    "beta_in",
    "decay_in",
    "length_ref",
    "cq_in",
    "ck_in",
    "cv_in",
    "rate_in",
    "gain_in",
    "ow_in",
    "again_in",
    "qw_in",
    "kvw_in",
]
OUTPUTS = ["hidden_out", "attention_out"]


def remote(source, target, send, recv, axis, index):
    return pltpu.make_async_remote_copy(
        src_ref=source,
        dst_ref=target,
        send_sem=send,
        recv_sem=recv,
        device_id={axis: index},
        device_id_type=MESH,
    )


def sign_of(d):
    return 1 if d == 0 else -1


class Layer:
    def __init__(self, sizes, names, refs):
        self.count, self.groups, self.heads = sizes
        for name, ref in zip(names, refs, strict=True):
            setattr(self, name, ref)
        self.me = lax.axis_index("seq")
        self.part = lax.axis_index("groups")
        self.lane = lax.axis_index("head")
        self.core = lax.rem(self.lane, MATES)
        self.mate = self.lane + 1 - 2 * self.core
        self.rows = self.q_ref.shape[0]
        self.key_heads = self.q_ref.shape[1] // DK
        self.value_heads = self.v_ref.shape[1] // DV
        self.share = self.value_heads // self.key_heads
        self.depth = self.qw_in.shape[0]
        self.piece = self.depth // self.groups
        self.quarter = self.piece // MATES
        self.slab = self.rows // self.heads
        self.query_heads = self.qw_in.shape[1] // (2 * HEAD_WIDTH)
        self.kv_head = self.lane * self.query_heads // (QUERY_HEADS // KEY_VALUE_HEADS)
        self.own_rows = pl.ds(pl.multiple_of(self.me * self.depth, self.depth), self.depth)
        self.follower = self.clamp(self.me + 1)
        self.loads = 0

    def load(self, source, target):
        copy = pltpu.make_async_copy(source, target, self.load_sems.at[self.loads])
        copy.start()
        self.loads += 1
        return copy

    def inside(self, block):
        return (block >= 0) & (block < self.count)

    def clamp(self, block):
        return jnp.clip(block, 0, self.count - 1)

    def slab_of(self, index):
        return pl.ds(pl.multiple_of(index * self.slab, self.slab), self.slab)


    def kv_spot(self, block, which, half):
        first = block * self.depth + which * self.piece + half * self.quarter
        return self.wkv.at[pl.ds(pl.multiple_of(first, self.quarter), self.quarter)]

    def begin(self):
        load = self.load
        self.load_kv = [
            load(
                self.kvw_in.at[
                    :,
                    pl.ds(
                        pl.multiple_of(
                            (kind * KEY_VALUE_HEADS + self.kv_head) * HEAD_WIDTH, HEAD_WIDTH
                        ),
                        HEAD_WIDTH,
                    ),
                ],
                self.wkv.at[self.own_rows, pl.ds(kind * HEAD_WIDTH, HEAD_WIDTH)],
            )
            for kind in range(2)
        ]
        self.load_decay = [
            load(self.decay_in, self.decay_ref),
            load(self.rate_in, self.rate_ref),
            load(self.beta_in, self.beta_ref),
        ]
        self.load_conv = [
            load(self.q_in, self.q_ref),
            load(self.k_in, self.k_ref),
            load(self.v_in, self.v_ref),
            load(self.cq_in, self.cq_ref),
            load(self.ck_in, self.ck_ref),
            load(self.cv_in, self.cv_ref),
        ]

        barrier = pltpu.get_barrier_semaphore()
        for axis, size, place in (
            ("seq", self.count, self.me),
            ("groups", self.groups, self.part),
            ("head", self.heads, self.lane),
        ):
            for e in range(1, size):
                pl.semaphore_signal(
                    barrier,
                    inc=1,
                    device_id={axis: lax.rem(place + e, size)},
                    device_id_type=MESH,
                )
        pl.semaphore_wait(barrier, self.count + self.groups + self.heads - 3)

        last = pl.ds(self.rows - TAIL, TAIL)
        self.tails = [
            remote(
                source.at[last],
                target,
                self.tail_send.at[i],
                self.tail_recv.at[i],
                "seq",
                self.follower,
            )
            for i, (source, target) in enumerate(
                (
                    (self.q_in, self.tail_q),
                    (self.k_in, self.tail_k),
                    (self.v_in, self.tail_v),
                )
            )
        ]

        @pl.when(self.me < self.count - 1)
        def _():
            for copy in self.tails:
                copy.start()

    def load_rest(self):
        load = self.load
        self.load_late = [
            load(self.gate_in, self.gate_ref),
            load(self.gain_in, self.gain_ref),
            load(self.ow_in, self.ow_ref),
            load(self.residual_in.at[self.slab_of(self.lane)], self.residual_ref),
            load(self.again_in, self.again_ref),
        ]

    def delta(self, pumps):
        rows, value_heads, share = self.rows, self.value_heads, self.share
        key_heads = self.key_heads
        for copy in self.load_decay:
            copy.wait()
        length = self.length_ref[0]
        at = self.me * rows + lax.broadcasted_iota(jnp.int32, (value_heads, rows), 1)
        alive = (at < length).astype(jnp.float32)
        beta_t = jax.nn.sigmoid(self.beta_ref[...]) * alive
        square = (value_heads, value_heads)
        diagonal = lax.broadcasted_iota(jnp.int32, square, 0) == lax.broadcasted_iota(
            jnp.int32, square, 1
        )
        rate = jnp.sum(jnp.where(diagonal, self.rate_ref[...], 0.0), -1, keepdims=True)
        step_t = -rate * softplus(self.decay_ref[...]) * alive
        row = lax.broadcasted_iota(jnp.int32, (rows, rows), 0)
        column = lax.broadcasted_iota(jnp.int32, (rows, rows), 1)
        inclusive = row >= column
        run_t = exact(step_t, (row <= column).astype(jnp.float32))
        blank = jnp.zeros((rows - 2 * value_heads, rows), jnp.float32)
        turned_over = jnp.concatenate([beta_t, run_t, blank], 0).T
        beta = turned_over[:, :value_heads]
        run = turned_over[:, value_heads : 2 * value_heads]
        growth = jnp.exp(run)
        self.final = growth[rows - 1 : rows]
        ending_t = jnp.exp(run_t[:, rows - 1 : rows] - run_t)
        eye = (row == column).astype(jnp.float32)

        for copy in self.load_conv:
            copy.wait()
        q_width = key_heads * DK
        joined = self.joined
        joined[PAD:, :q_width] = self.q_ref[...].astype(jnp.float32)
        joined[PAD:, q_width : 2 * q_width] = self.k_ref[...].astype(jnp.float32)
        joined[PAD:, 2 * q_width :] = self.v_ref[...].astype(jnp.float32)

        @pl.when(self.me == 0)
        def _():
            self.enter[...] = jnp.zeros_like(self.enter)
            joined[:PAD] = jnp.zeros((PAD, joined.shape[1]), jnp.float32)

        @pl.when(self.me > 0)
        def _():
            for copy in self.tails:
                copy.wait_recv()
            joined[:PAD, :q_width] = self.tail_q[...].astype(jnp.float32)[TAIL - PAD :]
            joined[:PAD, q_width : 2 * q_width] = self.tail_k[...].astype(jnp.float32)[
                TAIL - PAD :
            ]
            joined[:PAD, 2 * q_width :] = self.tail_v[...].astype(jnp.float32)[TAIL - PAD :]

        def conv(base, taps, h):
            first_column = base + h * DK
            total = jnp.zeros((rows, DK), jnp.float32)
            for j in range(CONV):
                first = PAD - CONV + 1 + j
                total = total + taps[j : j + 1, h * DK : (h + 1) * DK] * joined[
                    first : first + rows, first_column : first_column + DK
                ]
            return total * jax.nn.sigmoid(total)

        queries, keyset, turned, grams = [], [], [], []
        for g in range(key_heads):
            q = unit(conv(0, self.cq_ref, g)) * DK ** (-0.5)
            k = unit(conv(q_width, self.ck_ref, g))
            k_t = k.T
            queries.append(q)
            keyset.append(k)
            turned.append(k_t)
            grams.append(mm(jnp.concatenate([k, q], 0), k_t))
            if g == key_heads // 2 - 1:
                pumps[0]()
        pumps[1]()

        mixes, lower, inverse = [], [], []
        for h in range(value_heads):
            spread = run[:, h : h + 1] - run_t[h : h + 1, :]
            w = jnp.exp(jnp.where(inclusive, spread, NEGATIVE))
            gram = grams[h // share]
            mixes.append((gram[rows:] * w).astype(jnp.bfloat16))
            low = jnp.where(row > column, beta[:, h : h + 1] * w * gram[:rows], 0.0)
            lower.append(low)
            pair = (row // 2 == column // 2) & (row > column)
            inverse.append(eye - jnp.where(pair, low, 0.0))
        size = 2
        while size < rows:
            off = (row // (2 * size) == column // (2 * size)) & (row // size > column // size)
            half = [mm(jnp.where(off, low, 0.0), x) for low, x in zip(lower, inverse)]
            inverse = [x - mm(x, y) for x, y in zip(inverse, half)]
            size *= 2
        pumps[2]()

        for h in range(value_heads):
            k = keyset[h // share]
            v = conv(2 * q_width, self.cv_ref, h)
            b = beta[:, h : h + 1]
            grown = growth[:, h : h + 1]
            wu = mm(inverse[h], jnp.concatenate([b * grown * k, b * v], 1))
            stop_t = (turned[h // share] * ending_t[h : h + 1, :]).astype(jnp.bfloat16)
            both = mm(jnp.concatenate([stop_t, mixes[h]], 0), wu)
            self.mapping[h, :DK] = both[:DK, :DK].astype(jnp.bfloat16)
            self.mapping[h, DK:] = (grown * queries[h // share] - both[DK:, :DK]).astype(
                jnp.bfloat16
            )
            self.injected[h] = both[:DK, DK:]
            self.local[h] = both[DK:, DK:]
        pumps[3]()

    def chain(self):
        for copy in self.load_late[:2]:
            copy.wait()
        self.states = []
        for h in range(self.value_heads):
            copy = remote(
                self.leave.at[h],
                self.enter.at[h],
                self.state_send.at[h],
                self.state_recv.at[h],
                "seq",
                self.follower,
            )
            self.states.append(copy)

            @pl.when(self.me > 0)
            def _():
                copy.wait_recv()

            state = self.enter[h]
            moved = mm(self.mapping[h], state)
            total = self.final[:, h : h + 1] * state.astype(jnp.float32)
            self.leave[h] = (total - moved[:DK] + self.injected[h]).astype(self.leave.dtype)
            o = self.local[h] + moved[DK:]
            scaled = (
                o * lax.rsqrt(jnp.mean(o * o, -1, keepdims=True) + EPSILON) * self.gain_ref[...]
            )
            gate = self.gate_ref[:, h * DV : (h + 1) * DV].astype(jnp.float32)
            self.gated[:, h * DV : (h + 1) * DV] = (
                scaled * (gate * jax.nn.sigmoid(gate))
            ).astype(self.gated.dtype)

            @pl.when(self.me < self.count - 1)
            def _():
                copy.start()

    def project_out(self):
        for copy in self.load_late[2:]:
            copy.wait()
        width = self.ow_ref.shape[1]
        tile = min(512, width)
        for c in range(0, width, tile):
            product = jnp.dot(
                self.gated[...],
                self.ow_ref[:, c : c + tile],
                preferred_element_type=jnp.float32,
            )
            self.summed[:, c : c + tile] = product
            self.partial[:, c : c + tile] = product.astype(self.partial.dtype)
        self.scatter = []
        for e in range(1, self.heads):
            peer = lax.rem(self.lane + e, self.heads)
            self.scatter.append(
                remote(
                    self.partial.at[self.slab_of(peer)],
                    self.landed.at[e - 1],
                    self.rs_send.at[e - 1],
                    self.rs_recv.at[e - 1],
                    "head",
                    peer,
                )
            )
        for copy in self.scatter:
            copy.start()

    def hidden_slab(self):
        for copy in self.scatter:
            copy.wait_recv()
        return self.residual_ref[...].astype(jnp.float32) + (
            self.summed[self.slab_of(self.lane)]
            + sum(self.landed[e].astype(jnp.float32) for e in range(self.heads - 1))
        )

    def gather_hidden(self, e, index):
        place = self.hidden.at[self.slab_of(index)]
        peer = lax.rem(self.lane + e, self.heads)
        return remote(
            place, place, self.ag_send.at[e - 1], self.ag_recv.at[e - 1], "head", peer
        )

    def send_hidden(self):
        for e in range(1, self.heads):
            self.gather_hidden(e, self.lane).start()

    def wait_hidden(self):
        for e in range(1, self.heads):
            self.gather_hidden(e, lax.rem(self.lane + self.heads - e, self.heads)).wait_recv()

    def scaled(self, hidden):
        widened = hidden.astype(jnp.float32)
        mean = jnp.mean(widened * widened, -1, keepdims=True)
        return (widened * lax.rsqrt(mean + EPSILON) * self.again_ref[...]).astype(jnp.bfloat16)

    def end(self):
        @pl.when(self.me < self.count - 1)
        def _():
            for copy in self.tails + self.states:
                copy.wait_send()

        for copy in self.scatter:
            copy.wait_send()
        for e in range(1, self.heads):
            self.gather_hidden(e, self.lane).wait_send()

    def attend(self, queries, keys, values, visible):
        scores = (
            lax.dot_general(
                queries, keys, (((1,), (1,)), ((), ())), preferred_element_type=jnp.float32
            )
            * HEAD_WIDTH ** (-0.5)
        )
        scores = jnp.where(visible, scores, NEGATIVE)
        peak = jnp.max(scores, -1, keepdims=True)
        weights = jnp.where(visible, jnp.exp(scores - peak), 0.0)
        norm = jnp.sum(weights, -1, keepdims=True)
        mixed = jnp.dot(weights.astype(jnp.bfloat16), values, preferred_element_type=jnp.float32)
        return mixed / norm


class Ring(Layer):
    def spot(self, block, which, half, u):
        if u == 0:
            return self.kv_spot(block, which, half)
        first = block * self.depth + which * self.piece
        return self.wq.at[u - 1, pl.ds(pl.multiple_of(first, self.piece), self.piece)]

    def along(self, d, j, u):
        sign = sign_of(d)
        block = self.clamp(self.me - sign * j)
        target = self.spot(block, self.part, self.core, u)
        source = target
        if j == 0 and u > 0:
            source = self.qw_in.at[
                pl.ds(pl.multiple_of(self.part * self.piece, self.piece), self.piece),
                pl.ds((u - 1) * 2 * HEAD_WIDTH, 2 * HEAD_WIDTH),
            ]
        copy = remote(
            source,
            target,
            self.z_send.at[d, j, u],
            self.z_recv.at[d, j, u],
            "seq",
            self.clamp(self.me + sign),
        )
        return copy, self.inside(self.me - sign * j) & self.inside(self.me + sign)

    def arriving(self, d, j, u):
        sign = sign_of(d)
        target = self.spot(self.clamp(self.me - sign * (j + 1)), self.part, self.core, u)
        copy = remote(
            target,
            target,
            self.z_send.at[d, j, u],
            self.z_recv.at[d, j, u],
            "seq",
            self.clamp(self.me + sign),
        )
        return copy, self.inside(self.me - sign * (j + 1))

    def across(self, e, d, j, u, which):
        target = self.spot(self.clamp(self.me - sign_of(d) * (j + 1)), which, self.core, u)
        return remote(
            target,
            target,
            self.y_send.at[e - 1, d, j, u],
            self.y_recv.at[e - 1, d, j, u],
            "groups",
            lax.rem(self.part + e, self.groups),
        )

    def beside(self, d, j, half):
        target = self.kv_spot(self.clamp(self.me - sign_of(d) * (j + 1)), self.part, half)
        return remote(target, target, self.m_send.at[d, j], self.m_recv.at[d, j], "head", self.mate)

    def source_of(self, e):
        return lax.rem(self.part + self.groups - e, self.groups)

    def beyond(self, e, d, j, half):
        target = self.kv_spot(self.clamp(self.me - sign_of(d) * (j + 1)), self.source_of(e), half)
        return remote(
            target,
            target,
            self.my_send.at[e - 1, d, j],
            self.my_recv.at[e - 1, d, j],
            "head",
            self.mate,
        )

    def onward(self, d, j, u):
        if j + 1 < self.count - 1:
            copy, go = self.along(d, j + 1, u)
            pl.when(go)(copy.start)

    def relay(self, d, j, u, forward=True):
        copy, here = self.arriving(d, j, u)

        @pl.when(here)
        def _():
            copy.wait_recv()
            for e in range(1, self.groups):
                self.across(e, d, j, u, self.part).start()
            if u == 0:
                self.beside(d, j, self.core).start()

        if forward:
            self.onward(d, j, u)

    def kv_relays(self, d, first, last):
        for j in range(max(first, 1), last):
            self.relay(d, j, 0)

    def share_kv(self, d, j):
        _, here = self.arriving(d, j, 0)

        @pl.when(here)
        def _():
            for e in range(1, self.groups):
                self.across(e, d, j, 0, self.source_of(e)).wait_recv()
                self.beyond(e, d, j, self.core).start()

    def wait_kv(self, d, j):
        _, here = self.arriving(d, j, 0)

        @pl.when(here)
        def _():
            self.beside(d, j, 1 - self.core).wait_recv()
            for e in range(1, self.groups):
                self.beyond(e, d, j, 1 - self.core).wait_recv()

    def end_weights(self, units):
        for j in range(self.count - 1):
            for d in range(2):
                for u in range(units):
                    copy, go = self.along(d, j, u)
                    pl.when(go)(copy.wait_send)
                _, here = self.arriving(d, j, 0)

                @pl.when(here)
                def _():
                    for e in range(1, self.groups):
                        for u in range(units):
                            self.across(e, d, j, u, self.part).wait_send()
                        self.beyond(e, d, j, self.core).wait_send()
                    self.beside(d, j, self.core).wait_send()


def ring_kernel(sizes, names, *refs):
    s = Ring(sizes, names, refs)
    count, groups, me, rows = s.count, s.groups, s.me, s.rows
    units = s.query_heads + 1
    early = min(EARLY, units)
    s.begin()
    for copy in s.load_kv:
        copy.wait()
    for u in range(units):
        for d in range(2):
            if d == 1 or u < early:
                copy, go = s.along(d, 0, u)
                pl.when(go)(copy.start)
    s.load_rest()
    load_q = [
        s.load(
            s.qw_in.at[:, pl.ds(i * 2 * HEAD_WIDTH, 2 * HEAD_WIDTH)], s.wq.at[i, s.own_rows]
        )
        for i in range(s.query_heads)
    ]

    for b in range(1, count):

        @pl.when(b > me)
        def _():
            s.kvall[:, b * rows : (b + 1) * rows] = jnp.zeros(
                (2, rows, HEAD_WIDTH), s.kvall.dtype
            )

    def pump(u):
        def run():
            if u < early:
                for d in range(2):
                    s.relay(d, 0, u, forward=d == 1)

        return run

    s.delta([lambda: None] + [pump(u) for u in range(3)])
    s.chain()
    for u in range(early, units):
        copy, go = s.along(0, 0, u)
        pl.when(go)(copy.start)
    for u in range(early):
        s.onward(0, 0, u)
    s.project_out()
    for u in range(early, units):
        for d in range(2):
            s.relay(d, 0, u)
    for d in range(2):
        s.share_kv(d, 0)
    s.hidden[s.slab_of(s.lane)] = s.hidden_slab().astype(s.hidden.dtype)
    s.send_hidden()
    for j in range(1, count - 1):
        for d in range(2):
            s.relay(d, j, 0)
    for j in range(1, count - 1):
        for d in range(2):
            s.share_kv(d, j)
    s.wait_hidden()
    save_hidden = s.load(s.hidden, s.hidden_out)
    s.normed[...] = s.scaled(s.hidden[...])

    for j in range(count - 1):
        for d in range(2):
            s.wait_kv(d, j)
    own_block = pl.ds(pl.multiple_of(me * rows, rows), rows)
    for kind in range(2):
        s.kvall[kind, own_block] = jnp.dot(
            s.normed[...],
            s.wkv[:, kind * HEAD_WIDTH : (kind + 1) * HEAD_WIDTH],
            preferred_element_type=jnp.float32,
        ).astype(s.kvall.dtype)

    def later(e, block, axis, index, kind, send, recv):
        place = s.kvall.at[kind, pl.ds(pl.multiple_of(s.clamp(block) * rows, rows), rows)]
        return remote(place, place, send.at[e - 1], recv.at[e - 1], axis, index)

    def sent_kv(e):
        return later(e, me, "seq", s.clamp(me + e), s.core, s.kv_send, s.kv_recv)

    def mate_kv(e, kind):
        return later(e, me - e, "head", s.mate, kind, s.km_send, s.km_recv)

    for e in range(1, count):
        pl.when(me + e < count)(sent_kv(e).start)

    for j in range(1, count - 1):
        for u in range(1, units):
            for d in range(2):
                if (j, u) < (count - 2, 1) or count == 2:
                    s.relay(d, j, u)

    for e in range(1, count):

        @pl.when(me >= e)
        def _():
            later(e, me - e, "seq", s.clamp(me - e), s.core, s.kv_send, s.kv_recv).wait_recv()
            mate_kv(e, s.core).start()

    for e in range(1, count):
        pl.when(me >= e)(mate_kv(e, 1 - s.core).wait_recv)

    for copy in load_q:
        copy.wait()
    keys_total = count * rows
    at_query = me * rows + lax.broadcasted_iota(jnp.int32, (rows, keys_total), 0)
    at_key = lax.broadcasted_iota(jnp.int32, (rows, keys_total), 1)
    visible = (at_key <= at_query) & (at_key < s.length_ref[0])
    for i in range(s.query_heads):
        if count > 2:
            for d in range(2):
                s.relay(d, count - 2, i + 1)
        for j in range(count - 1):
            for d in range(2):
                _, here = s.arriving(d, j, i + 1)

                @pl.when(here)
                def _():
                    for e in range(1, groups):
                        s.across(e, d, j, i + 1, s.source_of(e)).wait_recv()

        projected = jnp.dot(s.normed[...], s.wq[i], preferred_element_type=jnp.float32)
        mixed = s.attend(
            projected[:, :HEAD_WIDTH].astype(jnp.bfloat16), s.kvall[0], s.kvall[1], visible
        )
        s.attended[:, i * HEAD_WIDTH : (i + 1) * HEAD_WIDTH] = (
            mixed * jax.nn.sigmoid(projected[:, HEAD_WIDTH:])
        ).astype(s.attended.dtype)
    save_attended = s.load(s.attended, s.attention_out)

    s.end()
    s.end_weights(units)
    for e in range(1, count):
        pl.when(me + e < count)(sent_kv(e).wait_send)
        pl.when(me >= e)(mate_kv(e, s.core).wait_send)
    save_hidden.wait()
    save_attended.wait()


class Split(Ring):
    def weights(self, d, dist, p):
        sign = sign_of(d)
        peer = self.me + sign * dist
        wide = self.wq.shape[1]
        size = self.piece // PIECES
        first = pl.multiple_of(self.part * self.piece + p * size, size)
        copy = remote(
            self.qw_in.at[
                pl.ds(first, size),
                pl.ds(pl.multiple_of(self.clamp(peer) * wide, wide), wide),
            ],
            self.weight_rows(self.me, self.part, p),
            self.w_send.at[d, dist - 1, p],
            self.w_recv.at[d, dist - 1, p],
            "seq",
            self.clamp(peer),
        )
        return copy, self.inside(peer)

    def weight_rows(self, block, which, p):
        size = self.piece // PIECES
        first = self.clamp(block) * self.depth + which * self.piece + p * size
        return self.wq.at[pl.ds(pl.multiple_of(first, size), size)]

    def weights_across(self, e, d, dist, which, p):
        place = self.weight_rows(self.me - sign_of(d) * dist, which, p)
        return remote(
            place,
            place,
            self.wy_send.at[e - 1, d, dist - 1, p],
            self.wy_recv.at[e - 1, d, dist - 1, p],
            "groups",
            lax.rem(self.part + e, self.groups),
        )

    def weights_relay(self, d, dist):
        block = self.me - sign_of(d) * dist

        @pl.when(self.inside(block))
        def _():
            for p in range(PIECES):
                place = self.weight_rows(block, self.part, p)
                remote(
                    place,
                    place,
                    self.w_send.at[d, dist - 1, p],
                    self.w_recv.at[d, dist - 1, p],
                    "seq",
                    self.clamp(block),
                ).wait_recv()
                for e in range(1, self.groups):
                    self.weights_across(e, d, dist, self.part, p).start()

    def weights_wait(self, d, dist):
        @pl.when(self.inside(self.me - sign_of(d) * dist))
        def _():
            for e in range(1, self.groups):
                for p in range(PIECES):
                    self.weights_across(e, d, dist, self.source_of(e), p).wait_recv()


    def place(self, block, index):
        first = block * self.rows + index * self.slab
        return self.every.at[pl.ds(pl.multiple_of(first, self.slab), self.slab)]

    def far(self, d, dist, block):
        place = self.place(self.clamp(block), self.lane)
        return remote(
            place,
            place,
            self.n_send.at[d, dist],
            self.n_recv.at[d, dist],
            "seq",
            self.clamp(self.me + sign_of(d)),
        )

    def rows_onward(self, d, dist):
        block = self.me - sign_of(d) * dist
        go = self.inside(block) & self.inside(self.me + sign_of(d))
        return self.far(d, dist, block), go

    def near(self, d, dist, f, block, index):
        place = self.place(self.clamp(block), index)
        peer = lax.rem(self.lane + MATES * f, self.heads)
        return remote(
            place,
            place,
            self.x_send.at[d, dist, f - 1],
            self.x_recv.at[d, dist, f - 1],
            "head",
            peer,
        )

    def twin(self, d, dist, f, block, index):
        place = self.place(self.clamp(block), index)
        return remote(
            place, place, self.t_send.at[d, dist, f], self.t_recv.at[d, dist, f], "head", self.mate
        )

    def back(self, f, lane):
        return lax.rem(lane + self.heads - MATES * f, self.heads)

    def chips(self):
        return range(1, self.heads // MATES)

    def block_at(self, d, dist):
        return self.me - sign_of(d) * dist

    def steps(self, dist):
        return (0,) if dist == 0 else (0, 1)

    def rows_sent(self, d, dist):
        block = self.block_at(d, dist)

        @pl.when(self.inside(block))
        def _():
            if dist > 0:
                self.far(d, dist - 1, block).wait_recv()
            for f in self.chips():
                self.near(d, dist, f, block, self.lane).start()
            self.twin(d, dist, 0, block, self.lane).start()

        if 0 < dist < self.count - 1:
            copy, go = self.rows_onward(d, dist)
            pl.when(go)(copy.start)

    def rows_passed(self, d, dist):
        block = self.block_at(d, dist)

        @pl.when(self.inside(block))
        def _():
            for f in self.chips():
                self.near(d, dist, f, block, self.back(f, self.lane)).wait_recv()
                self.twin(d, dist, f, block, self.back(f, self.lane)).start()

    def rows_ready(self, d, dist, block):
        for f in range(self.heads // MATES):
            self.twin(d, dist, f, block, self.back(f, self.mate)).wait_recv()

    def end_rows(self):
        for dist in range(self.count - 1):
            for d in range(2):
                copy, go = self.rows_onward(d, dist)
                pl.when(go)(copy.wait_send)
        for dist in range(self.count):
            for d in self.steps(dist):
                block = self.block_at(d, dist)

                @pl.when(self.inside(block))
                def _():
                    for f in self.chips():
                        self.near(d, dist, f, block, self.lane).wait_send()
                    for f in range(self.heads // MATES):
                        self.twin(d, dist, f, block, self.back(f, self.lane)).wait_send()


def split_kernel(sizes, names, *refs):
    s = Split(sizes, names, refs)
    count, groups, me, rows = s.count, s.groups, s.me, s.rows
    wide = s.wq.shape[1]
    mine = wide // (2 * HEAD_WIDTH)
    s.begin()
    last = count - 1

    def send_weights(d, dist):
        for p in range(PIECES):
            copy, go = s.weights(d, dist, p)
            pl.when(go)(copy.start)

    for copy in s.load_kv:
        copy.wait()
    for d in range(2):
        copy, go = s.along(d, 0, 0)
        pl.when(go)(copy.start)
    pl.when(me > 0)(functools.partial(send_weights, 0, 1))
    s.load_rest()
    load_q = s.load(
        s.qw_in.at[:, pl.ds(pl.multiple_of(me * wide, wide), wide)], s.wq.at[s.own_rows]
    )

    def pump_heads():
        @pl.when(me > 0)
        def _():
            s.relay(0, 0, 0, forward=False)
            s.relay(1, 0, 0)
            send_weights(1, 1)

    def pump_updates():
        @pl.when(me > 0)
        def _():
            for j in range(1, last - 1):
                s.relay(1, j, 0)

        pl.when(me > 1)(functools.partial(s.weights_relay, 0, 1))
        for dist in range(2, count):
            send_weights(1, dist)

    s.delta([pump_heads, lambda: None, lambda: None, pump_updates])
    s.chain()
    s.onward(0, 0, 0)
    s.project_out()
    s.kv_relays(0, 1, last - 1)
    for dist in range(1, last):
        pl.when(me == dist)(functools.partial(s.rows_sent, 0, dist))
    hidden = s.hidden_slab().astype(s.hidden.dtype)
    s.hidden[s.slab_of(s.lane)] = hidden
    s.every[pl.ds(pl.multiple_of(me * rows + s.lane * s.slab, s.slab), s.slab)] = s.scaled(hidden)
    for d in range(2):
        copy, go = s.rows_onward(d, 0)
        pl.when(go)(copy.start)
    s.rows_sent(0, 0)

    def send_far():
        for dist in range(last, 1, -1):
            send_weights(0, dist)

    def far_weights(d):
        for dist in range(last - 1, 1, -1):
            s.weights_relay(d, dist)

    pl.when((me != 1) & (me != last))(functools.partial(s.rows_sent, 0, 1))

    @pl.when(me == 0)
    def _():
        send_weights(0, 1)
        s.relay(1, 0, 0)

    pl.when(me == 1)(functools.partial(s.weights_relay, 0, 1))
    s.weights_relay(1, 1)
    pl.when(me > 0)(send_far)
    for d in range(2):
        s.share_kv(d, 0)
    pl.when(me == 0)(functools.partial(s.kv_relays, 1, 1, last - 1))
    for d in range(2):
        s.kv_relays(d, last - 1, last)
    pl.when(me > 0)(functools.partial(far_weights, 1))
    if last > 1:
        s.rows_sent(0, last)
    s.rows_passed(0, 0)

    @pl.when(me == 0)
    def _():
        s.weights_relay(1, last)
        send_far()

    if last > 1:
        s.weights_relay(0, last)
    pl.when(me == last)(functools.partial(s.rows_sent, 0, 1))
    s.rows_sent(1, 1)
    for j in range(1, last):
        for d in range(2):
            s.share_kv(d, j)
    if last > 1:
        s.rows_passed(0, last)
    far_weights(0)
    for dist in range(2, last):
        pl.when(me != dist)(functools.partial(s.rows_sent, 0, dist))
    pl.when(me == 0)(functools.partial(far_weights, 1))
    for dist in range(2, last):
        s.rows_sent(1, dist)
    s.rows_passed(0, 1)
    s.rows_passed(1, 1)
    for dist in range(2, last):
        s.rows_passed(0, dist)
    if last > 1:
        s.rows_sent(1, last)
    for dist in range(2, last):
        s.rows_passed(1, dist)

    def project(first, size):
        at = pl.ds(pl.multiple_of(first, rows), size)
        x = s.every[at]
        for i in range(mine):
            first = i * 2 * HEAD_WIDTH
            query = jnp.dot(
                x, s.wq[:, first : first + HEAD_WIDTH], preferred_element_type=jnp.float32
            )
            gate = jnp.dot(
                x,
                s.wq[:, first + HEAD_WIDTH : first + 2 * HEAD_WIDTH],
                preferred_element_type=jnp.float32,
            )
            s.asked[i, at] = query.astype(jnp.bfloat16)
            s.opened[i, at] = jax.nn.sigmoid(gate)
        for kind in range(2):
            s.kvall[kind, at] = jnp.dot(
                x,
                s.wkv[:, kind * HEAD_WIDTH : (kind + 1) * HEAD_WIDTH],
                preferred_element_type=jnp.float32,
            ).astype(s.kvall.dtype)

    upper = 2 * me >= count

    def ready(far):
        for dist in range(count):
            for d in s.steps(dist):
                block = s.block_at(d, dist)
                end = jnp.where(upper, 0, last)
                wanted = block == end if far else block != end

                @pl.when(s.inside(block) & wanted)
                def _():
                    s.rows_ready(d, dist, block)

    s.send_hidden()
    for j in range(last):
        for d in range(2):
            s.wait_kv(d, j)
    load_q.wait()
    for dist in range(1, count):
        for d in range(2):
            s.weights_wait(d, dist)
    ready(False)
    project(jnp.where(upper, rows, 0), last * rows)
    if last > 1:
        s.rows_passed(1, last)
    ready(True)
    project(jnp.where(upper, 0, last * rows), rows)

    span = mine * HEAD_WIDTH
    length = s.length_ref[0]

    def result(b, rank):
        return remote(
            s.attended.at[b],
            s.attention_out.at[:, pl.ds(pl.multiple_of(rank * span, span), span)],
            s.r_send.at[b],
            s.r_recv.at[rank],
            "seq",
            b,
        )

    for b in range(count):
        seen = (b + 1) * rows
        at_query = b * rows + lax.broadcasted_iota(jnp.int32, (rows, seen), 0)
        at_key = lax.broadcasted_iota(jnp.int32, (rows, seen), 1)
        visible = (at_key <= at_query) & (at_key < length)
        at = slice(b * rows, seen)
        for i in range(mine):
            mixed = s.attend(s.asked[i, at], s.kvall[0, :seen], s.kvall[1, :seen], visible)
            s.attended[b, :, i * HEAD_WIDTH : (i + 1) * HEAD_WIDTH] = (
                mixed * s.opened[i, at]
            ).astype(s.attended.dtype)

        @pl.when(me != b)
        def _():
            result(b, me).start()

    own = s.load(
        s.attended.at[me],
        s.attention_out.at[:, pl.ds(pl.multiple_of(me * span, span), span)],
    )
    s.wait_hidden()
    save_hidden = s.load(s.hidden, s.hidden_out)
    for b in range(count):
        pl.when(me != b)(result(b, jnp.int32(b)).wait_recv)

    for b in range(count):
        pl.when(me != b)(result(b, me).wait_send)
    s.end()
    s.end_weights(1)
    s.end_rows()
    for dist in range(1, count):
        for d in range(2):
            for p in range(PIECES):
                copy, go = s.weights(d, dist, p)
                pl.when(go)(copy.wait_send)

            @pl.when(s.inside(me - sign_of(d) * dist))
            def _():
                for e in range(1, groups):
                    for p in range(PIECES):
                        s.weights_across(e, d, dist, s.part, p).wait_send()

    save_hidden.wait()
    own.wait()


def write_kernel(first_in, second_in, first_out, second_out, first, second, ins, outs):
    pairs = ((first_in, first, first_out), (second_in, second, second_out))
    reads = [pltpu.make_async_copy(a, b, ins.at[i]) for i, (a, b, _) in enumerate(pairs)]
    writes = [pltpu.make_async_copy(b, c, outs.at[i]) for i, (_, b, c) in enumerate(pairs)]
    for read in reads:
        read.start()
    for read, write in zip(reads, writes):
        read.wait()
        write.start()
    for write in writes:
        write.wait()


def shards(
    residual,
    query_in,
    key_in,
    value_in,
    gating_in,
    beta_logit,
    decay_logit,
    seq_length,
    conv_query,
    conv_key,
    conv_value,
    decay_rate,
    norm_gain,
    out_weight,
    attn_gain,
    query_weight,
    key_value_weight,
):
    count = lax.axis_size("seq")
    groups = lax.axis_size("groups")
    heads = lax.axis_size("head")
    rows, model = residual.shape
    value_heads = beta_logit.shape[1]
    query_heads = query_weight.shape[1] // (2 * HEAD_WIDTH)
    width = query_in.shape[1] + key_in.shape[1] + value_in.shape[1]
    depth = query_weight.shape[0] * count
    slab = rows // heads
    f32, bf16 = jnp.float32, jnp.bfloat16
    dma = pltpu.SemaphoreType.DMA
    anywhere = pl.BlockSpec(memory_space=pl.ANY)
    smem = pl.BlockSpec(memory_space=pltpu.SMEM)
    rate = decay_rate[None, :]
    beta_t, decay_t = beta_logit.T, decay_logit.T
    gain = norm_gain[None, :]
    attn = attn_gain[None, :]
    like = lambda a: pltpu.VMEM(a.shape, a.dtype)
    split = query_heads % count == 0
    units = 1 if split else query_heads + 1
    scratch = dict(
        q_ref=like(query_in),
        k_ref=like(key_in),
        v_ref=like(value_in),
        gate_ref=like(gating_in),
        beta_ref=like(beta_t),
        decay_ref=like(decay_t),
        cq_ref=like(conv_query),
        ck_ref=like(conv_key),
        cv_ref=like(conv_value),
        rate_ref=like(rate),
        gain_ref=like(gain),
        ow_ref=like(out_weight),
        again_ref=like(attn),
        residual_ref=pltpu.VMEM((slab, model), bf16),
        wkv=pltpu.VMEM((depth, 2 * HEAD_WIDTH), bf16),
        tail_q=pltpu.VMEM((TAIL, query_in.shape[1]), bf16),
        tail_k=pltpu.VMEM((TAIL, key_in.shape[1]), bf16),
        tail_v=pltpu.VMEM((TAIL, value_in.shape[1]), bf16),
        joined=pltpu.VMEM((rows + PAD, width), f32),
        mapping=pltpu.VMEM((value_heads, DK + rows, DK), bf16),
        local=pltpu.VMEM((value_heads, rows, DV), f32),
        injected=pltpu.VMEM((value_heads, DK, DV), f32),
        enter=pltpu.VMEM((value_heads, DK, DV), bf16),
        leave=pltpu.VMEM((value_heads, DK, DV), bf16),
        gated=pltpu.VMEM((rows, value_heads * DV), bf16),
        summed=pltpu.VMEM((rows, model), f32),
        partial=pltpu.VMEM((rows, model), bf16),
        landed=pltpu.VMEM((heads - 1, slab, model), bf16),
        hidden=pltpu.VMEM((rows, model), bf16),
        kvall=pltpu.VMEM((2, count * rows, HEAD_WIDTH), bf16),
        load_sems=dma((24 + query_heads,)),
        tail_send=dma((3,)),
        tail_recv=dma((3,)),
        state_send=dma((value_heads,)),
        state_recv=dma((value_heads,)),
        z_send=dma((2, count - 1, units)),
        z_recv=dma((2, count - 1, units)),
        y_send=dma((groups - 1, 2, count - 1, units)),
        y_recv=dma((groups - 1, 2, count - 1, units)),
        m_send=dma((2, count - 1)),
        m_recv=dma((2, count - 1)),
        my_send=dma((groups - 1, 2, count - 1)),
        my_recv=dma((groups - 1, 2, count - 1)),
        rs_send=dma((heads - 1,)),
        rs_recv=dma((heads - 1,)),
        ag_send=dma((heads - 1,)),
        ag_recv=dma((heads - 1,)),
    )
    if split:
        mine = query_heads // count
        chips = heads // MATES
        scratch.update(
            wq=pltpu.VMEM((depth, mine * 2 * HEAD_WIDTH), bf16),
            every=pltpu.VMEM((count * rows, model), bf16),
            asked=pltpu.VMEM((mine, count * rows, HEAD_WIDTH), bf16),
            opened=pltpu.VMEM((mine, count * rows, HEAD_WIDTH), f32),
            attended=pltpu.VMEM((count, rows, mine * HEAD_WIDTH), bf16),
            w_send=dma((2, count - 1, PIECES)),
            w_recv=dma((2, count - 1, PIECES)),
            wy_send=dma((groups - 1, 2, count - 1, PIECES)),
            wy_recv=dma((groups - 1, 2, count - 1, PIECES)),
            n_send=dma((2, count - 1)),
            n_recv=dma((2, count - 1)),
            x_send=dma((2, count, chips - 1)),
            x_recv=dma((2, count, chips - 1)),
            t_send=dma((2, count, chips)),
            t_recv=dma((2, count, chips)),
            r_send=dma((count,)),
            r_recv=dma((count,)),
        )
    else:
        scratch.update(
            wq=pltpu.VMEM((query_heads, depth, 2 * HEAD_WIDTH), bf16),
            normed=pltpu.VMEM((rows, model), bf16),
            attended=pltpu.VMEM((rows, query_heads * HEAD_WIDTH), bf16),
            kv_send=dma((count - 1,)),
            kv_recv=dma((count - 1,)),
            km_send=dma((count - 1,)),
            km_recv=dma((count - 1,)),
        )
    results = pl.pallas_call(
        functools.partial(
            split_kernel if split else ring_kernel,
            (count, groups, heads),
            INPUTS + OUTPUTS + list(scratch),
        ),
        out_shape=(
            jax.ShapeDtypeStruct(residual.shape, bf16),
            jax.ShapeDtypeStruct((rows, query_heads * HEAD_WIDTH), bf16),
        ),
        in_specs=[anywhere] * 7 + [smem] + [anywhere] * 9,
        out_specs=(anywhere, anywhere),
        scratch_shapes=list(scratch.values()),
        compiler_params=pltpu.CompilerParams(
            collective_id=0, has_side_effects=True, vmem_limit_bytes=56 * 2**20
        ),
        name="layer",
    )(
        residual,
        query_in,
        key_in,
        value_in,
        gating_in,
        beta_t,
        decay_t,
        seq_length,
        conv_query,
        conv_key,
        conv_value,
        rate,
        gain,
        out_weight,
        attn,
        query_weight,
        key_value_weight,
    )
    return pl.pallas_call(
        write_kernel,
        out_shape=tuple(jax.ShapeDtypeStruct(a.shape, a.dtype) for a in results),
        in_specs=[anywhere] * 2,
        out_specs=(anywhere, anywhere),
        scratch_shapes=[like(a) for a in results] + [dma((2,)), dma((2,))],
        compiler_params=pltpu.CompilerParams(vmem_limit_bytes=56 * 2**20),
        name="write",
    )(*results)


def solution(mesh):
    placed = (
        P(("groups", "seq"), None),
        P(("groups", "seq"), "head"),
        P(("groups", "seq"), "head"),
        P(("groups", "seq"), "head"),
        P(("groups", "seq"), "head"),
        P(("groups", "seq"), "head"),
        P(("groups", "seq"), "head"),
        P("groups"),
        P(None, "head"),
        P(None, "head"),
        P(None, "head"),
        P("head"),
        P(),
        P("head", None),
        P(),
        P("seq", "head"),
        P("seq", None),
    )
    return jax.shard_map(
        shards,
        mesh=mesh,
        in_specs=placed,
        out_specs=(P(("groups", "seq"), None), P(("groups", "seq"), "head")),
        check_vma=False,
    )
```

```python
import functools

import jax
import jax.numpy as jnp
from jax import lax
from jax.experimental import pallas as pl
from jax.experimental.pallas import tpu as pltpu
from jax.sharding import PartitionSpec as P

DK = 128
DV = 128
QUERY_HEADS = 16
KEY_VALUE_HEADS = 2
HEAD_WIDTH = 256
CONV = 4
PAD = 8
TAIL = 8
MATES = 2
EARLY = 3
PIECES = 2

EPSILON = 1e-06
NEGATIVE = -1e30
MESH = pl.DeviceIdType.MESH
HIGHEST = lax.Precision.HIGHEST


def exact(a, b, contract=((1,), (0,))):
    return lax.dot_general(
        a, b, (contract, ((), ())), precision=HIGHEST, preferred_element_type=jnp.float32
    )


def mm(a, b, contract=((1,), (0,))):
    return lax.dot_general(
        a.astype(jnp.bfloat16),
        b.astype(jnp.bfloat16),
        (contract, ((), ())),
        preferred_element_type=jnp.float32,
    )


def softplus(x):
    return jnp.maximum(x, 0.0) + jnp.log1p(jnp.exp(-jnp.abs(x)))


def unit(x):
    return x / jnp.sqrt(jnp.sum(x * x, -1, keepdims=True) + EPSILON)


INPUTS = [
    "residual_in",
    "q_in",
    "k_in",
    "v_in",
    "gate_in",
    "beta_in",
    "decay_in",
    "length_ref",
    "cq_in",
    "ck_in",
    "cv_in",
    "rate_in",
    "gain_in",
    "ow_in",
    "again_in",
    "qw_in",
    "kvw_in",
]
OUTPUTS = ["hidden_out", "attention_out"]


def remote(source, target, send, recv, axis, index):
    return pltpu.make_async_remote_copy(
        src_ref=source,
        dst_ref=target,
        send_sem=send,
        recv_sem=recv,
        device_id={axis: index},
        device_id_type=MESH,
    )


def sign_of(d):
    return 1 if d == 0 else -1


class Layer:
    def __init__(self, sizes, names, refs):
        self.count, self.groups, self.heads = sizes
        for name, ref in zip(names, refs, strict=True):
            setattr(self, name, ref)
        self.me = lax.axis_index("seq")
        self.part = lax.axis_index("groups")
        self.lane = lax.axis_index("head")
        self.core = lax.rem(self.lane, MATES)
        self.mate = self.lane + 1 - 2 * self.core
        self.rows = self.q_ref.shape[0]
        self.key_heads = self.q_ref.shape[1] // DK
        self.value_heads = self.v_ref.shape[1] // DV
        self.share = self.value_heads // self.key_heads
        self.depth = self.qw_in.shape[0]
        self.piece = self.depth // self.groups
        self.quarter = self.piece // MATES
        self.slab = self.rows // self.heads
        self.query_heads = self.qw_in.shape[1] // (2 * HEAD_WIDTH)
        self.kv_head = self.lane * self.query_heads // (QUERY_HEADS // KEY_VALUE_HEADS)
        self.own_rows = pl.ds(pl.multiple_of(self.me * self.depth, self.depth), self.depth)
        self.follower = self.clamp(self.me + 1)
        self.loads = 0

    def load(self, source, target):
        copy = pltpu.make_async_copy(source, target, self.load_sems.at[self.loads])
        copy.start()
        self.loads += 1
        return copy

    def inside(self, block):
        return (block >= 0) & (block < self.count)

    def clamp(self, block):
        return jnp.clip(block, 0, self.count - 1)

    def slab_of(self, index):
        return pl.ds(pl.multiple_of(index * self.slab, self.slab), self.slab)


    def kv_spot(self, block, which, half):
        first = block * self.depth + which * self.piece + half * self.quarter
        return self.wkv.at[pl.ds(pl.multiple_of(first, self.quarter), self.quarter)]

    def begin(self):
        load = self.load
        self.load_kv = [
            load(
                self.kvw_in.at[
                    :,
                    pl.ds(
                        pl.multiple_of(
                            (kind * KEY_VALUE_HEADS + self.kv_head) * HEAD_WIDTH, HEAD_WIDTH
                        ),
                        HEAD_WIDTH,
                    ),
                ],
                self.wkv.at[self.own_rows, pl.ds(kind * HEAD_WIDTH, HEAD_WIDTH)],
            )
            for kind in range(2)
        ]
        self.load_decay = [
            load(self.decay_in, self.decay_ref),
            load(self.rate_in, self.rate_ref),
            load(self.beta_in, self.beta_ref),
        ]
        self.load_conv = [
            load(self.q_in, self.q_ref),
            load(self.k_in, self.k_ref),
            load(self.v_in, self.v_ref),
            load(self.cq_in, self.cq_ref),
            load(self.ck_in, self.ck_ref),
            load(self.cv_in, self.cv_ref),
        ]

        barrier = pltpu.get_barrier_semaphore()
        for axis, size, place in (
            ("seq", self.count, self.me),
            ("groups", self.groups, self.part),
            ("head", self.heads, self.lane),
        ):
            for e in range(1, size):
                pl.semaphore_signal(
                    barrier,
                    inc=1,
                    device_id={axis: lax.rem(place + e, size)},
                    device_id_type=MESH,
                )
        pl.semaphore_wait(barrier, self.count + self.groups + self.heads - 3)

        last = pl.ds(self.rows - TAIL, TAIL)
        self.tails = [
            remote(
                source.at[last],
                target,
                self.tail_send.at[i],
                self.tail_recv.at[i],
                "seq",
                self.follower,
            )
            for i, (source, target) in enumerate(
                (
                    (self.q_in, self.tail_q),
                    (self.k_in, self.tail_k),
                    (self.v_in, self.tail_v),
                )
            )
        ]

        @pl.when(self.me < self.count - 1)
        def _():
            for copy in self.tails:
                copy.start()

    def load_rest(self):
        load = self.load
        self.load_late = [
            load(self.gate_in, self.gate_ref),
            load(self.gain_in, self.gain_ref),
            load(self.ow_in, self.ow_ref),
            load(self.residual_in.at[self.slab_of(self.lane)], self.residual_ref),
            load(self.again_in, self.again_ref),
        ]

    def delta(self, pumps):
        rows, value_heads, share = self.rows, self.value_heads, self.share
        key_heads = self.key_heads
        for copy in self.load_decay:
            copy.wait()
        length = self.length_ref[0]
        at = self.me * rows + lax.broadcasted_iota(jnp.int32, (value_heads, rows), 1)
        alive = (at < length).astype(jnp.float32)
        beta_t = jax.nn.sigmoid(self.beta_ref[...]) * alive
        square = (value_heads, value_heads)
        diagonal = lax.broadcasted_iota(jnp.int32, square, 0) == lax.broadcasted_iota(
            jnp.int32, square, 1
        )
        rate = jnp.sum(jnp.where(diagonal, self.rate_ref[...], 0.0), -1, keepdims=True)
        step_t = -rate * softplus(self.decay_ref[...]) * alive
        row = lax.broadcasted_iota(jnp.int32, (rows, rows), 0)
        column = lax.broadcasted_iota(jnp.int32, (rows, rows), 1)
        inclusive = row >= column
        run_t = exact(step_t, (row <= column).astype(jnp.float32))
        blank = jnp.zeros((rows - 2 * value_heads, rows), jnp.float32)
        turned_over = jnp.concatenate([beta_t, run_t, blank], 0).T
        beta = turned_over[:, :value_heads]
        run = turned_over[:, value_heads : 2 * value_heads]
        growth = jnp.exp(run)
        self.final = growth[rows - 1 : rows]
        ending_t = jnp.exp(run_t[:, rows - 1 : rows] - run_t)
        eye = (row == column).astype(jnp.float32)

        for copy in self.load_conv:
            copy.wait()
        q_width = key_heads * DK
        joined = self.joined
        joined[PAD:, :q_width] = self.q_ref[...].astype(jnp.float32)
        joined[PAD:, q_width : 2 * q_width] = self.k_ref[...].astype(jnp.float32)
        joined[PAD:, 2 * q_width :] = self.v_ref[...].astype(jnp.float32)

        @pl.when(self.me == 0)
        def _():
            self.enter[...] = jnp.zeros_like(self.enter)
            joined[:PAD] = jnp.zeros((PAD, joined.shape[1]), jnp.float32)

        @pl.when(self.me > 0)
        def _():
            for copy in self.tails:
                copy.wait_recv()
            joined[:PAD, :q_width] = self.tail_q[...].astype(jnp.float32)[TAIL - PAD :]
            joined[:PAD, q_width : 2 * q_width] = self.tail_k[...].astype(jnp.float32)[
                TAIL - PAD :
            ]
            joined[:PAD, 2 * q_width :] = self.tail_v[...].astype(jnp.float32)[TAIL - PAD :]

        def conv(base, taps, h):
            first_column = base + h * DK
            total = jnp.zeros((rows, DK), jnp.float32)
            for j in range(CONV):
                first = PAD - CONV + 1 + j
                total = total + taps[j : j + 1, h * DK : (h + 1) * DK] * joined[
                    first : first + rows, first_column : first_column + DK
                ]
            return total * jax.nn.sigmoid(total)

        queries, keyset, turned, grams = [], [], [], []
        for g in range(key_heads):
            q = unit(conv(0, self.cq_ref, g)) * DK ** (-0.5)
            k = unit(conv(q_width, self.ck_ref, g))
            k_t = k.T
            queries.append(q)
            keyset.append(k)
            turned.append(k_t)
            grams.append(mm(jnp.concatenate([k, q], 0), k_t))
            if g == key_heads // 2 - 1:
                pumps[0]()
        pumps[1]()

        mixes, lower, inverse = [], [], []
        for h in range(value_heads):
            spread = run[:, h : h + 1] - run_t[h : h + 1, :]
            w = jnp.exp(jnp.where(inclusive, spread, NEGATIVE))
            gram = grams[h // share]
            mixes.append((gram[rows:] * w).astype(jnp.bfloat16))
            low = jnp.where(row > column, beta[:, h : h + 1] * w * gram[:rows], 0.0)
            lower.append(low)
            pair = (row // 2 == column // 2) & (row > column)
            inverse.append(eye - jnp.where(pair, low, 0.0))
        size = 2
        while size < rows:
            off = (row // (2 * size) == column // (2 * size)) & (row // size > column // size)
            half = [mm(jnp.where(off, low, 0.0), x) for low, x in zip(lower, inverse)]
            inverse = [x - mm(x, y) for x, y in zip(inverse, half)]
            size *= 2
        pumps[2]()

        for h in range(value_heads):
            k = keyset[h // share]
            v = conv(2 * q_width, self.cv_ref, h)
            b = beta[:, h : h + 1]
            grown = growth[:, h : h + 1]
            wu = mm(inverse[h], jnp.concatenate([b * grown * k, b * v], 1))
            stop_t = (turned[h // share] * ending_t[h : h + 1, :]).astype(jnp.bfloat16)
            both = mm(jnp.concatenate([stop_t, mixes[h]], 0), wu)
            self.mapping[h, :DK] = both[:DK, :DK].astype(jnp.bfloat16)
            self.mapping[h, DK:] = (grown * queries[h // share] - both[DK:, :DK]).astype(
                jnp.bfloat16
            )
            self.injected[h] = both[:DK, DK:]
            self.local[h] = both[DK:, DK:]
        pumps[3]()

    def chain(self):
        for copy in self.load_late[:2]:
            copy.wait()
        self.states = []
        for h in range(self.value_heads):
            copy = remote(
                self.leave.at[h],
                self.enter.at[h],
                self.state_send.at[h],
                self.state_recv.at[h],
                "seq",
                self.follower,
            )
            self.states.append(copy)

            @pl.when(self.me > 0)
            def _():
                copy.wait_recv()

            state = self.enter[h]
            moved = mm(self.mapping[h], state)
            total = self.final[:, h : h + 1] * state.astype(jnp.float32)
            self.leave[h] = (total - moved[:DK] + self.injected[h]).astype(self.leave.dtype)
            o = self.local[h] + moved[DK:]
            scaled = (
                o * lax.rsqrt(jnp.mean(o * o, -1, keepdims=True) + EPSILON) * self.gain_ref[...]
            )
            gate = self.gate_ref[:, h * DV : (h + 1) * DV].astype(jnp.float32)
            self.gated[:, h * DV : (h + 1) * DV] = (
                scaled * (gate * jax.nn.sigmoid(gate))
            ).astype(self.gated.dtype)

            @pl.when(self.me < self.count - 1)
            def _():
                copy.start()

    def project_out(self):
        for copy in self.load_late[2:]:
            copy.wait()
        width = self.ow_ref.shape[1]
        tile = min(512, width)
        for c in range(0, width, tile):
            product = jnp.dot(
                self.gated[...],
                self.ow_ref[:, c : c + tile],
                preferred_element_type=jnp.float32,
            )
            self.summed[:, c : c + tile] = product
            self.partial[:, c : c + tile] = product.astype(self.partial.dtype)
        self.scatter = []
        for e in range(1, self.heads):
            peer = lax.rem(self.lane + e, self.heads)
            self.scatter.append(
                remote(
                    self.partial.at[self.slab_of(peer)],
                    self.landed.at[e - 1],
                    self.rs_send.at[e - 1],
                    self.rs_recv.at[e - 1],
                    "head",
                    peer,
                )
            )
        for copy in self.scatter:
            copy.start()

    def hidden_slab(self):
        for copy in self.scatter:
            copy.wait_recv()
        return self.residual_ref[...].astype(jnp.float32) + (
            self.summed[self.slab_of(self.lane)]
            + sum(self.landed[e].astype(jnp.float32) for e in range(self.heads - 1))
        )

    def gather_hidden(self, e, index):
        place = self.hidden.at[self.slab_of(index)]
        peer = lax.rem(self.lane + e, self.heads)
        return remote(
            place, place, self.ag_send.at[e - 1], self.ag_recv.at[e - 1], "head", peer
        )

    def send_hidden(self):
        for e in range(1, self.heads):
            self.gather_hidden(e, self.lane).start()

    def wait_hidden(self):
        for e in range(1, self.heads):
            self.gather_hidden(e, lax.rem(self.lane + self.heads - e, self.heads)).wait_recv()

    def scaled(self, hidden):
        widened = hidden.astype(jnp.float32)
        mean = jnp.mean(widened * widened, -1, keepdims=True)
        return (widened * lax.rsqrt(mean + EPSILON) * self.again_ref[...]).astype(jnp.bfloat16)

    def end(self):
        @pl.when(self.me < self.count - 1)
        def _():
            for copy in self.tails + self.states:
                copy.wait_send()

        for copy in self.scatter:
            copy.wait_send()
        for e in range(1, self.heads):
            self.gather_hidden(e, self.lane).wait_send()

    def attend(self, queries, keys, values, visible):
        scores = (
            lax.dot_general(
                queries, keys, (((1,), (1,)), ((), ())), preferred_element_type=jnp.float32
            )
            * HEAD_WIDTH ** (-0.5)
        )
        scores = jnp.where(visible, scores, NEGATIVE)
        peak = jnp.max(scores, -1, keepdims=True)
        weights = jnp.where(visible, jnp.exp(scores - peak), 0.0)
        norm = jnp.sum(weights, -1, keepdims=True)
        mixed = jnp.dot(weights.astype(jnp.bfloat16), values, preferred_element_type=jnp.float32)
        return mixed / norm


class Ring(Layer):
    def spot(self, block, which, half, u):
        if u == 0:
            return self.kv_spot(block, which, half)
        first = block * self.depth + which * self.piece
        return self.wq.at[u - 1, pl.ds(pl.multiple_of(first, self.piece), self.piece)]

    def along(self, d, j, u):
        sign = sign_of(d)
        block = self.clamp(self.me - sign * j)
        target = self.spot(block, self.part, self.core, u)
        source = target
        if j == 0 and u > 0:
            source = self.qw_in.at[
                pl.ds(pl.multiple_of(self.part * self.piece, self.piece), self.piece),
                pl.ds((u - 1) * 2 * HEAD_WIDTH, 2 * HEAD_WIDTH),
            ]
        copy = remote(
            source,
            target,
            self.z_send.at[d, j, u],
            self.z_recv.at[d, j, u],
            "seq",
            self.clamp(self.me + sign),
        )
        return copy, self.inside(self.me - sign * j) & self.inside(self.me + sign)

    def arriving(self, d, j, u):
        sign = sign_of(d)
        target = self.spot(self.clamp(self.me - sign * (j + 1)), self.part, self.core, u)
        copy = remote(
            target,
            target,
            self.z_send.at[d, j, u],
            self.z_recv.at[d, j, u],
            "seq",
            self.clamp(self.me + sign),
        )
        return copy, self.inside(self.me - sign * (j + 1))

    def across(self, e, d, j, u, which):
        target = self.spot(self.clamp(self.me - sign_of(d) * (j + 1)), which, self.core, u)
        return remote(
            target,
            target,
            self.y_send.at[e - 1, d, j, u],
            self.y_recv.at[e - 1, d, j, u],
            "groups",
            lax.rem(self.part + e, self.groups),
        )

    def beside(self, d, j, half):
        target = self.kv_spot(self.clamp(self.me - sign_of(d) * (j + 1)), self.part, half)
        return remote(target, target, self.m_send.at[d, j], self.m_recv.at[d, j], "head", self.mate)

    def source_of(self, e):
        return lax.rem(self.part + self.groups - e, self.groups)

    def beyond(self, e, d, j, half):
        target = self.kv_spot(self.clamp(self.me - sign_of(d) * (j + 1)), self.source_of(e), half)
        return remote(
            target,
            target,
            self.my_send.at[e - 1, d, j],
            self.my_recv.at[e - 1, d, j],
            "head",
            self.mate,
        )

    def onward(self, d, j, u):
        if j + 1 < self.count - 1:
            copy, go = self.along(d, j + 1, u)
            pl.when(go)(copy.start)

    def relay(self, d, j, u, forward=True):
        copy, here = self.arriving(d, j, u)

        @pl.when(here)
        def _():
            copy.wait_recv()
            for e in range(1, self.groups):
                self.across(e, d, j, u, self.part).start()
            if u == 0:
                self.beside(d, j, self.core).start()

        if forward:
            self.onward(d, j, u)

    def kv_relays(self, d, first, last):
        for j in range(max(first, 1), last):
            self.relay(d, j, 0)

    def share_kv(self, d, j):
        _, here = self.arriving(d, j, 0)

        @pl.when(here)
        def _():
            for e in range(1, self.groups):
                self.across(e, d, j, 0, self.source_of(e)).wait_recv()
                self.beyond(e, d, j, self.core).start()

    def wait_kv(self, d, j):
        _, here = self.arriving(d, j, 0)

        @pl.when(here)
        def _():
            self.beside(d, j, 1 - self.core).wait_recv()
            for e in range(1, self.groups):
                self.beyond(e, d, j, 1 - self.core).wait_recv()

    def end_weights(self, units):
        for j in range(self.count - 1):
            for d in range(2):
                for u in range(units):
                    copy, go = self.along(d, j, u)
                    pl.when(go)(copy.wait_send)
                _, here = self.arriving(d, j, 0)

                @pl.when(here)
                def _():
                    for e in range(1, self.groups):
                        for u in range(units):
                            self.across(e, d, j, u, self.part).wait_send()
                        self.beyond(e, d, j, self.core).wait_send()
                    self.beside(d, j, self.core).wait_send()


def ring_kernel(sizes, names, *refs):
    s = Ring(sizes, names, refs)
    count, groups, me, rows = s.count, s.groups, s.me, s.rows
    units = s.query_heads + 1
    early = min(EARLY, units)
    s.begin()
    for copy in s.load_kv:
        copy.wait()
    for u in range(units):
        for d in range(2):
            if d == 1 or u < early:
                copy, go = s.along(d, 0, u)
                pl.when(go)(copy.start)
    s.load_rest()
    load_q = [
        s.load(
            s.qw_in.at[:, pl.ds(i * 2 * HEAD_WIDTH, 2 * HEAD_WIDTH)], s.wq.at[i, s.own_rows]
        )
        for i in range(s.query_heads)
    ]

    for b in range(1, count):

        @pl.when(b > me)
        def _():
            s.kvall[:, b * rows : (b + 1) * rows] = jnp.zeros(
                (2, rows, HEAD_WIDTH), s.kvall.dtype
            )

    def pump(u):
        def run():
            if u < early:
                for d in range(2):
                    s.relay(d, 0, u, forward=d == 1)

        return run

    s.delta([lambda: None] + [pump(u) for u in range(3)])
    s.chain()
    for u in range(early, units):
        copy, go = s.along(0, 0, u)
        pl.when(go)(copy.start)
    for u in range(early):
        s.onward(0, 0, u)
    s.project_out()
    for u in range(early, units):
        for d in range(2):
            s.relay(d, 0, u)
    for d in range(2):
        s.share_kv(d, 0)
    s.hidden[s.slab_of(s.lane)] = s.hidden_slab().astype(s.hidden.dtype)
    s.send_hidden()
    for j in range(1, count - 1):
        for d in range(2):
            s.relay(d, j, 0)
    for j in range(1, count - 1):
        for d in range(2):
            s.share_kv(d, j)
    s.wait_hidden()
    save_hidden = s.load(s.hidden, s.hidden_out)
    s.normed[...] = s.scaled(s.hidden[...])

    for j in range(count - 1):
        for d in range(2):
            s.wait_kv(d, j)
    own_block = pl.ds(pl.multiple_of(me * rows, rows), rows)
    for kind in range(2):
        s.kvall[kind, own_block] = jnp.dot(
            s.normed[...],
            s.wkv[:, kind * HEAD_WIDTH : (kind + 1) * HEAD_WIDTH],
            preferred_element_type=jnp.float32,
        ).astype(s.kvall.dtype)

    def later(e, block, axis, index, kind, send, recv):
        place = s.kvall.at[kind, pl.ds(pl.multiple_of(s.clamp(block) * rows, rows), rows)]
        return remote(place, place, send.at[e - 1], recv.at[e - 1], axis, index)

    def sent_kv(e):
        return later(e, me, "seq", s.clamp(me + e), s.core, s.kv_send, s.kv_recv)

    def mate_kv(e, kind):
        return later(e, me - e, "head", s.mate, kind, s.km_send, s.km_recv)

    for e in range(1, count):
        pl.when(me + e < count)(sent_kv(e).start)

    for j in range(1, count - 1):
        for u in range(1, units):
            for d in range(2):
                if (j, u) < (count - 2, 1) or count == 2:
                    s.relay(d, j, u)

    for e in range(1, count):

        @pl.when(me >= e)
        def _():
            later(e, me - e, "seq", s.clamp(me - e), s.core, s.kv_send, s.kv_recv).wait_recv()
            mate_kv(e, s.core).start()

    for e in range(1, count):
        pl.when(me >= e)(mate_kv(e, 1 - s.core).wait_recv)

    for copy in load_q:
        copy.wait()
    keys_total = count * rows
    at_query = me * rows + lax.broadcasted_iota(jnp.int32, (rows, keys_total), 0)
    at_key = lax.broadcasted_iota(jnp.int32, (rows, keys_total), 1)
    visible = (at_key <= at_query) & (at_key < s.length_ref[0])
    for i in range(s.query_heads):
        if count > 2:
            for d in range(2):
                s.relay(d, count - 2, i + 1)
        for j in range(count - 1):
            for d in range(2):
                _, here = s.arriving(d, j, i + 1)

                @pl.when(here)
                def _():
                    for e in range(1, groups):
                        s.across(e, d, j, i + 1, s.source_of(e)).wait_recv()

        projected = jnp.dot(s.normed[...], s.wq[i], preferred_element_type=jnp.float32)
        mixed = s.attend(
            projected[:, :HEAD_WIDTH].astype(jnp.bfloat16), s.kvall[0], s.kvall[1], visible
        )
        s.attended[:, i * HEAD_WIDTH : (i + 1) * HEAD_WIDTH] = (
            mixed * jax.nn.sigmoid(projected[:, HEAD_WIDTH:])
        ).astype(s.attended.dtype)
    save_attended = s.load(s.attended, s.attention_out)

    s.end()
    s.end_weights(units)
    for e in range(1, count):
        pl.when(me + e < count)(sent_kv(e).wait_send)
        pl.when(me >= e)(mate_kv(e, s.core).wait_send)
    save_hidden.wait()
    save_attended.wait()


class Split(Ring):
    def weights(self, d, dist, p):
        sign = sign_of(d)
        peer = self.me + sign * dist
        wide = self.wq.shape[1]
        size = self.piece // PIECES
        first = pl.multiple_of(self.part * self.piece + p * size, size)
        copy = remote(
            self.qw_in.at[
                pl.ds(first, size),
                pl.ds(pl.multiple_of(self.clamp(peer) * wide, wide), wide),
            ],
            self.weight_rows(self.me, self.part, p),
            self.w_send.at[d, dist - 1, p],
            self.w_recv.at[d, dist - 1, p],
            "seq",
            self.clamp(peer),
        )
        return copy, self.inside(peer)

    def weight_rows(self, block, which, p):
        size = self.piece // PIECES
        first = self.clamp(block) * self.depth + which * self.piece + p * size
        return self.wq.at[pl.ds(pl.multiple_of(first, size), size)]

    def weights_across(self, e, d, dist, which, p):
        place = self.weight_rows(self.me - sign_of(d) * dist, which, p)
        return remote(
            place,
            place,
            self.wy_send.at[e - 1, d, dist - 1, p],
            self.wy_recv.at[e - 1, d, dist - 1, p],
            "groups",
            lax.rem(self.part + e, self.groups),
        )

    def weights_relay(self, d, dist):
        block = self.me - sign_of(d) * dist

        @pl.when(self.inside(block))
        def _():
            for p in range(PIECES):
                place = self.weight_rows(block, self.part, p)
                remote(
                    place,
                    place,
                    self.w_send.at[d, dist - 1, p],
                    self.w_recv.at[d, dist - 1, p],
                    "seq",
                    self.clamp(block),
                ).wait_recv()
                for e in range(1, self.groups):
                    self.weights_across(e, d, dist, self.part, p).start()

    def weights_wait(self, d, dist):
        @pl.when(self.inside(self.me - sign_of(d) * dist))
        def _():
            for e in range(1, self.groups):
                for p in range(PIECES):
                    self.weights_across(e, d, dist, self.source_of(e), p).wait_recv()


    def place(self, block, index):
        first = block * self.rows + index * self.slab
        return self.every.at[pl.ds(pl.multiple_of(first, self.slab), self.slab)]

    def far(self, d, dist, block):
        place = self.place(self.clamp(block), self.lane)
        return remote(
            place,
            place,
            self.n_send.at[d, dist],
            self.n_recv.at[d, dist],
            "seq",
            self.clamp(self.me + sign_of(d)),
        )

    def rows_onward(self, d, dist):
        block = self.me - sign_of(d) * dist
        go = self.inside(block) & self.inside(self.me + sign_of(d))
        return self.far(d, dist, block), go

    def near(self, d, dist, f, block, index):
        place = self.place(self.clamp(block), index)
        peer = lax.rem(self.lane + MATES * f, self.heads)
        return remote(
            place,
            place,
            self.x_send.at[d, dist, f - 1],
            self.x_recv.at[d, dist, f - 1],
            "head",
            peer,
        )

    def twin(self, d, dist, f, block, index):
        place = self.place(self.clamp(block), index)
        return remote(
            place, place, self.t_send.at[d, dist, f], self.t_recv.at[d, dist, f], "head", self.mate
        )

    def back(self, f, lane):
        return lax.rem(lane + self.heads - MATES * f, self.heads)

    def chips(self):
        return range(1, self.heads // MATES)

    def block_at(self, d, dist):
        return self.me - sign_of(d) * dist

    def steps(self, dist):
        return (0,) if dist == 0 else (0, 1)

    def rows_sent(self, d, dist):
        block = self.block_at(d, dist)

        @pl.when(self.inside(block))
        def _():
            if dist > 0:
                self.far(d, dist - 1, block).wait_recv()
            for f in self.chips():
                self.near(d, dist, f, block, self.lane).start()
            self.twin(d, dist, 0, block, self.lane).start()

        if 0 < dist < self.count - 1:
            copy, go = self.rows_onward(d, dist)
            pl.when(go)(copy.start)

    def rows_passed(self, d, dist):
        block = self.block_at(d, dist)

        @pl.when(self.inside(block))
        def _():
            for f in self.chips():
                self.near(d, dist, f, block, self.back(f, self.lane)).wait_recv()
                self.twin(d, dist, f, block, self.back(f, self.lane)).start()

    def rows_ready(self, d, dist, block):
        for f in range(self.heads // MATES):
            self.twin(d, dist, f, block, self.back(f, self.mate)).wait_recv()

    def end_rows(self):
        for dist in range(self.count - 1):
            for d in range(2):
                copy, go = self.rows_onward(d, dist)
                pl.when(go)(copy.wait_send)
        for dist in range(self.count):
            for d in self.steps(dist):
                block = self.block_at(d, dist)

                @pl.when(self.inside(block))
                def _():
                    for f in self.chips():
                        self.near(d, dist, f, block, self.lane).wait_send()
                    for f in range(self.heads // MATES):
                        self.twin(d, dist, f, block, self.back(f, self.lane)).wait_send()


def split_kernel(sizes, names, *refs):
    s = Split(sizes, names, refs)
    count, groups, me, rows = s.count, s.groups, s.me, s.rows
    wide = s.wq.shape[1]
    mine = wide // (2 * HEAD_WIDTH)
    s.begin()
    last = count - 1

    def send_weights(d, dist):
        for p in range(PIECES):
            copy, go = s.weights(d, dist, p)
            pl.when(go)(copy.start)

    for copy in s.load_kv:
        copy.wait()
    for d in range(2):
        copy, go = s.along(d, 0, 0)
        pl.when(go)(copy.start)
    pl.when(me > 0)(functools.partial(send_weights, 0, 1))
    s.load_rest()
    load_q = s.load(
        s.qw_in.at[:, pl.ds(pl.multiple_of(me * wide, wide), wide)], s.wq.at[s.own_rows]
    )

    def pump_heads():
        @pl.when(me > 0)
        def _():
            s.relay(0, 0, 0, forward=False)
            s.relay(1, 0, 0)
            send_weights(1, 1)

    def pump_updates():
        @pl.when(me > 0)
        def _():
            for j in range(1, last - 1):
                s.relay(1, j, 0)

        pl.when(me > 1)(functools.partial(s.weights_relay, 0, 1))
        for dist in range(2, count):
            send_weights(1, dist)

    s.delta([pump_heads, lambda: None, lambda: None, pump_updates])
    s.chain()
    s.onward(0, 0, 0)
    s.project_out()
    s.kv_relays(0, 1, last - 1)
    for dist in range(1, last):
        pl.when(me == dist)(functools.partial(s.rows_sent, 0, dist))
    hidden = s.hidden_slab().astype(s.hidden.dtype)
    s.hidden[s.slab_of(s.lane)] = hidden
    s.every[pl.ds(pl.multiple_of(me * rows + s.lane * s.slab, s.slab), s.slab)] = s.scaled(hidden)
    for d in range(2):
        copy, go = s.rows_onward(d, 0)
        pl.when(go)(copy.start)
    s.rows_sent(0, 0)

    def send_far():
        for dist in range(last, 1, -1):
            send_weights(0, dist)

    def far_weights(d):
        for dist in range(last - 1, 1, -1):
            s.weights_relay(d, dist)

    pl.when((me != 1) & (me != last))(functools.partial(s.rows_sent, 0, 1))

    @pl.when(me == 0)
    def _():
        send_weights(0, 1)
        s.relay(1, 0, 0)

    pl.when(me == 1)(functools.partial(s.weights_relay, 0, 1))
    s.weights_relay(1, 1)
    pl.when(me > 0)(send_far)
    for d in range(2):
        s.share_kv(d, 0)
    pl.when(me == 0)(functools.partial(s.kv_relays, 1, 1, last - 1))
    for d in range(2):
        s.kv_relays(d, last - 1, last)
    pl.when(me > 0)(functools.partial(far_weights, 1))
    if last > 1:
        s.rows_sent(0, last)
    s.rows_passed(0, 0)

    @pl.when(me == 0)
    def _():
        s.weights_relay(1, last)
        send_far()

    if last > 1:
        s.weights_relay(0, last)
    pl.when(me == last)(functools.partial(s.rows_sent, 0, 1))
    s.rows_sent(1, 1)
    for j in range(1, last):
        for d in range(2):
            s.share_kv(d, j)
    if last > 1:
        s.rows_passed(0, last)
    far_weights(0)
    for dist in range(2, last):
        pl.when(me != dist)(functools.partial(s.rows_sent, 0, dist))
    pl.when(me == 0)(functools.partial(far_weights, 1))
    for dist in range(2, last):
        s.rows_sent(1, dist)
    s.rows_passed(0, 1)
    s.rows_passed(1, 1)
    for dist in range(2, last):
        s.rows_passed(0, dist)
    if last > 1:
        s.rows_sent(1, last)
    for dist in range(2, last):
        s.rows_passed(1, dist)

    def project_query(first, size):
        at = slice(first, first + size)
        x = s.every[at]
        for i in range(mine):
            left = i * 2 * HEAD_WIDTH
            query = jnp.dot(
                x, s.wq[:, left : left + HEAD_WIDTH], preferred_element_type=jnp.float32
            )
            gate = jnp.dot(
                x,
                s.wq[:, left + HEAD_WIDTH : left + 2 * HEAD_WIDTH],
                preferred_element_type=jnp.float32,
            )
            s.asked[i, at] = query.astype(jnp.bfloat16)
            s.opened[i, at] = jax.nn.sigmoid(gate)

    def project_kv(first, size):
        at = slice(first, first + size)
        x = s.every[at]
        for kind in range(2):
            s.kvall[kind, at] = jnp.dot(
                x,
                s.wkv[:, kind * HEAD_WIDTH : (kind + 1) * HEAD_WIDTH],
                preferred_element_type=jnp.float32,
            ).astype(s.kvall.dtype)

    upper = 2 * me >= count

    def ready(far):
        for dist in range(count):
            for d in s.steps(dist):
                block = s.block_at(d, dist)
                end = jnp.where(upper, 0, last)
                wanted = block == end if far else block != end

                @pl.when(s.inside(block) & wanted)
                def _():
                    s.rows_ready(d, dist, block)

    s.send_hidden()
    for j in range(last):
        for d in range(2):
            s.wait_kv(d, j)

    @pl.when(upper)
    def _():
        ready(True)
        project_kv(0, rows)

    @pl.when(jnp.logical_not(upper))
    def _():
        ready(False)
        project_kv(0, last * rows)

    load_q.wait()
    for dist in range(1, count):
        for d in range(2):
            s.weights_wait(d, dist)

    @pl.when(upper)
    def _():
        project_query(0, rows)
        ready(False)
        project_kv(rows, last * rows)
        project_query(rows, last * rows)

    pl.when(jnp.logical_not(upper))(functools.partial(project_query, 0, last * rows))
    if last > 1:
        s.rows_passed(1, last)

    @pl.when(jnp.logical_not(upper))
    def _():
        ready(True)
        project_kv(last * rows, rows)
        project_query(last * rows, rows)

    span = mine * HEAD_WIDTH
    length = s.length_ref[0]

    def result(b, rank):
        return remote(
            s.attended.at[b],
            s.attention_out.at[:, pl.ds(pl.multiple_of(rank * span, span), span)],
            s.r_send.at[b],
            s.r_recv.at[rank],
            "seq",
            b,
        )

    for b in range(count):
        seen = (b + 1) * rows
        at_query = b * rows + lax.broadcasted_iota(jnp.int32, (rows, seen), 0)
        at_key = lax.broadcasted_iota(jnp.int32, (rows, seen), 1)
        visible = (at_key <= at_query) & (at_key < length)
        at = slice(b * rows, seen)
        for i in range(mine):
            mixed = s.attend(s.asked[i, at], s.kvall[0, :seen], s.kvall[1, :seen], visible)
            s.attended[b, :, i * HEAD_WIDTH : (i + 1) * HEAD_WIDTH] = (
                mixed * s.opened[i, at]
            ).astype(s.attended.dtype)

        @pl.when(me != b)
        def _():
            result(b, me).start()

    own = s.load(
        s.attended.at[me],
        s.attention_out.at[:, pl.ds(pl.multiple_of(me * span, span), span)],
    )
    s.wait_hidden()
    save_hidden = s.load(s.hidden, s.hidden_out)
    for b in range(count):
        pl.when(me != b)(result(b, jnp.int32(b)).wait_recv)

    for b in range(count):
        pl.when(me != b)(result(b, me).wait_send)
    s.end()
    s.end_weights(1)
    s.end_rows()
    for dist in range(1, count):
        for d in range(2):
            for p in range(PIECES):
                copy, go = s.weights(d, dist, p)
                pl.when(go)(copy.wait_send)

            @pl.when(s.inside(me - sign_of(d) * dist))
            def _():
                for e in range(1, groups):
                    for p in range(PIECES):
                        s.weights_across(e, d, dist, s.part, p).wait_send()

    save_hidden.wait()
    own.wait()


def write_kernel(first_in, second_in, first_out, second_out, first, second, ins, outs):
    pairs = ((first_in, first, first_out), (second_in, second, second_out))
    reads = [pltpu.make_async_copy(a, b, ins.at[i]) for i, (a, b, _) in enumerate(pairs)]
    writes = [pltpu.make_async_copy(b, c, outs.at[i]) for i, (_, b, c) in enumerate(pairs)]
    for read in reads:
        read.start()
    for read, write in zip(reads, writes):
        read.wait()
        write.start()
    for write in writes:
        write.wait()


def shards(
    residual,
    query_in,
    key_in,
    value_in,
    gating_in,
    beta_logit,
    decay_logit,
    seq_length,
    conv_query,
    conv_key,
    conv_value,
    decay_rate,
    norm_gain,
    out_weight,
    attn_gain,
    query_weight,
    key_value_weight,
):
    count = lax.axis_size("seq")
    groups = lax.axis_size("groups")
    heads = lax.axis_size("head")
    rows, model = residual.shape
    value_heads = beta_logit.shape[1]
    query_heads = query_weight.shape[1] // (2 * HEAD_WIDTH)
    width = query_in.shape[1] + key_in.shape[1] + value_in.shape[1]
    depth = query_weight.shape[0] * count
    slab = rows // heads
    f32, bf16 = jnp.float32, jnp.bfloat16
    dma = pltpu.SemaphoreType.DMA
    anywhere = pl.BlockSpec(memory_space=pl.ANY)
    smem = pl.BlockSpec(memory_space=pltpu.SMEM)
    rate = decay_rate[None, :]
    beta_t, decay_t = beta_logit.T, decay_logit.T
    gain = norm_gain[None, :]
    attn = attn_gain[None, :]
    like = lambda a: pltpu.VMEM(a.shape, a.dtype)
    split = query_heads % count == 0
    units = 1 if split else query_heads + 1
    scratch = dict(
        q_ref=like(query_in),
        k_ref=like(key_in),
        v_ref=like(value_in),
        gate_ref=like(gating_in),
        beta_ref=like(beta_t),
        decay_ref=like(decay_t),
        cq_ref=like(conv_query),
        ck_ref=like(conv_key),
        cv_ref=like(conv_value),
        rate_ref=like(rate),
        gain_ref=like(gain),
        ow_ref=like(out_weight),
        again_ref=like(attn),
        residual_ref=pltpu.VMEM((slab, model), bf16),
        wkv=pltpu.VMEM((depth, 2 * HEAD_WIDTH), bf16),
        tail_q=pltpu.VMEM((TAIL, query_in.shape[1]), bf16),
        tail_k=pltpu.VMEM((TAIL, key_in.shape[1]), bf16),
        tail_v=pltpu.VMEM((TAIL, value_in.shape[1]), bf16),
        joined=pltpu.VMEM((rows + PAD, width), f32),
        mapping=pltpu.VMEM((value_heads, DK + rows, DK), bf16),
        local=pltpu.VMEM((value_heads, rows, DV), f32),
        injected=pltpu.VMEM((value_heads, DK, DV), f32),
        enter=pltpu.VMEM((value_heads, DK, DV), bf16),
        leave=pltpu.VMEM((value_heads, DK, DV), bf16),
        gated=pltpu.VMEM((rows, value_heads * DV), bf16),
        summed=pltpu.VMEM((rows, model), f32),
        partial=pltpu.VMEM((rows, model), bf16),
        landed=pltpu.VMEM((heads - 1, slab, model), bf16),
        hidden=pltpu.VMEM((rows, model), bf16),
        kvall=pltpu.VMEM((2, count * rows, HEAD_WIDTH), bf16),
        load_sems=dma((24 + query_heads,)),
        tail_send=dma((3,)),
        tail_recv=dma((3,)),
        state_send=dma((value_heads,)),
        state_recv=dma((value_heads,)),
        z_send=dma((2, count - 1, units)),
        z_recv=dma((2, count - 1, units)),
        y_send=dma((groups - 1, 2, count - 1, units)),
        y_recv=dma((groups - 1, 2, count - 1, units)),
        m_send=dma((2, count - 1)),
        m_recv=dma((2, count - 1)),
        my_send=dma((groups - 1, 2, count - 1)),
        my_recv=dma((groups - 1, 2, count - 1)),
        rs_send=dma((heads - 1,)),
        rs_recv=dma((heads - 1,)),
        ag_send=dma((heads - 1,)),
        ag_recv=dma((heads - 1,)),
    )
    if split:
        mine = query_heads // count
        chips = heads // MATES
        scratch.update(
            wq=pltpu.VMEM((depth, mine * 2 * HEAD_WIDTH), bf16),
            every=pltpu.VMEM((count * rows, model), bf16),
            asked=pltpu.VMEM((mine, count * rows, HEAD_WIDTH), bf16),
            opened=pltpu.VMEM((mine, count * rows, HEAD_WIDTH), f32),
            attended=pltpu.VMEM((count, rows, mine * HEAD_WIDTH), bf16),
            w_send=dma((2, count - 1, PIECES)),
            w_recv=dma((2, count - 1, PIECES)),
            wy_send=dma((groups - 1, 2, count - 1, PIECES)),
            wy_recv=dma((groups - 1, 2, count - 1, PIECES)),
            n_send=dma((2, count - 1)),
            n_recv=dma((2, count - 1)),
            x_send=dma((2, count, chips - 1)),
            x_recv=dma((2, count, chips - 1)),
            t_send=dma((2, count, chips)),
            t_recv=dma((2, count, chips)),
            r_send=dma((count,)),
            r_recv=dma((count,)),
        )
    else:
        scratch.update(
            wq=pltpu.VMEM((query_heads, depth, 2 * HEAD_WIDTH), bf16),
            normed=pltpu.VMEM((rows, model), bf16),
            attended=pltpu.VMEM((rows, query_heads * HEAD_WIDTH), bf16),
            kv_send=dma((count - 1,)),
            kv_recv=dma((count - 1,)),
            km_send=dma((count - 1,)),
            km_recv=dma((count - 1,)),
        )
    results = pl.pallas_call(
        functools.partial(
            split_kernel if split else ring_kernel,
            (count, groups, heads),
            INPUTS + OUTPUTS + list(scratch),
        ),
        out_shape=(
            jax.ShapeDtypeStruct(residual.shape, bf16),
            jax.ShapeDtypeStruct((rows, query_heads * HEAD_WIDTH), bf16),
        ),
        in_specs=[anywhere] * 7 + [smem] + [anywhere] * 9,
        out_specs=(anywhere, anywhere),
        scratch_shapes=list(scratch.values()),
        compiler_params=pltpu.CompilerParams(
            collective_id=0, has_side_effects=True, vmem_limit_bytes=56 * 2**20
        ),
        name="layer",
    )(
        residual,
        query_in,
        key_in,
        value_in,
        gating_in,
        beta_t,
        decay_t,
        seq_length,
        conv_query,
        conv_key,
        conv_value,
        rate,
        gain,
        out_weight,
        attn,
        query_weight,
        key_value_weight,
    )
    return pl.pallas_call(
        write_kernel,
        out_shape=tuple(jax.ShapeDtypeStruct(a.shape, a.dtype) for a in results),
        in_specs=[anywhere] * 2,
        out_specs=(anywhere, anywhere),
        scratch_shapes=[like(a) for a in results] + [dma((2,)), dma((2,))],
        compiler_params=pltpu.CompilerParams(vmem_limit_bytes=56 * 2**20),
        name="write",
    )(*results)


def solution(mesh):
    placed = (
        P(("groups", "seq"), None),
        P(("groups", "seq"), "head"),
        P(("groups", "seq"), "head"),
        P(("groups", "seq"), "head"),
        P(("groups", "seq"), "head"),
        P(("groups", "seq"), "head"),
        P(("groups", "seq"), "head"),
        P("groups"),
        P(None, "head"),
        P(None, "head"),
        P(None, "head"),
        P("head"),
        P(),
        P("head", None),
        P(),
        P("seq", "head"),
        P("seq", None),
    )
    return jax.shard_map(
        shards,
        mesh=mesh,
        in_specs=placed,
        out_specs=(P(("groups", "seq"), None), P(("groups", "seq"), "head")),
        check_vma=False,
    )
```
